128 devices in a mesh: tile: 64 (over z, y, x), depth: 2 (over core).
Axes of the slice: x: 4, y: 4, z: 4, core: 2. Of those that a mesh axis runs over, the one named last changes fastest.
Arguments:
- transmission: float32 [2, 2, 1024, 8192], P('depth', None, None, 'tile'), may hold values from -4.2 to 4.2
- probe_modes: float32 [6, 2, 256, 256], replicated, may hold values from -6 to 6
- measured: float32 [256, 256, 256], P('tile'), may hold values from 1 to 30
- scan_rows: int32 [256], P('tile'), may hold values from 0 to 768
- scan_cols: int32 [256], P('tile'), may hold values from 0 to 127
- counts: int32 [64], P('tile'), may hold values from 1 to 4, as said below
- dataset: int32 [256], P('tile'), may hold values from 0 to 15
- dose_scale: float32 [16], replicated, may hold values from 0.5 to 2
- background: float32 [16], replicated, may hold values from 0.5 to 8
Outputs:
- object_grad: float32 [2, 2, 1024, 8192], P('depth', None, None, 'tile')
The draws below stay inside these ranges and needn't reach their ends.
Inputs may be any that keep to these rules, and one draw needn't show every extreme that they name: Tile t's valid positions are its first counts[t] slots; the other slots' rows, columns, datasets and intensities are ignored. Some tile has all 4 slots valid.
All inputs are finite; a program needn't handle non-finite values.
Results may differ from the reference program's by a relative error of at most 0.011.
Values may be sent and summed in bfloat16 or wider, within the bound.
A program may use at most 128 MiB of HBM per device.

```python
import math
import jax
import jax.numpy as jnp
from jax import lax

P_SIZE = 256
MODES = 6
DATASETS = 16
TW = 128
H = 1024
POS_CAP = 4
SLICES = 2
TILES = 64
W = 8192
NPOS = 256
N_TILE = 64


def draw_counts(key, part):
    first_key, second_key, third_key = jax.random.split(key, 3)
    first = jax.random.randint(first_key, (TILES,), 1, POS_CAP + 1)
    second = jax.random.randint(second_key, (TILES,), 1, POS_CAP + 1)
    upper = jnp.maximum(first, second)
    fullest = jax.random.randint(third_key, (), 0, TILES)
    return jnp.where(jnp.arange(TILES) == fullest, POS_CAP, upper).astype(jnp.int32)


def set_ends(array, rng, low, high):
    shape = array.shape
    spot = [jax.random.randint(jax.random.fold_in(rng, axis), (), 0, shape[axis]) for axis in range(len(shape))]
    array = array.at[tuple(spot)].set(low)
    longest = shape.index(max(shape))
    spot[longest] = (spot[longest] + 1) % shape[longest]
    return array.at[tuple(spot)].set(high)


def steps_of(stream_key, shape, cuts, low, high):
    factor_of, own = 1.0, jax.random.fold_in(stream_key, 6)
    for axis_at, shards_of in cuts:
        draws = jnp.exp(jax.random.uniform(jax.random.fold_in(own, axis_at), (shards_of,), jnp.float32, low / len(cuts), high / len(cuts)))
        factor_of = factor_of * jnp.repeat(draws, shape[axis_at] // shards_of).reshape([-1 if axis == axis_at else 1 for axis in range(len(shape))])
    return factor_of


def bell_draw(stream_key, extent, spread, limit, pieces=(), held_as=jnp.bfloat16):
    loudness = steps_of(stream_key, extent, pieces, -0.22, 0.18) if pieces else 1.0
    drawn = jax.random.normal(stream_key, extent, jnp.float32) * spread * loudness
    return jnp.minimum(jnp.maximum(drawn, -limit), limit).astype(held_as)


def setup_inputs(seed: int = 0) -> dict:
    keys = jax.random.split(jax.random.key(seed), 10)
    transmission = bell_draw(keys[0], (SLICES, 2, H, W), 0.7, 4.2, ((0, 2), (3, 64)), jnp.float32)
    probe_modes = bell_draw(keys[1], (MODES, 2, P_SIZE, P_SIZE), 1.0, 6.0, (), jnp.float32)
    measured = jnp.clip(jnp.exp(math.log(30.0) - 3.4011974 * jax.random.uniform(keys[2], (NPOS, P_SIZE, P_SIZE), jnp.float32) ** steps_of(keys[2], (NPOS, P_SIZE, P_SIZE), ((0, 64),), -0.2, 0.2)), 1.0, 30.0)
    scan_rows = set_ends(jax.random.randint(keys[3], (NPOS,), 0, H - P_SIZE + 1), jax.random.fold_in(keys[3], 1), 0, H - P_SIZE).astype(jnp.int32)
    scan_cols = set_ends(jax.random.randint(keys[4], (NPOS,), 0, TW), jax.random.fold_in(keys[4], 1), 0, TW - 1).astype(jnp.int32)
    counts = draw_counts(jax.random.fold_in(keys[9], 71), 0)
    dataset = set_ends(jax.random.randint(keys[6], (NPOS,), 0, DATASETS), jax.random.fold_in(keys[6], 1), 0, DATASETS - 1).astype(jnp.int32)
    dose_scale = jnp.clip(jnp.exp(jax.random.uniform(keys[7], (DATASETS,), jnp.float32, math.log(0.5), math.log(2.0))), 0.5, 2.0)
    background = jnp.clip(jnp.exp(jax.random.uniform(keys[8], (DATASETS,), jnp.float32, math.log(0.5), math.log(8.0))), 0.5, 8.0)
    return {"transmission": transmission, "probe_modes": probe_modes, "measured": measured, "scan_rows": scan_rows, "scan_cols": scan_cols, "counts": counts, "dataset": dataset, "dose_scale": dose_scale, "background": background}


def times_complex(first, second):
    first_re = first[..., 0, :, :]
    first_im = first[..., 1, :, :]
    second_re = second[..., 0, :, :]
    second_im = second[..., 1, :, :]
    return jnp.stack([first_re * second_re - first_im * second_im, first_re * second_im + first_im * second_re], axis=-3)

def times_conjugate(first, second):
    first_re = first[..., 0, :, :]
    first_im = first[..., 1, :, :]
    second_re = second[..., 0, :, :]
    second_im = second[..., 1, :, :]
    return jnp.stack([first_re * second_re + first_im * second_im, first_re * second_im - first_im * second_re], axis=-3)

def block_table(real_part, imag_part):
    upper = jnp.stack([real_part, -imag_part])
    lower = jnp.stack([imag_part, real_part])
    return jnp.stack([upper, lower]).astype(jnp.bfloat16)

def fresnel_tables(length):
    counter = jnp.arange(length, dtype=jnp.int32)
    product = counter[:, None] * counter[None, :] % length
    angles = 2.0 * math.pi / length * product.astype(jnp.float32)
    scaling = 1.0 / math.sqrt(length)
    dft_re = jnp.cos(angles) * scaling
    dft_im = -jnp.sin(angles) * scaling
    signed = jnp.where(counter < length // 2, counter, counter - length)
    phases = -math.pi / length * (signed * signed % (2 * length)).astype(jnp.float32)
    filter_re = jnp.cos(phases)[:, None]
    filter_im = jnp.sin(phases)[:, None]
    mixed_re = filter_re * dft_re - filter_im * dft_im
    mixed_im = filter_re * dft_im + filter_im * dft_re
    highest = lax.Precision.HIGHEST
    kernel_re = jnp.dot(dft_re, mixed_re, precision=highest) + jnp.dot(dft_im, mixed_im, precision=highest)
    kernel_im = jnp.dot(dft_re, mixed_im, precision=highest) - jnp.dot(dft_im, mixed_re, precision=highest)
    return (block_table(dft_re, dft_im), block_table(dft_re, -dft_im), block_table(kernel_re, kernel_im), block_table(kernel_re, -kernel_im))

def rounded_wave(values):
    return lax.optimization_barrier(values.astype(jnp.bfloat16)).astype(jnp.float32)

def apply_sides(table, waves):
    highest = lax.Precision.HIGHEST
    inner = jnp.einsum('cdij,bdjk->bcik', table.astype(jnp.float32), waves.astype(jnp.float32), precision=highest)
    inner = rounded_wave(inner)
    return jnp.einsum('bdij,cdjk->bcik', inner, table.astype(jnp.float32), precision=highest)

def reference(transmission, probe_modes, measured, scan_rows, scan_cols, counts, dataset, dose_scale, background):
    length = probe_modes.shape[-1]
    half_width = length // 2
    depth_count = transmission.shape[0]
    padded = jnp.pad(transmission, ((0, 0), (0, 0), (0, 0), (half_width, half_width)))
    dft_table, dft_adjoint, kernel_table, kernel_adjoint = fresnel_tables(length)
    zero = jnp.zeros((), jnp.int32)

    def visit(gradient, position):
        tile_index = position // POS_CAP
        slot_index = position - tile_index * POS_CAP
        row_start = scan_rows[position].astype(jnp.int32)
        col_start = (tile_index * TW + scan_cols[position]).astype(jnp.int32)

        def run(current):
            patches = lax.dynamic_slice(padded, (zero, zero, row_start, col_start), (depth_count, 2, length, length))
            waves = probe_modes.astype(jnp.float32)
            inputs = []
            far_field = waves
            for slice_index in range(depth_count):
                inputs.append(waves)
                applied = times_complex(waves, patches[slice_index][None]).astype(jnp.bfloat16)
                if slice_index < depth_count - 1:
                    waves = rounded_wave(apply_sides(kernel_table, applied))
                else:
                    far_field = apply_sides(dft_table, applied)
            scale = dose_scale[dataset[position]]
            offset = background[dataset[position]]
            intensity = scale * lax.optimization_barrier(jnp.sum(far_field * far_field, axis=(0, 1))) + offset
            factor = scale * (1.0 - jnp.sqrt(measured[position]) / jnp.sqrt(intensity))
            carried = (factor[None, None] * far_field).astype(jnp.bfloat16)
            for slice_index in reversed(range(depth_count)):
                adjoint = dft_adjoint if slice_index == depth_count - 1 else kernel_adjoint
                back_wave = apply_sides(adjoint, carried)
                term = lax.optimization_barrier(jnp.sum(times_conjugate(inputs[slice_index], back_wave), axis=0))
                place = (zero + slice_index, zero, row_start, col_start)
                present = lax.dynamic_slice(current, place, (1, 2, length, length))
                current = lax.dynamic_update_slice(current, present + term[None], place)
                if slice_index > 0:
                    carried = times_conjugate(patches[slice_index][None], back_wave).astype(jnp.bfloat16)
            return current
        updated = lax.cond(slot_index < counts[tile_index], run, lambda current: current, gradient)
        return (updated, None)
    start = jnp.zeros(padded.shape, jnp.float32)
    gradient, _ = lax.scan(visit, start, jnp.arange(N_TILE * POS_CAP, dtype=jnp.int32))
    return gradient[:, :, :, half_width:half_width + TW * N_TILE]
```

```python
import functools
import math

import jax
import jax.numpy as jnp
import numpy as np
from jax import lax
from jax.experimental import pallas as pl
from jax.experimental.pallas import tpu as pltpu
from jax.sharding import PartitionSpec as P

L = 256
Q = 128
MODES = 6
GROUP = 3
SLOTS = 2
ROWS = 1024
BF = jnp.bfloat16
F32 = jnp.float32
VMEM = pltpu.VMEM
SMEM = pltpu.SMEM


def rounded(values):
    return np.asarray(values, np.float32).astype(jnp.bfloat16).astype(np.float64)


def block(values):
    re, im = values.real, values.imag
    full = np.block([[re, -im], [im, re]])
    return np.stack([full, full.T])


@functools.cache
def tables():
    k = np.arange(L)
    dft = np.exp(-2j * np.pi / L * (k[:, None] * k[None, :] % L)) / math.sqrt(L)
    signed = np.where(k < Q, k, k - L)
    filt = np.exp(-1j * np.pi / L * (signed * signed % (2 * L)))
    prop = dft.conj() @ (filt[:, None] * dft)
    prop = rounded(prop.real) + 1j * rounded(prop.imag)
    dft = rounded(dft.real) + 1j * rounded(dft.imag)
    near, far = prop[:Q, :Q], prop[:Q, Q:]
    halves = [(near + far) / 2, (near - far) / 2]
    kinds = [[block(h) for h in halves], [block(dft[0::2, :Q]), block(dft[1::2, :Q])]]
    return np.stack([np.stack(kind) for kind in kinds]).astype(np.float32)


@functools.cache
def lane_split():
    k = np.arange(L)
    return (k[:, None] == np.where(k < Q, 2 * k, 2 * (k - Q) + 1)[None, :]).astype(np.float32)


def dot(a, b):
    return jnp.dot(a, b, preferred_element_type=F32)


def hadamard(q):
    s0, d0 = q[0][0] + q[0][1], q[0][0] - q[0][1]
    s1, d1 = q[1][0] + q[1][1], q[1][0] - q[1][1]
    return [[s0 + s1, d0 + d1], [s0 - s1, d0 - d1]]


def quads(fn):
    return [[fn(i, j) for j in range(2)] for i in range(2)]


CH = 16


def store_waves(z_ref, m, r, re, im):
    for i in range(2):
        for j in range(2):
            z_ref[m, i, r : r + CH, Q * j : Q * j + Q] = re[i][j].astype(BF)
            z_ref[m, i, Q + r : Q + r + CH, Q * j : Q * j + Q] = im[i][j].astype(BF)


def left_side(table, kind, back, z_ref, u_ref, m):
    for i in range(2):
        u = dot(table[kind, i, back], z_ref[m, i]).astype(BF)
        for j in range(2):
            u_ref[m, j, Q * i : Q * i + Q, 0:Q] = u[0:Q, Q * j : Q * j + Q]
            u_ref[m, j, Q * i : Q * i + Q, Q:L] = u[Q:L, Q * j : Q * j + Q]


def right_side(table, kind, back, u_ref, w_ref, m):
    for j in range(2):
        w_ref[m, j] = dot(u_ref[m, j], table[kind, j, 1 - back])


def read_waves(w_ref, m, r):
    re = quads(lambda i, j: w_ref[m, j, Q * i + r : Q * i + r + CH, 0:Q])
    im = quads(lambda i, j: w_ref[m, j, Q * i + r : Q * i + r + CH, Q:L])
    return re, im


def rotate_probe(probe, pr_ref, col):
    lane = lax.broadcasted_iota(jnp.int32, (32, Q), 1)
    wrapped = lane < col

    def one(m, _):
        for c in range(2):
            for r in range(0, L, 32):
                a = pltpu.roll(probe[m, c, r : r + 32, 0:Q], col, 1)
                b = pltpu.roll(probe[m, c, r : r + 32, Q:L], col, 1)
                pr_ref[m, c, r : r + 32, 0:Q] = jnp.where(wrapped, b, a)
                pr_ref[m, c, r : r + 32, Q:L] = jnp.where(wrapped, a, b)
        return 0

    lax.fori_loop(0, MODES, one, 0)


def load_patch(own, left, right, o_ref, tmp, place, row, col):
    lane = lax.broadcasted_iota(jnp.int32, (CH, Q), 1)
    base = pl.multiple_of(jnp.minimum(row // 16, (ROWS - L) // 16 - 1) * 16, 16)
    off = row - base
    for c in range(2):
        for r in range(0, L + 16, 16):
            a = left[c, pl.ds(base + r, 16), :].astype(F32)
            b = right[c, pl.ds(base + r, 16), :].astype(F32)
            tmp[c, r : r + 16, :] = jnp.where(lane < col, b, a)
        o_ref[place, c, :, Q:L] = own[c, pl.ds(row, L), :]
        o_ref[place, c, :, 0:Q] = tmp[c, pl.ds(off, L), :]


def amplitudes(measured, slot, split, amp_ref, tmp_ref):
    for j in range(2):
        tmp_ref[j] = jnp.sqrt(measured[slot, :, Q * j : Q * j + Q])
    for i in range(2):
        x = jnp.concatenate([tmp_ref[j, pl.ds(i, Q, stride=2), :] for j in range(2)], axis=1)
        hi = x.astype(BF)
        rest = x - hi.astype(F32)
        mid = rest.astype(BF)
        lo = (rest - mid.astype(F32)).astype(BF)
        amp_ref[i] = dot(hi, split[...]) + (dot(mid, split[...]) + dot(lo, split[...]))


def waves_forward(table, pr_ref, o_ref, p, z, u, w, psi_ref, far_ref, int_ref):
    int_ref[...] = jnp.zeros_like(int_ref)

    def group(g, _):
        for k in range(GROUP):
            m = g * GROUP + k
            for r in range(0, Q, CH):
                re, im = [[None] * 2 for _ in range(2)], [[None] * 2 for _ in range(2)]
                for i in range(2):
                    for j in range(2):
                        rows, lanes = slice(Q * i + r, Q * i + r + CH), slice(Q * j, Q * j + Q)
                        a, b = pr_ref[m, 0, rows, lanes], pr_ref[m, 1, rows, lanes]
                        c, d = o_ref[2 * p, 0, rows, lanes], o_ref[2 * p, 1, rows, lanes]
                        re[i][j], im[i][j] = a * c - b * d, a * d + b * c
                store_waves(z, k, r, hadamard(re), hadamard(im))
        for k in range(GROUP):
            left_side(table, 0, 0, z, u, k)
        for k in range(GROUP):
            right_side(table, 0, 0, u, w, k)
        for k in range(GROUP):
            m = g * GROUP + k
            for r in range(0, Q, CH):
                vre, vim = read_waves(w, k, r)
                vre, vim = hadamard(vre), hadamard(vim)
                re, im = [[None] * 2 for _ in range(2)], [[None] * 2 for _ in range(2)]
                for i in range(2):
                    for j in range(2):
                        rows, lanes = slice(Q * i + r, Q * i + r + CH), slice(Q * j, Q * j + Q)
                        a, b = vre[i][j], vim[i][j]
                        psi_ref[m, 0, rows, lanes] = a.astype(BF)
                        psi_ref[m, 1, rows, lanes] = b.astype(BF)
                        c, d = o_ref[2 * p + 1, 0, rows, lanes], o_ref[2 * p + 1, 1, rows, lanes]
                        re[i][j], im[i][j] = a * c - b * d, a * d + b * c
                store_waves(z, k, r, hadamard(re), hadamard(im))
        for k in range(GROUP):
            left_side(table, 1, 0, z, u, k)
        for k in range(GROUP):
            for j in range(2):
                far_ref[g * GROUP + k, j] = dot(u[k, j], table[1, j, 1])
        for j in range(2):
            for r in range(0, L, CH):
                total = int_ref[j, r : r + CH, :]
                for k in range(GROUP):
                    x = far_ref[g * GROUP + k, j, r : r + CH, 0:Q]
                    y = far_ref[g * GROUP + k, j, r : r + CH, Q:L]
                    total = total + (x * x + y * y)
                int_ref[j, r : r + CH, :] = total
        return 0

    lax.fori_loop(0, MODES // GROUP, group, 0)


def residual_factor(int_ref, amp_ref, fac_ref, scale, offset, valid):
    for j in range(2):
        for i in range(2):
            intensity = scale * int_ref[j, Q * i : Q * i + Q, :] + offset
            ratio = amp_ref[i, :, Q * j : Q * j + Q] / jnp.sqrt(intensity)
            fac_ref[j, Q * i : Q * i + Q, :] = jnp.where(valid, scale * (1.0 - ratio), 0.0)


def waves_backward(table, pr_ref, o_ref, p, z, u, w, psi_ref, far_ref, fac_ref, grad_ref):
    grad_ref[pl.ds(2 * p, 2)] = jnp.zeros((2, 2, L, L), F32)

    def conj_terms(place, r, terms):
        for i in range(2):
            for j in range(2):
                rows, lanes = slice(Q * i + r, Q * i + r + CH), slice(Q * j, Q * j + Q)
                gre, gim = grad_ref[place, 0, rows, lanes], grad_ref[place, 1, rows, lanes]
                for a, b, x, y in terms(i, j, rows, lanes):
                    gre = gre + (a * x + b * y)
                    gim = gim + (a * y - b * x)
                grad_ref[place, 0, rows, lanes] = gre
                grad_ref[place, 1, rows, lanes] = gim

    def group(g, _):
        for k in range(GROUP):
            m = g * GROUP + k
            for j in range(2):
                for r in range(0, L, CH):
                    f = fac_ref[j, r : r + CH, :]
                    i, s = r // Q, r % Q
                    z[k, i, s : s + CH, Q * j : Q * j + Q] = (f * far_ref[m, j, r : r + CH, 0:Q]).astype(BF)
                    z[k, i, Q + s : Q + s + CH, Q * j : Q * j + Q] = (
                        f * far_ref[m, j, r : r + CH, Q:L]
                    ).astype(BF)
        for k in range(GROUP):
            left_side(table, 1, 1, z, u, k)
        for k in range(GROUP):
            right_side(table, 1, 1, u, w, k)
        for k in range(GROUP):
            m = g * GROUP + k
            for r in range(0, Q, CH):
                vre, vim = read_waves(w, k, r)
                vre, vim = hadamard(vre), hadamard(vim)
                conj_terms(
                    2 * p + 1,
                    r,
                    lambda i, j, rows, lanes: [
                        (
                            psi_ref[m, 0, rows, lanes].astype(F32),
                            psi_ref[m, 1, rows, lanes].astype(F32),
                            vre[i][j],
                            vim[i][j],
                        )
                    ],
                )
                re, im = [[None] * 2 for _ in range(2)], [[None] * 2 for _ in range(2)]
                for i in range(2):
                    for j in range(2):
                        rows, lanes = slice(Q * i + r, Q * i + r + CH), slice(Q * j, Q * j + Q)
                        c, d = o_ref[2 * p + 1, 0, rows, lanes], o_ref[2 * p + 1, 1, rows, lanes]
                        x, y = vre[i][j], vim[i][j]
                        re[i][j], im[i][j] = c * x + d * y, c * y - d * x
                store_waves(z, k, r, hadamard(re), hadamard(im))
        for k in range(GROUP):
            left_side(table, 0, 1, z, u, k)
        for k in range(GROUP):
            right_side(table, 0, 1, u, w, k)
        for k in range(GROUP):
            m = g * GROUP + k
            for r in range(0, Q, CH):
                vre, vim = read_waves(w, k, r)
                vre, vim = hadamard(vre), hadamard(vim)
                conj_terms(
                    2 * p,
                    r,
                    lambda i, j, rows, lanes: [
                        (pr_ref[m, 0, rows, lanes], pr_ref[m, 1, rows, lanes], vre[i][j], vim[i][j])
                    ],
                )
        return 0

    lax.fori_loop(0, MODES // GROUP, group, 0)


def wave_kernel(
    rows, cols, counts, dataset, dose, ground,
    own0, left0, right0, own1, left1, right1, probe, measured, table, split,
    own_mine, own_theirs, halo_mine, halo_theirs,
    o_ref, pr_ref, psi_ref, far_ref, int_ref, fac_ref, amp_ref, z, u, w, grad_ref, tmp,
):
    depth = lax.axis_index("depth")

    def position(p, _):
        slot = depth * SLOTS + p
        row = jnp.clip(rows[slot], 0, ROWS - L)
        col = jnp.clip(cols[slot], 0, Q - 1)
        which = jnp.clip(dataset[slot], 0, dose.shape[0] - 1)
        load_patch(own0, left0, right0, o_ref, tmp, 2 * p + depth, row, col)
        load_patch(own1, left1, right1, o_ref, tmp, 2 * p + 1 - depth, row, col)
        rotate_probe(probe, pr_ref, col)
        amplitudes(measured, slot, split, amp_ref, int_ref)
        waves_forward(table, pr_ref, o_ref, p, z, u, w, psi_ref, far_ref, int_ref)
        residual_factor(int_ref, amp_ref, fac_ref, dose[which], ground[which], slot < counts[0])
        waves_backward(table, pr_ref, o_ref, p, z, u, w, psi_ref, far_ref, fac_ref, grad_ref)
        mine, theirs = 2 * p + depth, 2 * p + 1 - depth
        own_mine[p] = grad_ref[mine, :, :, Q:L]
        own_theirs[p] = grad_ref[theirs, :, :, Q:L].astype(BF)
        halo_mine[p] = grad_ref[mine, :, :, 0:Q].astype(BF)
        halo_theirs[p] = grad_ref[theirs, :, :, 0:Q].astype(BF)
        return 0

    lax.fori_loop(0, SLOTS, position, 0)


def waves(scalars, transmissions, probe, measured):
    part = jax.ShapeDtypeStruct((SLOTS, 2, L, Q), F32)
    short = jax.ShapeDtypeStruct((SLOTS, 2, L, Q), BF)
    vm = pl.BlockSpec(memory_space=VMEM)
    return pl.pallas_call(
        wave_kernel,
        out_shape=(part, short, short, short),
        in_specs=[pl.BlockSpec(memory_space=SMEM)] * 6 + [vm] * 10,
        out_specs=(vm,) * 4,
        scratch_shapes=[
            VMEM((4, 2, L, L), F32),
            VMEM((MODES, 2, L, L), F32),
            VMEM((MODES, 2, L, L), BF),
            VMEM((MODES, 2, L, L), F32),
            VMEM((2, L, Q), F32),
            VMEM((2, L, Q), F32),
            VMEM((2, Q, L), F32),
            VMEM((GROUP, 2, L, L), BF),
            VMEM((GROUP, 2, L, L), BF),
            VMEM((GROUP, 2, L, L), F32),
            VMEM((4, 2, L, L), F32),
            VMEM((2, L + 16, Q), F32),
        ],
        compiler_params=pltpu.CompilerParams(vmem_limit_bytes=60 * 2**20),
        name="waves",
    )(
        *scalars,
        *transmissions,
        probe,
        measured,
        jnp.asarray(tables()).astype(BF),
        jnp.asarray(lane_split()).astype(BF),
    )


def combine_kernel(
    rows, lrows, lcols, rrows, rcols, mine, theirs, ll0, ll1, rr0, rr1, out
):
    depth = lax.axis_index("depth")
    lane = lax.broadcasted_iota(jnp.int32, (L, Q), 1)
    out[...] = jnp.zeros_like(out)

    def add(row, values):
        row = jnp.clip(row, 0, ROWS - L)
        for c in range(2):
            out[c, pl.ds(row, L), :] += values(c)

    for p in range(SLOTS):
        add(rows[depth * SLOTS + p], lambda c: mine[p, c])
        add(rows[(1 - depth) * SLOTS + p], lambda c: theirs[p, c].astype(F32))
        for ref, core in ((ll0, depth), (ll1, 1 - depth)):
            slot = core * SLOTS + p
            add(lrows[slot], lambda c: jnp.where(lane < lcols[slot], ref[p, c].astype(F32), 0.0))
        for ref, core in ((rr0, depth), (rr1, 1 - depth)):
            slot = core * SLOTS + p
            add(rrows[slot], lambda c: jnp.where(lane < rcols[slot], 0.0, ref[p, c].astype(F32)))


def combine(scalars, parts):
    vm = pl.BlockSpec(memory_space=VMEM)
    return pl.pallas_call(
        combine_kernel,
        out_shape=jax.ShapeDtypeStruct((2, ROWS, Q), F32),
        in_specs=[pl.BlockSpec(memory_space=SMEM)] * 5 + [vm] * 6,
        out_specs=vm,
        compiler_params=pltpu.CompilerParams(vmem_limit_bytes=60 * 2**20),
        name="combine",
    )(*scalars, *parts)


def shards(transmission, probe_modes, measured, scan_rows, scan_cols, counts, dataset, dose_scale, background):
    tiles = lax.axis_size("tile")
    up = [(i, i + 1) for i in range(tiles - 1)]
    down = [(i + 1, i) for i in range(tiles - 1)]
    swap = [(0, 1), (1, 0)]
    up_cross = [(2 * i + c, 2 * (i + 1) + 1 - c) for i in range(tiles - 1) for c in range(2)]
    down_cross = [(2 * (i + 1) + c, 2 * i + 1 - c) for i in range(tiles - 1) for c in range(2)]
    own = transmission[0, :, :, :]
    short = own.astype(BF)
    left = lax.ppermute(short, "tile", up)
    right = lax.ppermute(short, "tile", down)
    own1 = lax.ppermute(own, "depth", swap)
    left1 = lax.ppermute(left, "depth", swap)
    right1 = lax.ppermute(right, "depth", swap)
    places = jnp.stack([scan_rows, scan_cols])
    lplaces = lax.ppermute(places, "tile", up)
    rplaces = lax.ppermute(places, "tile", down)
    own_mine, own_theirs, halo_mine, halo_theirs = waves(
        (scan_rows, scan_cols, counts, dataset, dose_scale, background),
        (own, left, right, own1, left1, right1),
        probe_modes,
        measured,
    )
    theirs = lax.ppermute(own_theirs, "depth", swap)
    ll0 = lax.ppermute(halo_mine, "tile", up)
    rr0 = lax.ppermute(halo_mine, "tile", down)
    ll1 = lax.ppermute(halo_theirs, ("tile", "depth"), up_cross)
    rr1 = lax.ppermute(halo_theirs, ("tile", "depth"), down_cross)
    out = combine(
        (scan_rows, lplaces[0], lplaces[1], rplaces[0], rplaces[1]),
        (own_mine, theirs, ll0, ll1, rr0, rr1),
    )
    return out[None]


def solution(mesh):
    in_specs = (
        P("depth", None, None, "tile"),
        P(),
        P("tile", None, None),
        P("tile"),
        P("tile"),
        P("tile"),
        P("tile"),
        P(),
        P(),
    )
    out_specs = P("depth", None, None, "tile")
    return jax.shard_map(shards, mesh=mesh, in_specs=in_specs, out_specs=out_specs, check_vma=False)
```

```python
import functools
import math

import jax
import jax.numpy as jnp
import numpy as np
from jax import lax
from jax.experimental import pallas as pl
from jax.experimental.pallas import tpu as pltpu
from jax.sharding import PartitionSpec as P

L = 256
Q = 128
MODES = 6
GROUP = 3
SLOTS = 2
ROWS = 1024
BF = jnp.bfloat16
F32 = jnp.float32
VMEM = pltpu.VMEM
SMEM = pltpu.SMEM


def rounded(values):
    return np.asarray(values, np.float32).astype(jnp.bfloat16).astype(np.float64)


def block(values):
    re, im = values.real, values.imag
    full = np.block([[re, -im], [im, re]])
    return np.stack([full, full.T])


@functools.cache
def tables():
    k = np.arange(L)
    dft = np.exp(-2j * np.pi / L * (k[:, None] * k[None, :] % L)) / math.sqrt(L)
    signed = np.where(k < Q, k, k - L)
    filt = np.exp(-1j * np.pi / L * (signed * signed % (2 * L)))
    prop = dft.conj() @ (filt[:, None] * dft)
    prop = rounded(prop.real) + 1j * rounded(prop.imag)
    dft = rounded(dft.real) + 1j * rounded(dft.imag)
    near, far = prop[:Q, :Q], prop[:Q, Q:]
    halves = [(near + far) / 2, (near - far) / 2]
    kinds = [[block(h) for h in halves], [block(dft[0::2, :Q]), block(dft[1::2, :Q])]]
    return np.stack([np.stack(kind) for kind in kinds]).astype(np.float32)


@functools.cache
def lane_split():
    k = np.arange(L)
    return (k[:, None] == np.where(k < Q, 2 * k, 2 * (k - Q) + 1)[None, :]).astype(np.float32)


def dot(a, b):
    return jnp.dot(a, b, preferred_element_type=F32)


def hadamard(q):
    s0, d0 = q[0][0] + q[0][1], q[0][0] - q[0][1]
    s1, d1 = q[1][0] + q[1][1], q[1][0] - q[1][1]
    return [[s0 + s1, d0 + d1], [s0 - s1, d0 - d1]]


def quads(fn):
    return [[fn(i, j) for j in range(2)] for i in range(2)]


CH = 16


def store_waves(z_ref, m, r, re, im):
    for i in range(2):
        for j in range(2):
            z_ref[m, i, r : r + CH, Q * j : Q * j + Q] = re[i][j].astype(BF)
            z_ref[m, i, Q + r : Q + r + CH, Q * j : Q * j + Q] = im[i][j].astype(BF)


def left_side(table, kind, back, z_ref, u_ref, m):
    for i in range(2):
        u = dot(table[kind, i, back], z_ref[m, i]).astype(BF)
        for j in range(2):
            u_ref[m, j, Q * i : Q * i + Q, 0:Q] = u[0:Q, Q * j : Q * j + Q]
            u_ref[m, j, Q * i : Q * i + Q, Q:L] = u[Q:L, Q * j : Q * j + Q]


def right_side(table, kind, back, u_ref, w_ref, m):
    for j in range(2):
        w_ref[m, j] = dot(u_ref[m, j], table[kind, j, 1 - back])


def read_waves(w_ref, m, r):
    re = quads(lambda i, j: w_ref[m, j, Q * i + r : Q * i + r + CH, 0:Q])
    im = quads(lambda i, j: w_ref[m, j, Q * i + r : Q * i + r + CH, Q:L])
    return re, im


def rotate_probe(probe, pr_ref, spin, p, col):
    shift = lax.broadcasted_iota(jnp.int32, (L, L), 1) - lax.broadcasted_iota(jnp.int32, (L, L), 0)
    spin[...] = jnp.where((shift == col) | (shift == col - L), 1.0, 0.0).astype(BF)

    def one(m, _):
        for c in range(2):
            x = probe[m, c]
            hi = x.astype(BF)
            lo = (x - hi.astype(F32)).astype(BF)
            pr_ref[p, m, c] = dot(hi, spin[...]) + dot(lo, spin[...])
        return 0

    lax.fori_loop(0, MODES, one, 0)


def widen(halo, wide):
    for side in range(2):
        for c in range(2):
            wide[side, c] = halo[side, c].astype(F32)


def load_patch(own, wide, o_ref, place, row, col, first, last):
    lane = lax.broadcasted_iota(jnp.int32, (L, Q), 1)
    right = lane < col
    empty = jnp.where(right, last, first) > 0
    for c in range(2):
        halo = jnp.where(right, wide[1, c, pl.ds(row, L), :], wide[0, c, pl.ds(row, L), :])
        o_ref[place, c, :, 0:Q] = jnp.where(empty, 0.0, halo)
        o_ref[place, c, :, Q:L] = own[c, pl.ds(row, L), :]


def amplitudes(measured, slot, split, amp_ref, tmp_ref):
    for j in range(2):
        tmp_ref[j] = jnp.sqrt(measured[slot, :, Q * j : Q * j + Q])
    for i in range(2):
        x = jnp.concatenate([tmp_ref[j, pl.ds(i, Q, stride=2), :] for j in range(2)], axis=1)
        hi = x.astype(BF)
        rest = x - hi.astype(F32)
        mid = rest.astype(BF)
        lo = (rest - mid.astype(F32)).astype(BF)
        amp_ref[i] = dot(hi, split[...]) + (dot(mid, split[...]) + dot(lo, split[...]))


def forward_first(table, pr_ref, o_ref, p, z, u, w, psi_ref):
    def group(g, _):
        for k in range(GROUP):
            m = g * GROUP + k
            for r in range(0, Q, CH):
                re, im = [[None] * 2 for _ in range(2)], [[None] * 2 for _ in range(2)]
                for i in range(2):
                    for j in range(2):
                        rows, lanes = slice(Q * i + r, Q * i + r + CH), slice(Q * j, Q * j + Q)
                        a, b = pr_ref[p, m, 0, rows, lanes], pr_ref[p, m, 1, rows, lanes]
                        c, d = o_ref[2 * p, 0, rows, lanes], o_ref[2 * p, 1, rows, lanes]
                        re[i][j], im[i][j] = a * c - b * d, a * d + b * c
                store_waves(z, k, r, hadamard(re), hadamard(im))
        for k in range(GROUP):
            left_side(table, 0, 0, z, u, k)
        for k in range(GROUP):
            right_side(table, 0, 0, u, w, k)
        for k in range(GROUP):
            m = g * GROUP + k
            for r in range(0, Q, CH):
                vre, vim = read_waves(w, k, r)
                vre, vim = hadamard(vre), hadamard(vim)
                for i in range(2):
                    for j in range(2):
                        rows, lanes = slice(Q * i + r, Q * i + r + CH), slice(Q * j, Q * j + Q)
                        psi_ref[p, m, 0, rows, lanes] = vre[i][j].astype(BF)
                        psi_ref[p, m, 1, rows, lanes] = vim[i][j].astype(BF)
        return 0

    lax.fori_loop(0, MODES // GROUP, group, 0)


def forward_last(table, o_ref, p, z, u, psi_ref, far_ref, int_ref):
    int_ref[...] = jnp.zeros_like(int_ref)

    def group(g, _):
        for k in range(GROUP):
            m = g * GROUP + k
            for r in range(0, Q, CH):
                re, im = [[None] * 2 for _ in range(2)], [[None] * 2 for _ in range(2)]
                for i in range(2):
                    for j in range(2):
                        rows, lanes = slice(Q * i + r, Q * i + r + CH), slice(Q * j, Q * j + Q)
                        a = psi_ref[p, m, 0, rows, lanes].astype(F32)
                        b = psi_ref[p, m, 1, rows, lanes].astype(F32)
                        c, d = o_ref[2 * p + 1, 0, rows, lanes], o_ref[2 * p + 1, 1, rows, lanes]
                        re[i][j], im[i][j] = a * c - b * d, a * d + b * c
                store_waves(z, k, r, hadamard(re), hadamard(im))
        for k in range(GROUP):
            left_side(table, 1, 0, z, u, k)
        for k in range(GROUP):
            for j in range(2):
                far_ref[g * GROUP + k, j] = dot(u[k, j], table[1, j, 1])
        for j in range(2):
            for r in range(0, L, CH):
                total = int_ref[j, r : r + CH, :]
                for k in range(GROUP):
                    x = far_ref[g * GROUP + k, j, r : r + CH, 0:Q]
                    y = far_ref[g * GROUP + k, j, r : r + CH, Q:L]
                    total = total + (x * x + y * y)
                int_ref[j, r : r + CH, :] = total
        return 0

    lax.fori_loop(0, MODES // GROUP, group, 0)


def residual_factor(int_ref, amp_ref, fac_ref, scale, offset, valid):
    for j in range(2):
        for i in range(2):
            intensity = scale * int_ref[j, Q * i : Q * i + Q, :] + offset
            ratio = amp_ref[i, :, Q * j : Q * j + Q] / jnp.sqrt(intensity)
            fac_ref[j, Q * i : Q * i + Q, :] = jnp.where(valid, scale * (1.0 - ratio), 0.0)


def conj_terms(grad_ref, place, r, terms):
    for i in range(2):
        for j in range(2):
            rows, lanes = slice(Q * i + r, Q * i + r + CH), slice(Q * j, Q * j + Q)
            gre, gim = grad_ref[place, 0, rows, lanes], grad_ref[place, 1, rows, lanes]
            a, b, x, y = terms(i, j, rows, lanes)
            grad_ref[place, 0, rows, lanes] = gre + (a * x + b * y)
            grad_ref[place, 1, rows, lanes] = gim + (a * y - b * x)


def backward_last(table, o_ref, p, z, u, w, psi_ref, far_ref, fac_ref, grad_ref, gz_ref):
    grad_ref[2 * p + 1] = jnp.zeros((2, L, L), F32)

    def group(g, _):
        for k in range(GROUP):
            m = g * GROUP + k
            for j in range(2):
                for r in range(0, L, CH):
                    f = fac_ref[j, r : r + CH, :]
                    i, s = r // Q, r % Q
                    z[k, i, s : s + CH, Q * j : Q * j + Q] = (f * far_ref[m, j, r : r + CH, 0:Q]).astype(BF)
                    z[k, i, Q + s : Q + s + CH, Q * j : Q * j + Q] = (
                        f * far_ref[m, j, r : r + CH, Q:L]
                    ).astype(BF)
        for k in range(GROUP):
            left_side(table, 1, 1, z, u, k)
        for k in range(GROUP):
            right_side(table, 1, 1, u, w, k)
        for k in range(GROUP):
            m = g * GROUP + k
            for r in range(0, Q, CH):
                vre, vim = read_waves(w, k, r)
                vre, vim = hadamard(vre), hadamard(vim)
                conj_terms(
                    grad_ref,
                    2 * p + 1,
                    r,
                    lambda i, j, rows, lanes: (
                        psi_ref[p, m, 0, rows, lanes].astype(F32),
                        psi_ref[p, m, 1, rows, lanes].astype(F32),
                        vre[i][j],
                        vim[i][j],
                    ),
                )
                re, im = [[None] * 2 for _ in range(2)], [[None] * 2 for _ in range(2)]
                for i in range(2):
                    for j in range(2):
                        rows, lanes = slice(Q * i + r, Q * i + r + CH), slice(Q * j, Q * j + Q)
                        c, d = o_ref[2 * p + 1, 0, rows, lanes], o_ref[2 * p + 1, 1, rows, lanes]
                        x, y = vre[i][j], vim[i][j]
                        re[i][j], im[i][j] = c * x + d * y, c * y - d * x
                store_waves(gz_ref, m, r, hadamard(re), hadamard(im))
        return 0

    lax.fori_loop(0, MODES // GROUP, group, 0)


def backward_first(table, pr_ref, p, u, w, grad_ref, gz_ref):
    grad_ref[2 * p] = jnp.zeros((2, L, L), F32)

    def group(g, _):
        for k in range(GROUP):
            m = g * GROUP + k
            for i in range(2):
                x = dot(table[0, i, 1], gz_ref[m, i]).astype(BF)
                for j in range(2):
                    u[k, j, Q * i : Q * i + Q, 0:Q] = x[0:Q, Q * j : Q * j + Q]
                    u[k, j, Q * i : Q * i + Q, Q:L] = x[Q:L, Q * j : Q * j + Q]
        for k in range(GROUP):
            right_side(table, 0, 1, u, w, k)
        for k in range(GROUP):
            m = g * GROUP + k
            for r in range(0, Q, CH):
                vre, vim = read_waves(w, k, r)
                vre, vim = hadamard(vre), hadamard(vim)
                conj_terms(
                    grad_ref,
                    2 * p,
                    r,
                    lambda i, j, rows, lanes: (
                        pr_ref[p, m, 0, rows, lanes],
                        pr_ref[p, m, 1, rows, lanes],
                        vre[i][j],
                        vim[i][j],
                    ),
                )
        return 0

    lax.fori_loop(0, MODES // GROUP, group, 0)


CHUNKS = 4
MESH = pl.DeviceIdType.MESH


def wave_kernel(
    rows, cols, counts, dataset, dose, ground,
    trans, probe_in, measured_in, table_in, split_in,
    own_mine, own_in, halo_in, places_in,
    own_a, own_b, halo_a, halo_b, short, places, own_out, halo_out,
    probe, measured, table, split, spin,
    o_ref, pr_ref, psi_ref, far_ref, int_ref, fac_ref, amp_ref, z, u, w, gz, grad_ref, wide,
    load_sem, own_send, own_recv, side_send, side_recv, relay_send, relay_recv,
    place_send, place_recv, grad_send, grad_recv, part_send, part_recv, go,
):
    depth = lax.axis_index("depth")
    tile = lax.axis_index("tile")
    tiles = lax.axis_size("tile")
    ahead, behind = lax.rem(tile + 1, tiles), lax.rem(tile + tiles - 1, tiles)
    other = 1 - depth
    beside = (ahead, behind)

    barrier = pltpu.get_barrier_semaphore()
    for target in ((ahead, depth), (behind, depth), (ahead, other), (behind, other), (tile, other)):
        pl.semaphore_signal(barrier, inc=1, device_id=target, device_id_type=MESH)

    def remote(src, dst, send, recv, target):
        return pltpu.make_async_remote_copy(
            src_ref=src, dst_ref=dst, send_sem=send, recv_sem=recv, device_id=target, device_id_type=MESH
        )

    loads = [
        pltpu.make_async_copy(probe_in, probe, load_sem.at[0]),
        pltpu.make_async_copy(measured_in.at[pl.ds(depth * SLOTS, SLOTS)], measured, load_sem.at[1]),
        pltpu.make_async_copy(table_in, table, load_sem.at[2]),
        pltpu.make_async_copy(split_in, split, load_sem.at[3]),
    ]

    def own_load(ref):
        return pltpu.make_async_copy(trans.at[0], ref, load_sem.at[4])

    def own_copy(ref):
        return remote(trans.at[0], ref, own_send, own_recv, (tile, other))

    def side_copy(ref, side, k):
        span = pl.ds(k * (ROWS // CHUNKS), ROWS // CHUNKS)
        return remote(
            short.at[:, span, :], ref.at[side, :, span, :], side_send.at[side, k], side_recv.at[side, k],
            (beside[side], depth),
        )

    def relay_copy(ref, side, k):
        span = pl.ds(k * (ROWS // CHUNKS), ROWS // CHUNKS)
        return remote(
            ref.at[side, :, span, :], ref.at[side, :, span, :], relay_send.at[side, k], relay_recv.at[side, k],
            (tile, other),
        )

    def place_copy(side):
        return remote(places, places_in.at[side], place_send.at[side], place_recv.at[side], (beside[side], depth))

    def grad_copy(p, home, side):
        target = depth if home == 0 else other
        return remote(
            halo_out.at[p, home], halo_in.at[side, depth, p], grad_send.at[p, home, side],
            grad_recv.at[side, depth, p], (beside[side], target),
        )

    def grad_arrival(p, core, side):
        return remote(
            halo_out.at[p, 0], halo_in.at[side, core, p], grad_send.at[p, 0, side], grad_recv.at[side, core, p],
            (beside[side], depth),
        )

    def part_copy(p):
        return remote(own_out.at[p], own_in.at[p], part_send.at[p], part_recv.at[p], (tile, other))

    mine = {0: (own_a, halo_a), 1: (own_b, halo_b)}
    for d in range(2):
        @pl.when(depth == d)
        def _():
            own_load(mine[d][0]).start()
    for load in loads:
        load.start()
    for n in range(4):
        places[n : n + 1, :] = jnp.full((1, Q), rows[n], jnp.int32)
        places[n + 4 : n + 5, :] = jnp.full((1, Q), cols[n], jnp.int32)
    for d in range(2):
        @pl.when(depth == d)
        def _():
            own_load(mine[d][0]).wait()
            for c in range(2):
                short[c] = mine[d][0][c].astype(BF)
    pl.semaphore_wait(barrier, 5)

    for d in range(2):
        @pl.when(depth == d)
        def _():
            own_copy(mine[d][0]).start()
    @pl.when(depth == 0)
    def _():
        for k in range(CHUNKS):
            for side in range(2):
                side_copy(halo_a, side, k).start()
    for side in range(2):
        place_copy(side).start()

    def spot(p):
        slot = depth * SLOTS + p
        return slot, jnp.clip(rows[slot], 0, ROWS - L), jnp.clip(cols[slot], 0, Q - 1)

    loads[0].wait()

    def turn(p, _):
        rotate_probe(probe, pr_ref, spin, p, spot(p)[2])
        return 0

    lax.fori_loop(0, SLOTS, turn, 0)
    for load in loads[1:]:
        load.wait()

    @pl.when(depth == 0)
    def _():
        for k in range(CHUNKS):
            for side in range(2):
                side_copy(halo_a, side, k).wait_recv()
                relay_copy(halo_a, side, k).start()
        for k in range(CHUNKS):
            for side in range(2):
                side_copy(halo_a, side, k).wait_send()
        pl.semaphore_signal(go, inc=1, device_id=(tile, other), device_id_type=MESH)
        own_copy(own_b).wait_recv()

    @pl.when(depth == 1)
    def _():
        pl.semaphore_wait(go, 1)
        for k in range(CHUNKS):
            for side in range(2):
                side_copy(halo_b, side, k).start()
        own_copy(own_a).wait_recv()
        for k in range(CHUNKS):
            for side in range(2):
                relay_copy(halo_a, side, k).wait_recv()
    own_copy(own_a).wait_send()
    widen(halo_a, wide)

    first = (tile == 0).astype(jnp.int32)
    last = (tile == tiles - 1).astype(jnp.int32)

    def start(p, _):
        _, row, col = spot(p)
        load_patch(own_a, wide, o_ref, 2 * p, row, col, first, last)
        forward_first(table, pr_ref, o_ref, p, z, u, w, psi_ref)

        @pl.when(depth == 1)
        def _():
            for kk in range(CHUNKS // SLOTS):
                for side in range(2):
                    k = p * (CHUNKS // SLOTS) + kk
                    side_copy(halo_b, side, k).wait_recv()
                    relay_copy(halo_b, side, k).start()
        return 0

    lax.fori_loop(0, SLOTS, start, 0)

    @pl.when(depth == 0)
    def _():
        for k in range(CHUNKS):
            for side in range(2):
                relay_copy(halo_b, side, k).wait_recv()
                relay_copy(halo_a, side, k).wait_send()

    @pl.when(depth == 1)
    def _():
        for k in range(CHUNKS):
            for side in range(2):
                side_copy(halo_b, side, k).wait_send()
                relay_copy(halo_b, side, k).wait_send()

    widen(halo_b, wide)

    def hand_over(p, s):
        place = 2 * p + s
        @pl.when(depth == s)
        def _():
            own_mine[p] = grad_ref[place, :, :, Q:L]
            halo_out[p, 0] = grad_ref[place, :, :, 0:Q].astype(BF)
            for side in range(2):
                grad_copy(p, 0, side).start()
        @pl.when(depth != s)
        def _():
            own_out[p] = grad_ref[place, :, :, Q:L].astype(BF)
            halo_out[p, 1] = grad_ref[place, :, :, 0:Q].astype(BF)
            for side in range(2):
                grad_copy(p, 1, side).start()
            part_copy(p).start()

    def finish(p, _):
        slot, row, col = spot(p)
        which = jnp.clip(dataset[slot], 0, dose.shape[0] - 1)
        load_patch(own_b, wide, o_ref, 2 * p + 1, row, col, first, last)
        amplitudes(measured, p, split, amp_ref, int_ref)
        forward_last(table, o_ref, p, z, u, psi_ref, far_ref, int_ref)
        residual_factor(int_ref, amp_ref, fac_ref, dose[which], ground[which], slot < counts[0])
        backward_last(table, o_ref, p, z, u, w, psi_ref, far_ref, fac_ref, grad_ref, gz)
        hand_over(p, 1)
        backward_first(table, pr_ref, p, u, w, grad_ref, gz)
        hand_over(p, 0)
        return 0

    lax.fori_loop(0, SLOTS, finish, 0)

    for side in range(2):
        place_copy(side).wait()
    for p in range(SLOTS):
        part_copy(p).wait()
        for side in range(2):
            for home in range(2):
                grad_copy(p, home, side).wait_send()
            for core in range(2):
                grad_arrival(p, core, side).wait_recv()


def waves(scalars, transmission, probe, measured):
    vm = pl.BlockSpec(memory_space=VMEM)
    hbm = pl.BlockSpec(memory_space=pltpu.HBM)
    dma = pltpu.SemaphoreType.DMA
    return pl.pallas_call(
        wave_kernel,
        out_shape=(
            jax.ShapeDtypeStruct((SLOTS, 2, L, Q), F32),
            jax.ShapeDtypeStruct((SLOTS, 2, L, Q), BF),
            jax.ShapeDtypeStruct((2, 2, SLOTS, 2, L, Q), BF),
            jax.ShapeDtypeStruct((2, 8, Q), jnp.int32),
        ),
        in_specs=[pl.BlockSpec(memory_space=SMEM)] * 6 + [hbm] * 5,
        out_specs=(vm,) * 4,
        scratch_shapes=[
            VMEM((2, ROWS, Q), F32),
            VMEM((2, ROWS, Q), F32),
            VMEM((2, 2, ROWS, Q), BF),
            VMEM((2, 2, ROWS, Q), BF),
            VMEM((2, ROWS, Q), BF),
            VMEM((8, Q), jnp.int32),
            VMEM((SLOTS, 2, L, Q), BF),
            VMEM((SLOTS, 2, 2, L, Q), BF),
            VMEM((MODES, 2, L, L), F32),
            VMEM((SLOTS, L, L), F32),
            VMEM((2, 2, 2, L, L), BF),
            VMEM((L, L), BF),
            VMEM((L, L), BF),
            VMEM((4, 2, L, L), F32),
            VMEM((SLOTS, MODES, 2, L, L), F32),
            VMEM((SLOTS, MODES, 2, L, L), BF),
            VMEM((MODES, 2, L, L), F32),
            VMEM((2, L, Q), F32),
            VMEM((2, L, Q), F32),
            VMEM((2, Q, L), F32),
            VMEM((GROUP, 2, L, L), BF),
            VMEM((GROUP, 2, L, L), BF),
            VMEM((GROUP, 2, L, L), F32),
            VMEM((MODES, 2, L, L), BF),
            VMEM((4, 2, L, L), F32),
            VMEM((2, 2, ROWS, Q), F32),
            dma((5,)),
            dma(()),
            dma(()),
            dma((2, CHUNKS)),
            dma((2, CHUNKS)),
            dma((2, CHUNKS)),
            dma((2, CHUNKS)),
            dma((2,)),
            dma((2,)),
            dma((SLOTS, 2, 2)),
            dma((2, 2, SLOTS)),
            dma((SLOTS,)),
            dma((SLOTS,)),
            pltpu.SemaphoreType.REGULAR,
        ],
        compiler_params=pltpu.CompilerParams(
            vmem_limit_bytes=60 * 2**20, collective_id=0, has_side_effects=True
        ),
        name="waves",
    )(
        *scalars,
        transmission,
        probe,
        measured,
        jnp.asarray(tables()).astype(BF),
        jnp.asarray(lane_split()).astype(BF),
    )


def combine_kernel(rows, places, mine, theirs, halo, out):
    depth = lax.axis_index("depth")
    tile = lax.axis_index("tile")
    lane = lax.broadcasted_iota(jnp.int32, (L, Q), 1)
    out[...] = jnp.zeros_like(out)

    def add(row, values):
        row = jnp.clip(row, 0, ROWS - L)
        for c in range(2):
            out[c, pl.ds(row, L), :] += values(c)

    for p in range(SLOTS):
        add(rows[depth * SLOTS + p], lambda c: mine[p, c])
        add(rows[(1 - depth) * SLOTS + p], lambda c: theirs[p, c].astype(F32))
        for core in range(2):
            slot = core * SLOTS + p

            @pl.when(tile > 0)
            def _():
                kept = lane < places[0, slot + 4, 0]
                add(places[0, slot, 0], lambda c: jnp.where(kept, halo[0, core, p, c].astype(F32), 0.0))

            @pl.when(tile < lax.axis_size("tile") - 1)
            def _():
                kept = lane >= places[1, slot + 4, 0]
                add(places[1, slot, 0], lambda c: jnp.where(kept, halo[1, core, p, c].astype(F32), 0.0))


def combine(rows, places, parts):
    vm = pl.BlockSpec(memory_space=VMEM)
    return pl.pallas_call(
        combine_kernel,
        out_shape=jax.ShapeDtypeStruct((2, ROWS, Q), F32),
        in_specs=[pl.BlockSpec(memory_space=SMEM)] * 2 + [vm] * 3,
        out_specs=vm,
        compiler_params=pltpu.CompilerParams(vmem_limit_bytes=60 * 2**20),
        name="combine",
    )(rows, places, *parts)


def shards(transmission, probe_modes, measured, scan_rows, scan_cols, counts, dataset, dose_scale, background):
    mine, theirs, halo, places = waves(
        (scan_rows, scan_cols, counts, dataset, dose_scale, background), transmission, probe_modes, measured
    )
    return combine(scan_rows, places, (mine, theirs, halo))[None]


def solution(mesh):
    in_specs = (
        P("depth", None, None, "tile"),
        P(),
        P("tile", None, None),
        P("tile"),
        P("tile"),
        P("tile"),
        P("tile"),
        P(),
        P(),
    )
    out_specs = P("depth", None, None, "tile")
    return jax.shard_map(shards, mesh=mesh, in_specs=in_specs, out_specs=out_specs, check_vma=False)
```

```python
import functools
import math

import jax
import jax.numpy as jnp
import numpy as np
from jax import lax
from jax.experimental import pallas as pl
from jax.experimental.pallas import tpu as pltpu
from jax.sharding import PartitionSpec as P

L = 256
Q = 128
MODES = 6
GROUP = 3
SLOTS = 2
ROWS = 1024
BF = jnp.bfloat16
F32 = jnp.float32
VMEM = pltpu.VMEM
SMEM = pltpu.SMEM


def rounded(values):
    return np.asarray(values, np.float32).astype(jnp.bfloat16).astype(np.float64)


def block(values):
    re, im = values.real, values.imag
    full = np.block([[re, -im], [im, re]])
    return np.stack([full, full.T])


@functools.cache
def tables():
    k = np.arange(L)
    dft = np.exp(-2j * np.pi / L * (k[:, None] * k[None, :] % L)) / math.sqrt(L)
    signed = np.where(k < Q, k, k - L)
    filt = np.exp(-1j * np.pi / L * (signed * signed % (2 * L)))
    prop = dft.conj() @ (filt[:, None] * dft)
    prop = rounded(prop.real) + 1j * rounded(prop.imag)
    dft = rounded(dft.real) + 1j * rounded(dft.imag)
    near, far = prop[:Q, :Q], prop[:Q, Q:]
    halves = [(near + far) / 2, (near - far) / 2]
    kinds = [[block(h) for h in halves], [block(dft[0::2, :Q]), block(dft[1::2, :Q])]]
    return np.stack([np.stack(kind) for kind in kinds]).astype(np.float32)


@functools.cache
def lane_split():
    k = np.arange(L)
    return (k[:, None] == np.where(k < Q, 2 * k, 2 * (k - Q) + 1)[None, :]).astype(np.float32)


def dot(a, b):
    return jnp.dot(a, b, preferred_element_type=F32)


def hadamard(q):
    s0, d0 = q[0][0] + q[0][1], q[0][0] - q[0][1]
    s1, d1 = q[1][0] + q[1][1], q[1][0] - q[1][1]
    return [[s0 + s1, d0 + d1], [s0 - s1, d0 - d1]]


def quads(fn):
    return [[fn(i, j) for j in range(2)] for i in range(2)]


CH = 16


def store_waves(z_ref, m, r, re, im):
    for i in range(2):
        for j in range(2):
            z_ref[m, i, r : r + CH, Q * j : Q * j + Q] = re[i][j].astype(BF)
            z_ref[m, i, Q + r : Q + r + CH, Q * j : Q * j + Q] = im[i][j].astype(BF)


def left_side(table, kind, back, z_ref, u_ref, m):
    for i in range(2):
        u = dot(table[kind, i, back], z_ref[m, i]).astype(BF)
        for j in range(2):
            u_ref[m, j, Q * i : Q * i + Q, 0:Q] = u[0:Q, Q * j : Q * j + Q]
            u_ref[m, j, Q * i : Q * i + Q, Q:L] = u[Q:L, Q * j : Q * j + Q]


def right_side(table, kind, back, u_ref, w_ref, m):
    for j in range(2):
        w_ref[m, j] = dot(u_ref[m, j], table[kind, j, 1 - back])


def read_waves(w_ref, m, r):
    re = quads(lambda i, j: w_ref[m, j, Q * i + r : Q * i + r + CH, 0:Q])
    im = quads(lambda i, j: w_ref[m, j, Q * i + r : Q * i + r + CH, Q:L])
    return re, im


def rotate_probe(probe, pr_ref, spin, p, col):
    shift = lax.broadcasted_iota(jnp.int32, (L, L), 1) - lax.broadcasted_iota(jnp.int32, (L, L), 0)
    spin[...] = jnp.where((shift == col) | (shift == col - L), 1.0, 0.0).astype(BF)

    def one(m, _):
        for c in range(2):
            x = probe[m, c]
            hi = x.astype(BF)
            lo = (x - hi.astype(F32)).astype(BF)
            pr_ref[p, m, c] = dot(hi, spin[...]) + dot(lo, spin[...])
        return 0

    lax.fori_loop(0, MODES, one, 0)


def widen(halo, wide, takes):
    for side in range(2):
        @pl.when(takes[side])
        def _():
            for c in range(2):
                wide[side, c] = halo[side, c].astype(F32)

        @pl.when(jnp.logical_not(takes[side]))
        def _():
            wide[side] = jnp.zeros((2, ROWS, Q), F32)


def load_patch(own, wide, o_ref, place, row, col):
    lane = lax.broadcasted_iota(jnp.int32, (L, Q), 1)
    right = lane < col
    for c in range(2):
        o_ref[place, c, :, 0:Q] = jnp.where(right, wide[1, c, pl.ds(row, L), :], wide[0, c, pl.ds(row, L), :])
        o_ref[place, c, :, Q:L] = own[c, pl.ds(row, L), :]


def amplitudes(measured, slot, split, amp_ref, tmp_ref):
    for j in range(2):
        tmp_ref[j] = jnp.sqrt(measured[slot, :, Q * j : Q * j + Q])
    for i in range(2):
        x = jnp.concatenate([tmp_ref[j, pl.ds(i, Q, stride=2), :] for j in range(2)], axis=1)
        hi = x.astype(BF)
        rest = x - hi.astype(F32)
        mid = rest.astype(BF)
        lo = (rest - mid.astype(F32)).astype(BF)
        amp_ref[i] = dot(hi, split[...]) + (dot(mid, split[...]) + dot(lo, split[...]))


def forward_first(table, pr_ref, o_ref, p, z, u, w, psi_ref):
    def group(g, _):
        for k in range(GROUP):
            m = g * GROUP + k
            for r in range(0, Q, CH):
                re, im = [[None] * 2 for _ in range(2)], [[None] * 2 for _ in range(2)]
                for i in range(2):
                    for j in range(2):
                        rows, lanes = slice(Q * i + r, Q * i + r + CH), slice(Q * j, Q * j + Q)
                        a, b = pr_ref[p, m, 0, rows, lanes], pr_ref[p, m, 1, rows, lanes]
                        c, d = o_ref[2 * p, 0, rows, lanes], o_ref[2 * p, 1, rows, lanes]
                        re[i][j], im[i][j] = a * c - b * d, a * d + b * c
                store_waves(z, k, r, hadamard(re), hadamard(im))
        for k in range(GROUP):
            left_side(table, 0, 0, z, u, k)
        for k in range(GROUP):
            right_side(table, 0, 0, u, w, k)
        for k in range(GROUP):
            m = g * GROUP + k
            for r in range(0, Q, CH):
                vre, vim = read_waves(w, k, r)
                vre, vim = hadamard(vre), hadamard(vim)
                for i in range(2):
                    for j in range(2):
                        rows, lanes = slice(Q * i + r, Q * i + r + CH), slice(Q * j, Q * j + Q)
                        psi_ref[p, m, 0, rows, lanes] = vre[i][j].astype(BF)
                        psi_ref[p, m, 1, rows, lanes] = vim[i][j].astype(BF)
        return 0

    lax.fori_loop(0, MODES // GROUP, group, 0)


def forward_last(table, o_ref, p, z, u, psi_ref, far_ref, int_ref):
    int_ref[...] = jnp.zeros_like(int_ref)

    def group(g, _):
        for k in range(GROUP):
            m = g * GROUP + k
            for r in range(0, Q, CH):
                re, im = [[None] * 2 for _ in range(2)], [[None] * 2 for _ in range(2)]
                for i in range(2):
                    for j in range(2):
                        rows, lanes = slice(Q * i + r, Q * i + r + CH), slice(Q * j, Q * j + Q)
                        a = psi_ref[p, m, 0, rows, lanes].astype(F32)
                        b = psi_ref[p, m, 1, rows, lanes].astype(F32)
                        c, d = o_ref[2 * p + 1, 0, rows, lanes], o_ref[2 * p + 1, 1, rows, lanes]
                        re[i][j], im[i][j] = a * c - b * d, a * d + b * c
                store_waves(z, k, r, hadamard(re), hadamard(im))
        for k in range(GROUP):
            left_side(table, 1, 0, z, u, k)
        for k in range(GROUP):
            for j in range(2):
                far_ref[g * GROUP + k, j] = dot(u[k, j], table[1, j, 1])
        for j in range(2):
            for r in range(0, L, CH):
                total = int_ref[j, r : r + CH, :]
                for k in range(GROUP):
                    x = far_ref[g * GROUP + k, j, r : r + CH, 0:Q]
                    y = far_ref[g * GROUP + k, j, r : r + CH, Q:L]
                    total = total + (x * x + y * y)
                int_ref[j, r : r + CH, :] = total
        return 0

    lax.fori_loop(0, MODES // GROUP, group, 0)


def residual_factor(int_ref, amp_ref, fac_ref, scale, offset, valid):
    for j in range(2):
        for i in range(2):
            intensity = scale * int_ref[j, Q * i : Q * i + Q, :] + offset
            ratio = amp_ref[i, :, Q * j : Q * j + Q] / jnp.sqrt(intensity)
            fac_ref[j, Q * i : Q * i + Q, :] = jnp.where(valid, scale * (1.0 - ratio), 0.0)


def conj_terms(grad_ref, place, r, terms):
    for i in range(2):
        for j in range(2):
            rows, lanes = slice(Q * i + r, Q * i + r + CH), slice(Q * j, Q * j + Q)
            gre, gim = grad_ref[place, 0, rows, lanes], grad_ref[place, 1, rows, lanes]
            a, b, x, y = terms(i, j, rows, lanes)
            grad_ref[place, 0, rows, lanes] = gre + (a * x + b * y)
            grad_ref[place, 1, rows, lanes] = gim + (a * y - b * x)


def backward_last(table, o_ref, p, z, u, w, psi_ref, far_ref, fac_ref, grad_ref, gz_ref):
    grad_ref[2 * p + 1] = jnp.zeros((2, L, L), F32)

    def group(g, _):
        for k in range(GROUP):
            m = g * GROUP + k
            for j in range(2):
                for r in range(0, L, CH):
                    f = fac_ref[j, r : r + CH, :]
                    i, s = r // Q, r % Q
                    z[k, i, s : s + CH, Q * j : Q * j + Q] = (f * far_ref[m, j, r : r + CH, 0:Q]).astype(BF)
                    z[k, i, Q + s : Q + s + CH, Q * j : Q * j + Q] = (
                        f * far_ref[m, j, r : r + CH, Q:L]
                    ).astype(BF)
        for k in range(GROUP):
            left_side(table, 1, 1, z, u, k)
        for k in range(GROUP):
            right_side(table, 1, 1, u, w, k)
        for k in range(GROUP):
            m = g * GROUP + k
            for r in range(0, Q, CH):
                vre, vim = read_waves(w, k, r)
                vre, vim = hadamard(vre), hadamard(vim)
                conj_terms(
                    grad_ref,
                    2 * p + 1,
                    r,
                    lambda i, j, rows, lanes: (
                        psi_ref[p, m, 0, rows, lanes].astype(F32),
                        psi_ref[p, m, 1, rows, lanes].astype(F32),
                        vre[i][j],
                        vim[i][j],
                    ),
                )
                re, im = [[None] * 2 for _ in range(2)], [[None] * 2 for _ in range(2)]
                for i in range(2):
                    for j in range(2):
                        rows, lanes = slice(Q * i + r, Q * i + r + CH), slice(Q * j, Q * j + Q)
                        c, d = o_ref[2 * p + 1, 0, rows, lanes], o_ref[2 * p + 1, 1, rows, lanes]
                        x, y = vre[i][j], vim[i][j]
                        re[i][j], im[i][j] = c * x + d * y, c * y - d * x
                store_waves(gz_ref, m, r, hadamard(re), hadamard(im))
        return 0

    lax.fori_loop(0, MODES // GROUP, group, 0)


def backward_first(table, pr_ref, p, u, w, grad_ref, gz_ref):
    grad_ref[2 * p] = jnp.zeros((2, L, L), F32)

    def group(g, _):
        for k in range(GROUP):
            m = g * GROUP + k
            for i in range(2):
                x = dot(table[0, i, 1], gz_ref[m, i]).astype(BF)
                for j in range(2):
                    u[k, j, Q * i : Q * i + Q, 0:Q] = x[0:Q, Q * j : Q * j + Q]
                    u[k, j, Q * i : Q * i + Q, Q:L] = x[Q:L, Q * j : Q * j + Q]
        for k in range(GROUP):
            right_side(table, 0, 1, u, w, k)
        for k in range(GROUP):
            m = g * GROUP + k
            for r in range(0, Q, CH):
                vre, vim = read_waves(w, k, r)
                vre, vim = hadamard(vre), hadamard(vim)
                conj_terms(
                    grad_ref,
                    2 * p,
                    r,
                    lambda i, j, rows, lanes: (
                        pr_ref[p, m, 0, rows, lanes],
                        pr_ref[p, m, 1, rows, lanes],
                        vre[i][j],
                        vim[i][j],
                    ),
                )
        return 0

    lax.fori_loop(0, MODES // GROUP, group, 0)


CHUNKS = 4
RELEASE = 2
MESH = pl.DeviceIdType.MESH


def wave_kernel(
    rows_in, cols_in, counts_in, dataset_in, dose_in, ground_in,
    trans, probe_in, measured_in, table_in, split_in,
    own_mine, own_in, halo_in, places_in,
    own_a, own_b, halo_a, halo_b, short, places, own_out, halo_out,
    probe, measured, table, split, spin,
    o_ref, pr_ref, psi_ref, far_ref, int_ref, fac_ref, amp_ref, z, u, w, gz, grad_ref, wide,
    load_sem, own_send, own_recv, side_send, side_recv, relay_send, relay_recv,
    place_send, place_recv, grad_send, grad_recv, part_send, part_recv, go,
    rows, cols, counts, dataset, dose, ground, small_sem,
):
    depth = lax.axis_index("depth")
    tile = lax.axis_index("tile")
    tiles = lax.axis_size("tile")
    ahead, behind = lax.rem(tile + 1, tiles), lax.rem(tile + tiles - 1, tiles)
    other = 1 - depth
    beside = (ahead, behind)

    upper, lower = tile < tiles - 1, tile > 0
    sends, takes = (upper, lower), (lower, upper)

    barrier = pltpu.get_barrier_semaphore()
    pl.semaphore_signal(barrier, inc=1, device_id=(tile, other), device_id_type=MESH)
    for side in range(2):
        @pl.when(sends[side])
        def _():
            for core in (depth, other):
                pl.semaphore_signal(barrier, inc=1, device_id=(beside[side], core), device_id_type=MESH)

    def remote(src, dst, send, recv, target):
        return pltpu.make_async_remote_copy(
            src_ref=src, dst_ref=dst, send_sem=send, recv_sem=recv, device_id=target, device_id_type=MESH
        )

    loads = [
        pltpu.make_async_copy(probe_in, probe, load_sem.at[0]),
        pltpu.make_async_copy(measured_in.at[pl.ds(depth * SLOTS, SLOTS)], measured, load_sem.at[1]),
        pltpu.make_async_copy(table_in, table, load_sem.at[2]),
        pltpu.make_async_copy(split_in, split, load_sem.at[3]),
    ]

    def own_load(ref):
        return pltpu.make_async_copy(trans.at[0], ref, load_sem.at[4])

    def own_copy(ref):
        return remote(trans.at[0], ref, own_send, own_recv, (tile, other))

    def side_copy(ref, side, k):
        span = pl.ds(k * (ROWS // CHUNKS), ROWS // CHUNKS)
        return remote(
            short.at[:, span, :], ref.at[side, :, span, :], side_send.at[side, k], side_recv.at[side, k],
            (beside[side], depth),
        )

    def relay_copy(ref, side, k):
        span = pl.ds(k * (ROWS // CHUNKS), ROWS // CHUNKS)
        return remote(
            ref.at[side, :, span, :], ref.at[side, :, span, :], relay_send.at[side, k], relay_recv.at[side, k],
            (tile, other),
        )

    def place_copy(side):
        return remote(places, places_in.at[side], place_send.at[side], place_recv.at[side], (beside[side], depth))

    def grad_copy(p, home, side):
        target = depth if home == 0 else other
        return remote(
            halo_out.at[p, home], halo_in.at[side, depth, p], grad_send.at[p, home, side],
            grad_recv.at[side, depth, p], (beside[side], target),
        )

    def grad_arrival(p, core, side):
        return remote(
            halo_out.at[p, 0], halo_in.at[side, core, p], grad_send.at[p, 0, side], grad_recv.at[side, core, p],
            (beside[side], depth),
        )

    def part_copy(p):
        return remote(own_out.at[p], own_in.at[p], part_send.at[p], part_recv.at[p], (tile, other))

    mine = {0: (own_a, halo_a), 1: (own_b, halo_b)}
    for d in range(2):
        @pl.when(depth == d)
        def _():
            own_load(mine[d][0]).start()
    smalls = [
        pltpu.make_async_copy(src, dst, small_sem.at[n])
        for n, (src, dst) in enumerate(
            (
                (rows_in, rows), (cols_in, cols), (counts_in, counts),
                (dataset_in, dataset), (dose_in, dose), (ground_in, ground),
            )
        )
    ]
    for load in smalls + loads:
        load.start()
    for d in range(2):
        @pl.when(depth == d)
        def _():
            own_load(mine[d][0]).wait()
            for c in range(2):
                short[c] = mine[d][0][c].astype(BF)
    pl.semaphore_wait(barrier, 1 + 2 * (lower.astype(jnp.int32) + upper.astype(jnp.int32)))

    def sides(flags, act):
        for side in range(2):
            @pl.when(flags[side])
            def _():
                act(side)

    def send_tiles(ref):
        for k in range(CHUNKS):
            sides(sends, lambda side: side_copy(ref, side, k).start())

    for d in range(2):
        @pl.when(depth == d)
        def _():
            own_copy(mine[d][0]).start()
    @pl.when(depth == 0)
    def _():
        send_tiles(halo_a)

    def spot(p):
        slot = depth * SLOTS + p
        return slot, jnp.clip(rows[slot], 0, ROWS - L), jnp.clip(cols[slot], 0, Q - 1)

    for load in smalls:
        load.wait()
    for n in range(4):
        places[n : n + 1, :] = jnp.full((1, Q), rows[n], jnp.int32)
        places[n + 4 : n + 5, :] = jnp.full((1, Q), cols[n], jnp.int32)
    loads[0].wait()

    def turn(p, _):
        rotate_probe(probe, pr_ref, spin, p, spot(p)[2])
        return 0

    lax.fori_loop(0, SLOTS, turn, 0)
    for load in loads[1:]:
        load.wait()

    def take(side, k, ref):
        side_copy(ref, side, k).wait_recv()
        relay_copy(ref, side, k).start()

    @pl.when(depth == 0)
    def _():
        for k in range(RELEASE):
            sides(sends, lambda side: side_copy(halo_a, side, k).wait_send())
        pl.semaphore_signal(go, inc=1, device_id=(tile, other), device_id_type=MESH)
        for k in range(CHUNKS):
            sides(takes, lambda side: take(side, k, halo_a))
        for k in range(RELEASE, CHUNKS):
            sides(sends, lambda side: side_copy(halo_a, side, k).wait_send())
        own_copy(own_b).wait_recv()

    @pl.when(depth == 1)
    def _():
        pl.semaphore_wait(go, 1)
        send_tiles(halo_b)
        own_copy(own_a).wait_recv()
        for k in range(CHUNKS):
            sides(takes, lambda side: relay_copy(halo_a, side, k).wait_recv())
    own_copy(own_a).wait_send()
    sides(sends, lambda side: place_copy(side).start())
    widen(halo_a, wide, takes)

    def start(p, _):
        _, row, col = spot(p)
        load_patch(own_a, wide, o_ref, 2 * p, row, col)
        forward_first(table, pr_ref, o_ref, p, z, u, w, psi_ref)

        @pl.when(depth == 1)
        def _():
            for kk in range(CHUNKS // SLOTS):
                sides(takes, lambda side: take(side, p * (CHUNKS // SLOTS) + kk, halo_b))
        return 0

    lax.fori_loop(0, SLOTS, start, 0)

    @pl.when(depth == 0)
    def _():
        for k in range(CHUNKS):
            sides(takes, lambda side: relay_copy(halo_b, side, k).wait_recv())
            sides(takes, lambda side: relay_copy(halo_a, side, k).wait_send())

    @pl.when(depth == 1)
    def _():
        for k in range(CHUNKS):
            sides(sends, lambda side: side_copy(halo_b, side, k).wait_send())
            sides(takes, lambda side: relay_copy(halo_b, side, k).wait_send())

    widen(halo_b, wide, takes)

    def hand_over(p, s):
        place = 2 * p + s
        @pl.when(depth == s)
        def _():
            own_mine[p] = grad_ref[place, :, :, Q:L]
            halo_out[p, 0] = grad_ref[place, :, :, 0:Q].astype(BF)
            sides(sends, lambda side: grad_copy(p, 0, side).start())
        @pl.when(depth != s)
        def _():
            own_out[p] = grad_ref[place, :, :, Q:L].astype(BF)
            halo_out[p, 1] = grad_ref[place, :, :, 0:Q].astype(BF)
            sides(sends, lambda side: grad_copy(p, 1, side).start())
            part_copy(p).start()

    def finish(p, _):
        slot, row, col = spot(p)
        which = jnp.clip(dataset[slot], 0, dose.shape[0] - 1)
        load_patch(own_b, wide, o_ref, 2 * p + 1, row, col)
        amplitudes(measured, p, split, amp_ref, int_ref)
        forward_last(table, o_ref, p, z, u, psi_ref, far_ref, int_ref)
        residual_factor(int_ref, amp_ref, fac_ref, dose[which], ground[which], slot < counts[0])
        backward_last(table, o_ref, p, z, u, w, psi_ref, far_ref, fac_ref, grad_ref, gz)
        hand_over(p, 1)
        backward_first(table, pr_ref, p, u, w, grad_ref, gz)
        hand_over(p, 0)
        return 0

    lax.fori_loop(0, SLOTS, finish, 0)

    sides(sends, lambda side: place_copy(side).wait_send())
    sides(takes, lambda side: place_copy(side).wait_recv())
    for p in range(SLOTS):
        part_copy(p).wait()
        for n in range(2):
            sides(sends, lambda side: grad_copy(p, n, side).wait_send())
            sides(takes, lambda side: grad_arrival(p, n, side).wait_recv())


def waves(scalars, transmission, probe, measured):
    vm = pl.BlockSpec(memory_space=VMEM)
    hbm = pl.BlockSpec(memory_space=pltpu.HBM)
    dma = pltpu.SemaphoreType.DMA
    return pl.pallas_call(
        wave_kernel,
        out_shape=(
            jax.ShapeDtypeStruct((SLOTS, 2, L, Q), F32),
            jax.ShapeDtypeStruct((SLOTS, 2, L, Q), BF),
            jax.ShapeDtypeStruct((2, 2, SLOTS, 2, L, Q), BF),
            jax.ShapeDtypeStruct((2, 8, Q), jnp.int32),
        ),
        in_specs=[hbm] * 11,
        out_specs=(vm,) * 4,
        scratch_shapes=[
            VMEM((2, ROWS, Q), F32),
            VMEM((2, ROWS, Q), F32),
            VMEM((2, 2, ROWS, Q), BF),
            VMEM((2, 2, ROWS, Q), BF),
            VMEM((2, ROWS, Q), BF),
            VMEM((8, Q), jnp.int32),
            VMEM((SLOTS, 2, L, Q), BF),
            VMEM((SLOTS, 2, 2, L, Q), BF),
            VMEM((MODES, 2, L, L), F32),
            VMEM((SLOTS, L, L), F32),
            VMEM((2, 2, 2, L, L), BF),
            VMEM((L, L), BF),
            VMEM((L, L), BF),
            VMEM((4, 2, L, L), F32),
            VMEM((SLOTS, MODES, 2, L, L), F32),
            VMEM((SLOTS, MODES, 2, L, L), BF),
            VMEM((MODES, 2, L, L), F32),
            VMEM((2, L, Q), F32),
            VMEM((2, L, Q), F32),
            VMEM((2, Q, L), F32),
            VMEM((GROUP, 2, L, L), BF),
            VMEM((GROUP, 2, L, L), BF),
            VMEM((GROUP, 2, L, L), F32),
            VMEM((MODES, 2, L, L), BF),
            VMEM((4, 2, L, L), F32),
            VMEM((2, 2, ROWS, Q), F32),
            dma((5,)),
            dma(()),
            dma(()),
            dma((2, CHUNKS)),
            dma((2, CHUNKS)),
            dma((2, CHUNKS)),
            dma((2, CHUNKS)),
            dma((2,)),
            dma((2,)),
            dma((SLOTS, 2, 2)),
            dma((2, 2, SLOTS)),
            dma((SLOTS,)),
            dma((SLOTS,)),
            pltpu.SemaphoreType.REGULAR,
            SMEM((4,), jnp.int32),
            SMEM((4,), jnp.int32),
            SMEM((1,), jnp.int32),
            SMEM((4,), jnp.int32),
            SMEM((16,), F32),
            SMEM((16,), F32),
            dma((6,)),
        ],
        compiler_params=pltpu.CompilerParams(
            vmem_limit_bytes=60 * 2**20, collective_id=0, has_side_effects=True
        ),
        name="waves",
    )(
        *scalars,
        transmission,
        probe,
        measured,
        jnp.asarray(tables()).astype(BF),
        jnp.asarray(lane_split()).astype(BF),
    )


def combine_kernel(rows, places, mine, theirs, halo, out):
    depth = lax.axis_index("depth")
    tile = lax.axis_index("tile")
    lane = lax.broadcasted_iota(jnp.int32, (L, Q), 1)
    out[...] = jnp.zeros_like(out)

    def add(row, values):
        row = jnp.clip(row, 0, ROWS - L)
        for c in range(2):
            out[c, pl.ds(row, L), :] += values(c)

    for p in range(SLOTS):
        add(rows[depth * SLOTS + p], lambda c: mine[p, c])
        add(rows[(1 - depth) * SLOTS + p], lambda c: theirs[p, c].astype(F32))
        for core in range(2):
            slot = core * SLOTS + p

            @pl.when(tile > 0)
            def _():
                kept = lane < places[0, slot + 4, 0]
                add(places[0, slot, 0], lambda c: jnp.where(kept, halo[0, core, p, c].astype(F32), 0.0))

            @pl.when(tile < lax.axis_size("tile") - 1)
            def _():
                kept = lane >= places[1, slot + 4, 0]
                add(places[1, slot, 0], lambda c: jnp.where(kept, halo[1, core, p, c].astype(F32), 0.0))


def combine(rows, places, parts):
    vm = pl.BlockSpec(memory_space=VMEM)
    return pl.pallas_call(
        combine_kernel,
        out_shape=jax.ShapeDtypeStruct((2, ROWS, Q), F32),
        in_specs=[pl.BlockSpec(memory_space=SMEM)] * 2 + [vm] * 3,
        out_specs=vm,
        compiler_params=pltpu.CompilerParams(vmem_limit_bytes=60 * 2**20),
        name="combine",
    )(rows, places, *parts)


def shards(transmission, probe_modes, measured, scan_rows, scan_cols, counts, dataset, dose_scale, background):
    mine, theirs, halo, places = waves(
        (scan_rows, scan_cols, counts, dataset, dose_scale, background), transmission, probe_modes, measured
    )
    return combine(scan_rows, places, (mine, theirs, halo))[None]


def solution(mesh):
    in_specs = (
        P("depth", None, None, "tile"),
        P(),
        P("tile", None, None),
        P("tile"),
        P("tile"),
        P("tile"),
        P("tile"),
        P(),
        P(),
    )
    out_specs = P("depth", None, None, "tile")
    return jax.shard_map(shards, mesh=mesh, in_specs=in_specs, out_specs=out_specs, check_vma=False)
```

```python
import functools
import math

import jax
import jax.numpy as jnp
import numpy as np
from jax import lax
from jax.experimental import pallas as pl
from jax.experimental.pallas import tpu as pltpu
from jax.sharding import PartitionSpec as P

L = 256
Q = 128
MODES = 6
GROUP = 6
SLOTS = 2
ROWS = 1024
BF = jnp.bfloat16
F32 = jnp.float32
VMEM = pltpu.VMEM
SMEM = pltpu.SMEM


def rounded(values):
    return np.asarray(values, np.float32).astype(jnp.bfloat16).astype(np.float64)


def block(values):
    re, im = values.real, values.imag
    full = np.block([[re, -im], [im, re]])
    return np.stack([full, full.T])


@functools.cache
def tables():
    k = np.arange(L)
    dft = np.exp(-2j * np.pi / L * (k[:, None] * k[None, :] % L)) / math.sqrt(L)
    signed = np.where(k < Q, k, k - L)
    filt = np.exp(-1j * np.pi / L * (signed * signed % (2 * L)))
    prop = dft.conj() @ (filt[:, None] * dft)
    prop = rounded(prop.real) + 1j * rounded(prop.imag)
    dft = rounded(dft.real) + 1j * rounded(dft.imag)
    near, far = prop[:Q, :Q], prop[:Q, Q:]
    halves = [(near + far) / 2, (near - far) / 2]
    kinds = [[block(h) for h in halves], [block(dft[0::2, :Q]), block(dft[1::2, :Q])]]
    return np.stack([np.stack(kind) for kind in kinds]).astype(np.float32)


@functools.cache
def lane_split():
    k = np.arange(L)
    return (k[:, None] == np.where(k < Q, 2 * k, 2 * (k - Q) + 1)[None, :]).astype(np.float32)


def dot(a, b):
    return jnp.dot(a, b, preferred_element_type=F32)


def hadamard(q):
    s0, d0 = q[0][0] + q[0][1], q[0][0] - q[0][1]
    s1, d1 = q[1][0] + q[1][1], q[1][0] - q[1][1]
    return [[s0 + s1, d0 + d1], [s0 - s1, d0 - d1]]


def quads(fn):
    return [[fn(i, j) for j in range(2)] for i in range(2)]


CH = 8


def store_waves(z_ref, m, r, re, im):
    for i in range(2):
        for j in range(2):
            z_ref[m, i, r : r + CH, Q * j : Q * j + Q] = re[i][j].astype(BF)
            z_ref[m, i, Q + r : Q + r + CH, Q * j : Q * j + Q] = im[i][j].astype(BF)


def left_side(table, kind, back, z_ref, u_ref, m):
    for i in range(2):
        u = dot(table[kind, i, back], z_ref[m, i]).astype(BF)
        for j in range(2):
            u_ref[m, j, Q * i : Q * i + Q, 0:Q] = u[0:Q, Q * j : Q * j + Q]
            u_ref[m, j, Q * i : Q * i + Q, Q:L] = u[Q:L, Q * j : Q * j + Q]


def right_side(table, kind, back, u_ref, w_ref, m):
    for j in range(2):
        w_ref[m, j] = dot(u_ref[m, j], table[kind, j, 1 - back])


def read_waves(w_ref, m, r):
    re = quads(lambda i, j: w_ref[m, j, Q * i + r : Q * i + r + CH, 0:Q])
    im = quads(lambda i, j: w_ref[m, j, Q * i + r : Q * i + r + CH, Q:L])
    return re, im


def rotate_probe(probe, pr_ref, spin, p, col):
    shift = lax.broadcasted_iota(jnp.int32, (L, L), 1) - lax.broadcasted_iota(jnp.int32, (L, L), 0)
    spin[...] = jnp.where((shift == col) | (shift == col - L), 1.0, 0.0).astype(BF)

    def one(m, _):
        for c in range(2):
            x = probe[m, c]
            hi = x.astype(BF)
            lo = (x - hi.astype(F32)).astype(BF)
            pr_ref[p, m, c] = dot(hi, spin[...]) + dot(lo, spin[...])
        return 0

    lax.fori_loop(0, MODES, one, 0)


def widen(halo, wide, takes):
    for side in range(2):
        @pl.when(takes[side])
        def _():
            for c in range(2):
                wide[side, c] = halo[side, c].astype(F32)

        @pl.when(jnp.logical_not(takes[side]))
        def _():
            wide[side] = jnp.zeros((2, ROWS, Q), F32)


def load_patch(own, wide, o_ref, place, row, col):
    lane = lax.broadcasted_iota(jnp.int32, (L, Q), 1)
    right = lane < col
    for c in range(2):
        o_ref[place, c, :, 0:Q] = jnp.where(right, wide[1, c, pl.ds(row, L), :], wide[0, c, pl.ds(row, L), :])
        o_ref[place, c, :, Q:L] = own[c, pl.ds(row, L), :]


def amplitudes(measured, slot, split, amp_ref, tmp_ref):
    for j in range(2):
        tmp_ref[j] = jnp.sqrt(measured[slot, :, Q * j : Q * j + Q])
    for i in range(2):
        x = jnp.concatenate([tmp_ref[j, pl.ds(i, Q, stride=2), :] for j in range(2)], axis=1)
        hi = x.astype(BF)
        rest = x - hi.astype(F32)
        mid = rest.astype(BF)
        lo = (rest - mid.astype(F32)).astype(BF)
        amp_ref[slot, i] = dot(hi, split[...]) + (dot(mid, split[...]) + dot(lo, split[...]))


def forward_first(table, pr_ref, o_ref, p, z, u, w, psi_ref):
    def group(g, _):
        for k in range(GROUP):
            m = g * GROUP + k
            for r in range(0, Q, CH):
                re, im = [[None] * 2 for _ in range(2)], [[None] * 2 for _ in range(2)]
                for i in range(2):
                    for j in range(2):
                        rows, lanes = slice(Q * i + r, Q * i + r + CH), slice(Q * j, Q * j + Q)
                        a, b = pr_ref[p, m, 0, rows, lanes], pr_ref[p, m, 1, rows, lanes]
                        c, d = o_ref[2 * p, 0, rows, lanes], o_ref[2 * p, 1, rows, lanes]
                        re[i][j], im[i][j] = a * c - b * d, a * d + b * c
                store_waves(z, k, r, hadamard(re), hadamard(im))
        for k in range(GROUP):
            left_side(table, 0, 0, z, u, k)
        for k in range(GROUP):
            right_side(table, 0, 0, u, w, k)
        for k in range(GROUP):
            m = g * GROUP + k
            for r in range(0, Q, CH):
                vre, vim = read_waves(w, k, r)
                vre, vim = hadamard(vre), hadamard(vim)
                for i in range(2):
                    for j in range(2):
                        rows, lanes = slice(Q * i + r, Q * i + r + CH), slice(Q * j, Q * j + Q)
                        psi_ref[p, m, 0, rows, lanes] = vre[i][j].astype(BF)
                        psi_ref[p, m, 1, rows, lanes] = vim[i][j].astype(BF)
        return 0

    group(0, 0)


def forward_last(table, o_ref, p, z, u, psi_ref, far_ref, int_ref):
    def group(g, _):
        for k in range(GROUP):
            m = g * GROUP + k
            for r in range(0, Q, CH):
                re, im = [[None] * 2 for _ in range(2)], [[None] * 2 for _ in range(2)]
                for i in range(2):
                    for j in range(2):
                        rows, lanes = slice(Q * i + r, Q * i + r + CH), slice(Q * j, Q * j + Q)
                        a = psi_ref[p, m, 0, rows, lanes].astype(F32)
                        b = psi_ref[p, m, 1, rows, lanes].astype(F32)
                        c, d = o_ref[2 * p + 1, 0, rows, lanes], o_ref[2 * p + 1, 1, rows, lanes]
                        re[i][j], im[i][j] = a * c - b * d, a * d + b * c
                store_waves(z, k, r, hadamard(re), hadamard(im))
        for k in range(GROUP):
            left_side(table, 1, 0, z, u, k)
        for k in range(GROUP):
            for j in range(2):
                far_ref[g * GROUP + k, j] = dot(u[k, j], table[1, j, 1])
        for j in range(2):
            for r in range(0, L, CH):
                total = None
                for k in range(GROUP):
                    x = far_ref[g * GROUP + k, j, r : r + CH, 0:Q]
                    y = far_ref[g * GROUP + k, j, r : r + CH, Q:L]
                    power = x * x + y * y
                    total = power if total is None else total + power
                int_ref[j, r : r + CH, :] = total
        return 0

    group(0, 0)


def residual_factor(int_ref, amp_ref, p, fac_ref, scale, offset, valid):
    for j in range(2):
        for i in range(2):
            intensity = scale * int_ref[j, Q * i : Q * i + Q, :] + offset
            ratio = amp_ref[p, i, :, Q * j : Q * j + Q] / jnp.sqrt(intensity)
            fac_ref[j, Q * i : Q * i + Q, :] = jnp.where(valid, scale * (1.0 - ratio), 0.0)


def cells(r):
    return [(i, j, slice(Q * i + r, Q * i + r + CH), slice(Q * j, Q * j + Q)) for i in range(2) for j in range(2)]


def add_conj(sums, n, a, b, x, y):
    gre, gim = a * x + b * y, a * y - b * x
    sums[n] = (gre, gim) if sums[n] is None else (sums[n][0] + gre, sums[n][1] + gim)


def store_sums(grad_ref, place, r, sums):
    for n, (i, j, rows, lanes) in enumerate(cells(r)):
        grad_ref[place, 0, rows, lanes], grad_ref[place, 1, rows, lanes] = sums[n]


def backward_last(table, o_ref, p, z, u, w, psi_ref, far_ref, fac_ref, grad_ref, gz_ref):
    def group(g, _):
        for k in range(GROUP):
            m = g * GROUP + k
            for j in range(2):
                for r in range(0, L, CH):
                    f = fac_ref[j, r : r + CH, :]
                    i, s = r // Q, r % Q
                    z[k, i, s : s + CH, Q * j : Q * j + Q] = (f * far_ref[m, j, r : r + CH, 0:Q]).astype(BF)
                    z[k, i, Q + s : Q + s + CH, Q * j : Q * j + Q] = (
                        f * far_ref[m, j, r : r + CH, Q:L]
                    ).astype(BF)
        for k in range(GROUP):
            left_side(table, 1, 1, z, u, k)
        for k in range(GROUP):
            right_side(table, 1, 1, u, w, k)
        for k in range(GROUP):
            m = g * GROUP + k
            for r in range(0, Q, CH):
                vre, vim = read_waves(w, k, r)
                vre, vim = hadamard(vre), hadamard(vim)
                re, im = [[None] * 2 for _ in range(2)], [[None] * 2 for _ in range(2)]
                for n, (i, j, rows, lanes) in enumerate(cells(r)):
                    x, y = vre[i][j], vim[i][j]
                    a, b = psi_ref[p, m, 0, rows, lanes].astype(F32), psi_ref[p, m, 1, rows, lanes].astype(F32)
                    gre, gim = a * x + b * y, a * y - b * x
                    if k > 0:
                        gre, gim = grad_ref.at[2 * p + 1][0, rows, lanes] + gre, grad_ref.at[2 * p + 1][1, rows, lanes] + gim
                    grad_ref.at[2 * p + 1][0, rows, lanes], grad_ref.at[2 * p + 1][1, rows, lanes] = gre, gim
                    c, d = o_ref[2 * p + 1, 0, rows, lanes], o_ref[2 * p + 1, 1, rows, lanes]
                    re[i][j], im[i][j] = c * x + d * y, c * y - d * x
                store_waves(gz_ref, m, r, hadamard(re), hadamard(im))
        return 0

    group(0, 0)


def backward_first(table, pr_ref, p, u, w, grad_ref, gz_ref):
    def group(g, _):
        for k in range(GROUP):
            m = g * GROUP + k
            for i in range(2):
                x = dot(table[0, i, 1], gz_ref[m, i]).astype(BF)
                for j in range(2):
                    u[k, j, Q * i : Q * i + Q, 0:Q] = x[0:Q, Q * j : Q * j + Q]
                    u[k, j, Q * i : Q * i + Q, Q:L] = x[Q:L, Q * j : Q * j + Q]
        for k in range(GROUP):
            right_side(table, 0, 1, u, w, k)
        for r in range(0, Q, CH):
            sums = [None] * 4
            for k in range(GROUP):
                m = g * GROUP + k
                vre, vim = read_waves(w, k, r)
                vre, vim = hadamard(vre), hadamard(vim)
                for n, (i, j, rows, lanes) in enumerate(cells(r)):
                    a, b = pr_ref[p, m, 0, rows, lanes], pr_ref[p, m, 1, rows, lanes]
                    add_conj(sums, n, a, b, vre[i][j], vim[i][j])
            store_sums(grad_ref, 2 * p, r, sums)
        return 0

    group(0, 0)


CHUNKS = 4
RELEASE = 2
MESH = pl.DeviceIdType.MESH


def wave_kernel(
    rows_in, cols_in, counts_in, dataset_in, dose_in, ground_in,
    trans, probe_in, measured_in, table_in, split_in,
    own_mine, own_in, halo_in, places_in,
    own_a, own_b, halo_a, halo_b, short, places, own_out, halo_out,
    probe, measured, table, split, spin,
    o_ref, pr_ref, psi_ref, far_ref, int_ref, fac_ref, amp_ref, z, u, w, gz, grad_ref, wide,
    load_sem, own_send, own_recv, side_send, side_recv, relay_send, relay_recv,
    place_send, place_recv, grad_send, grad_recv, part_send, part_recv, go,
    rows, cols, counts, dataset, dose, ground, small_sem,
):
    depth = lax.axis_index("depth")
    tile = lax.axis_index("tile")
    tiles = lax.axis_size("tile")
    ahead, behind = lax.rem(tile + 1, tiles), lax.rem(tile + tiles - 1, tiles)
    other = 1 - depth
    beside = (ahead, behind)

    upper, lower = tile < tiles - 1, tile > 0
    sends, takes = (upper, lower), (lower, upper)

    barrier = pltpu.get_barrier_semaphore()
    pl.semaphore_signal(barrier, inc=1, device_id=(tile, other), device_id_type=MESH)
    for side in range(2):
        @pl.when(sends[side])
        def _():
            for core in (depth, other):
                pl.semaphore_signal(barrier, inc=1, device_id=(beside[side], core), device_id_type=MESH)

    def remote(src, dst, send, recv, target):
        return pltpu.make_async_remote_copy(
            src_ref=src, dst_ref=dst, send_sem=send, recv_sem=recv, device_id=target, device_id_type=MESH
        )

    loads = [
        pltpu.make_async_copy(probe_in, probe, load_sem.at[0]),
        pltpu.make_async_copy(measured_in.at[pl.ds(depth * SLOTS, SLOTS)], measured, load_sem.at[1]),
        pltpu.make_async_copy(table_in, table, load_sem.at[2]),
        pltpu.make_async_copy(split_in, split, load_sem.at[3]),
    ]

    def own_load(ref):
        return pltpu.make_async_copy(trans.at[0], ref, load_sem.at[4])

    def own_copy(ref):
        return remote(trans.at[0], ref, own_send, own_recv, (tile, other))

    def side_copy(ref, side, k):
        span = pl.ds(k * (ROWS // CHUNKS), ROWS // CHUNKS)
        return remote(
            short.at[:, span, :], ref.at[side, :, span, :], side_send.at[side, k], side_recv.at[side, k],
            (beside[side], depth),
        )

    def relay_copy(ref, side, k):
        span = pl.ds(k * (ROWS // CHUNKS), ROWS // CHUNKS)
        return remote(
            ref.at[side, :, span, :], ref.at[side, :, span, :], relay_send.at[side, k], relay_recv.at[side, k],
            (tile, other),
        )

    def place_copy(side):
        return remote(places, places_in.at[side], place_send.at[side], place_recv.at[side], (beside[side], depth))

    def grad_copy(p, home, side):
        target = depth if home == 0 else other
        return remote(
            halo_out.at[p, home], halo_in.at[side, depth, p], grad_send.at[p, home, side],
            grad_recv.at[side, depth, p], (beside[side], target),
        )

    def grad_arrival(p, core, side):
        return remote(
            halo_out.at[p, 0], halo_in.at[side, core, p], grad_send.at[p, 0, side], grad_recv.at[side, core, p],
            (beside[side], depth),
        )

    def part_copy(p):
        return remote(own_out.at[p], own_in.at[p], part_send.at[p], part_recv.at[p], (tile, other))

    mine = {0: (own_a, halo_a), 1: (own_b, halo_b)}
    for d in range(2):
        @pl.when(depth == d)
        def _():
            own_load(mine[d][0]).start()
    smalls = [
        pltpu.make_async_copy(src, dst, small_sem.at[n])
        for n, (src, dst) in enumerate(
            (
                (rows_in, rows), (cols_in, cols), (counts_in, counts),
                (dataset_in, dataset), (dose_in, dose), (ground_in, ground),
            )
        )
    ]
    for load in smalls + loads:
        load.start()
    for d in range(2):
        @pl.when(depth == d)
        def _():
            own_load(mine[d][0]).wait()
            for c in range(2):
                short[c] = mine[d][0][c].astype(BF)
    pl.semaphore_wait(barrier, 1 + 2 * (lower.astype(jnp.int32) + upper.astype(jnp.int32)))

    def sides(flags, act):
        for side in range(2):
            @pl.when(flags[side])
            def _():
                act(side)

    def send_tiles(ref):
        for k in range(CHUNKS):
            sides(sends, lambda side: side_copy(ref, side, k).start())

    for d in range(2):
        @pl.when(depth == d)
        def _():
            own_copy(mine[d][0]).start()
    @pl.when(depth == 0)
    def _():
        send_tiles(halo_a)

    def spot(p):
        slot = depth * SLOTS + p
        return slot, jnp.clip(rows[slot], 0, ROWS - L), jnp.clip(cols[slot], 0, Q - 1)

    for load in smalls:
        load.wait()
    for n in range(4):
        places[n : n + 1, :] = jnp.full((1, Q), rows[n], jnp.int32)
        places[n + 4 : n + 5, :] = jnp.full((1, Q), cols[n], jnp.int32)
    for load in loads:
        load.wait()

    def turn(p, _):
        rotate_probe(probe, pr_ref, spin, p, spot(p)[2])
        amplitudes(measured, p, split, amp_ref, int_ref)
        return 0

    lax.fori_loop(0, SLOTS, turn, 0)

    def take(side, k, ref):
        side_copy(ref, side, k).wait_recv()
        relay_copy(ref, side, k).start()

    @pl.when(depth == 0)
    def _():
        for k in range(RELEASE):
            sides(sends, lambda side: side_copy(halo_a, side, k).wait_send())
        pl.semaphore_signal(go, inc=1, device_id=(tile, other), device_id_type=MESH)
        for k in range(CHUNKS):
            sides(takes, lambda side: take(side, k, halo_a))
        for k in range(RELEASE, CHUNKS):
            sides(sends, lambda side: side_copy(halo_a, side, k).wait_send())
        own_copy(own_b).wait_recv()

    @pl.when(depth == 1)
    def _():
        pl.semaphore_wait(go, 1)
        send_tiles(halo_b)
        own_copy(own_a).wait_recv()
        for k in range(CHUNKS):
            sides(takes, lambda side: relay_copy(halo_a, side, k).wait_recv())
    own_copy(own_a).wait_send()
    sides(sends, lambda side: place_copy(side).start())
    widen(halo_a, wide, takes)

    def start(p, _):
        _, row, col = spot(p)
        load_patch(own_a, wide, o_ref, 2 * p, row, col)
        forward_first(table, pr_ref, o_ref, p, z, u, w, psi_ref)

        @pl.when(depth == 1)
        def _():
            for kk in range(CHUNKS // SLOTS):
                sides(takes, lambda side: take(side, p * (CHUNKS // SLOTS) + kk, halo_b))
        return 0

    lax.fori_loop(0, SLOTS, start, 0)

    @pl.when(depth == 0)
    def _():
        for k in range(CHUNKS):
            sides(takes, lambda side: relay_copy(halo_b, side, k).wait_recv())
            sides(takes, lambda side: relay_copy(halo_a, side, k).wait_send())

    @pl.when(depth == 1)
    def _():
        for k in range(CHUNKS):
            sides(sends, lambda side: side_copy(halo_b, side, k).wait_send())
            sides(takes, lambda side: relay_copy(halo_b, side, k).wait_send())

    widen(halo_b, wide, takes)

    def hand_over(p, s):
        place = 2 * p + s
        @pl.when(depth == s)
        def _():
            own_mine[p] = grad_ref[place, :, :, Q:L]
            halo_out[p, 0] = grad_ref[place, :, :, 0:Q].astype(BF)
            sides(sends, lambda side: grad_copy(p, 0, side).start())
        @pl.when(depth != s)
        def _():
            own_out[p] = grad_ref[place, :, :, Q:L].astype(BF)
            halo_out[p, 1] = grad_ref[place, :, :, 0:Q].astype(BF)
            sides(sends, lambda side: grad_copy(p, 1, side).start())
            part_copy(p).start()

    def finish(p, _):
        slot, row, col = spot(p)
        which = jnp.clip(dataset[slot], 0, dose.shape[0] - 1)
        load_patch(own_b, wide, o_ref, 2 * p + 1, row, col)
        forward_last(table, o_ref, p, z, u, psi_ref, far_ref, int_ref)
        residual_factor(int_ref, amp_ref, p, fac_ref, dose[which], ground[which], slot < counts[0])
        backward_last(table, o_ref, p, z, u, w, psi_ref, far_ref, fac_ref, grad_ref, gz)
        hand_over(p, 1)
        backward_first(table, pr_ref, p, u, w, grad_ref, gz)
        hand_over(p, 0)
        return 0

    lax.fori_loop(0, SLOTS, finish, 0)

    sides(sends, lambda side: place_copy(side).wait_send())
    sides(takes, lambda side: place_copy(side).wait_recv())
    for p in range(SLOTS):
        part_copy(p).wait()
        for n in range(2):
            sides(sends, lambda side: grad_copy(p, n, side).wait_send())
            sides(takes, lambda side: grad_arrival(p, n, side).wait_recv())


def waves(scalars, transmission, probe, measured):
    vm = pl.BlockSpec(memory_space=VMEM)
    hbm = pl.BlockSpec(memory_space=pltpu.HBM)
    dma = pltpu.SemaphoreType.DMA
    return pl.pallas_call(
        wave_kernel,
        out_shape=(
            jax.ShapeDtypeStruct((SLOTS, 2, L, Q), F32),
            jax.ShapeDtypeStruct((SLOTS, 2, L, Q), BF),
            jax.ShapeDtypeStruct((2, 2, SLOTS, 2, L, Q), BF),
            jax.ShapeDtypeStruct((2, 8, Q), jnp.int32),
        ),
        in_specs=[hbm] * 11,
        out_specs=(vm,) * 4,
        scratch_shapes=[
            VMEM((2, ROWS, Q), F32),
            VMEM((2, ROWS, Q), F32),
            VMEM((2, 2, ROWS, Q), BF),
            VMEM((2, 2, ROWS, Q), BF),
            VMEM((2, ROWS, Q), BF),
            VMEM((8, Q), jnp.int32),
            VMEM((SLOTS, 2, L, Q), BF),
            VMEM((SLOTS, 2, 2, L, Q), BF),
            VMEM((MODES, 2, L, L), F32),
            VMEM((SLOTS, L, L), F32),
            VMEM((2, 2, 2, L, L), BF),
            VMEM((L, L), BF),
            VMEM((L, L), BF),
            VMEM((4, 2, L, L), F32),
            VMEM((SLOTS, MODES, 2, L, L), F32),
            VMEM((SLOTS, MODES, 2, L, L), BF),
            VMEM((MODES, 2, L, L), F32),
            VMEM((2, L, Q), F32),
            VMEM((2, L, Q), F32),
            VMEM((SLOTS, 2, Q, L), F32),
            VMEM((GROUP, 2, L, L), BF),
            VMEM((GROUP, 2, L, L), BF),
            VMEM((GROUP, 2, L, L), F32),
            VMEM((MODES, 2, L, L), BF),
            VMEM((4, 2, L, L), F32),
            VMEM((2, 2, ROWS, Q), F32),
            dma((5,)),
            dma(()),
            dma(()),
            dma((2, CHUNKS)),
            dma((2, CHUNKS)),
            dma((2, CHUNKS)),
            dma((2, CHUNKS)),
            dma((2,)),
            dma((2,)),
            dma((SLOTS, 2, 2)),
            dma((2, 2, SLOTS)),
            dma((SLOTS,)),
            dma((SLOTS,)),
            pltpu.SemaphoreType.REGULAR,
            SMEM((4,), jnp.int32),
            SMEM((4,), jnp.int32),
            SMEM((1,), jnp.int32),
            SMEM((4,), jnp.int32),
            SMEM((16,), F32),
            SMEM((16,), F32),
            dma((6,)),
        ],
        compiler_params=pltpu.CompilerParams(
            vmem_limit_bytes=60 * 2**20, collective_id=0, has_side_effects=True
        ),
        name="waves",
    )(
        *scalars,
        transmission,
        probe,
        measured,
        jnp.asarray(tables()).astype(BF),
        jnp.asarray(lane_split()).astype(BF),
    )


def combine_kernel(rows, places, mine, theirs, halo, out):
    depth = lax.axis_index("depth")
    tile = lax.axis_index("tile")
    lane = lax.broadcasted_iota(jnp.int32, (L, Q), 1)
    out[...] = jnp.zeros_like(out)

    def add(row, values):
        row = jnp.clip(row, 0, ROWS - L)
        for c in range(2):
            out[c, pl.ds(row, L), :] += values(c)

    for p in range(SLOTS):
        add(rows[depth * SLOTS + p], lambda c: mine[p, c])
        add(rows[(1 - depth) * SLOTS + p], lambda c: theirs[p, c].astype(F32))
        for core in range(2):
            slot = core * SLOTS + p

            @pl.when(tile > 0)
            def _():
                kept = lane < places[0, slot + 4, 0]
                add(places[0, slot, 0], lambda c: jnp.where(kept, halo[0, core, p, c].astype(F32), 0.0))

            @pl.when(tile < lax.axis_size("tile") - 1)
            def _():
                kept = lane >= places[1, slot + 4, 0]
                add(places[1, slot, 0], lambda c: jnp.where(kept, halo[1, core, p, c].astype(F32), 0.0))


def combine(rows, places, parts):
    vm = pl.BlockSpec(memory_space=VMEM)
    return pl.pallas_call(
        combine_kernel,
        out_shape=jax.ShapeDtypeStruct((2, ROWS, Q), F32),
        in_specs=[pl.BlockSpec(memory_space=SMEM)] * 2 + [vm] * 3,
        out_specs=vm,
        compiler_params=pltpu.CompilerParams(vmem_limit_bytes=60 * 2**20),
        name="combine",
    )(rows, places, *parts)


def shards(transmission, probe_modes, measured, scan_rows, scan_cols, counts, dataset, dose_scale, background):
    mine, theirs, halo, places = waves(
        (scan_rows, scan_cols, counts, dataset, dose_scale, background), transmission, probe_modes, measured
    )
    return combine(scan_rows, places, (mine, theirs, halo))[None]


def solution(mesh):
    in_specs = (
        P("depth", None, None, "tile"),
        P(),
        P("tile", None, None),
        P("tile"),
        P("tile"),
        P("tile"),
        P("tile"),
        P(),
        P(),
    )
    out_specs = P("depth", None, None, "tile")
    return jax.shard_map(shards, mesh=mesh, in_specs=in_specs, out_specs=out_specs, check_vma=False)
```

```python
import functools
import math

import jax
import jax.numpy as jnp
import numpy as np
from jax import lax
from jax.experimental import pallas as pl
from jax.experimental.pallas import tpu as pltpu
from jax.sharding import PartitionSpec as P

L = 256
Q = 128
MODES = 6
GROUP = 6
SLOTS = 2
ROWS = 1024
BF = jnp.bfloat16
F32 = jnp.float32
VMEM = pltpu.VMEM
SMEM = pltpu.SMEM


def rounded(values):
    return np.asarray(values, np.float32).astype(jnp.bfloat16).astype(np.float64)


def block(values):
    re, im = values.real, values.imag
    full = np.block([[re, -im], [im, re]])
    return np.stack([full, full.T])


@functools.cache
def tables():
    k = np.arange(L)
    dft = np.exp(-2j * np.pi / L * (k[:, None] * k[None, :] % L)) / math.sqrt(L)
    signed = np.where(k < Q, k, k - L)
    filt = np.exp(-1j * np.pi / L * (signed * signed % (2 * L)))
    prop = dft.conj() @ (filt[:, None] * dft)
    prop = rounded(prop.real) + 1j * rounded(prop.imag)
    dft = rounded(dft.real) + 1j * rounded(dft.imag)
    near, far = prop[:Q, :Q], prop[:Q, Q:]
    halves = [(near + far) / 2, (near - far) / 2]
    kinds = [[block(h) for h in halves], [block(dft[0::2, :Q]), block(dft[1::2, :Q])]]
    return np.stack([np.stack(kind) for kind in kinds]).astype(np.float32)


@functools.cache
def lane_split():
    k = np.arange(L)
    return (k[:, None] == np.where(k < Q, 2 * k, 2 * (k - Q) + 1)[None, :]).astype(np.float32)


def dot(a, b):
    return jnp.dot(a, b, preferred_element_type=F32)


def hadamard(q):
    s0, d0 = q[0][0] + q[0][1], q[0][0] - q[0][1]
    s1, d1 = q[1][0] + q[1][1], q[1][0] - q[1][1]
    return [[s0 + s1, d0 + d1], [s0 - s1, d0 - d1]]


def quads(fn):
    return [[fn(i, j) for j in range(2)] for i in range(2)]


CH = 8


def store_waves(z_ref, m, r, re, im):
    for i in range(2):
        for j in range(2):
            z_ref[m, i, r : r + CH, Q * j : Q * j + Q] = re[i][j].astype(BF)
            z_ref[m, i, Q + r : Q + r + CH, Q * j : Q * j + Q] = im[i][j].astype(BF)


def left_side(table, kind, back, z_ref, u_ref, m):
    for i in range(2):
        u = dot(table[kind, i, back], z_ref[m, i]).astype(BF)
        for j in range(2):
            u_ref[m, j, Q * i : Q * i + Q, 0:Q] = u[0:Q, Q * j : Q * j + Q]
            u_ref[m, j, Q * i : Q * i + Q, Q:L] = u[Q:L, Q * j : Q * j + Q]


def right_side(table, kind, back, u_ref, w_ref, m):
    for j in range(2):
        w_ref[m, j] = dot(u_ref[m, j], table[kind, j, 1 - back])


def read_waves(w_ref, m, r):
    re = quads(lambda i, j: w_ref[m, j, Q * i + r : Q * i + r + CH, 0:Q])
    im = quads(lambda i, j: w_ref[m, j, Q * i + r : Q * i + r + CH, Q:L])
    return re, im


def rotate_probe(probe, pr_ref, spin, p, col):
    shift = lax.broadcasted_iota(jnp.int32, (L, L), 1) - lax.broadcasted_iota(jnp.int32, (L, L), 0)
    spin[...] = jnp.where((shift == col) | (shift == col - L), 1.0, 0.0).astype(BF)

    def one(m, _):
        for c in range(2):
            x = probe[m, c]
            hi = x.astype(BF)
            lo = (x - hi.astype(F32)).astype(BF)
            pr_ref[p, m, c] = dot(hi, spin[...]) + dot(lo, spin[...])
        return 0

    lax.fori_loop(0, MODES, one, 0)


def widen(halo, wide, takes):
    for side in range(2):
        @pl.when(takes[side])
        def _():
            for c in range(2):
                wide[side, c] = halo[side, c].astype(F32)

        @pl.when(jnp.logical_not(takes[side]))
        def _():
            wide[side] = jnp.zeros((2, ROWS, Q), F32)


def load_patch(own, wide, o_ref, place, row, col):
    lane = lax.broadcasted_iota(jnp.int32, (L, Q), 1)
    right = lane < col
    for c in range(2):
        o_ref[place, c, :, 0:Q] = jnp.where(right, wide[1, c, pl.ds(row, L), :], wide[0, c, pl.ds(row, L), :])
        o_ref[place, c, :, Q:L] = own[c, pl.ds(row, L), :]


def amplitudes(measured, slot, split, amp_ref, tmp_ref):
    for j in range(2):
        tmp_ref[j] = jnp.sqrt(measured[slot, :, Q * j : Q * j + Q])
    for i in range(2):
        x = jnp.concatenate([tmp_ref[j, pl.ds(i, Q, stride=2), :] for j in range(2)], axis=1)
        hi = x.astype(BF)
        rest = x - hi.astype(F32)
        mid = rest.astype(BF)
        lo = (rest - mid.astype(F32)).astype(BF)
        amp_ref[slot, i] = dot(hi, split[...]) + (dot(mid, split[...]) + dot(lo, split[...]))


def forward_first(table, pr_ref, o_ref, p, z, u, w, psi_ref):
    def group(g, _):
        for k in range(GROUP):
            m = g * GROUP + k
            for r in range(0, Q, CH):
                re, im = [[None] * 2 for _ in range(2)], [[None] * 2 for _ in range(2)]
                for i in range(2):
                    for j in range(2):
                        rows, lanes = slice(Q * i + r, Q * i + r + CH), slice(Q * j, Q * j + Q)
                        a, b = pr_ref[p, m, 0, rows, lanes], pr_ref[p, m, 1, rows, lanes]
                        c, d = o_ref[2 * p, 0, rows, lanes], o_ref[2 * p, 1, rows, lanes]
                        re[i][j], im[i][j] = a * c - b * d, a * d + b * c
                store_waves(z, k, r, hadamard(re), hadamard(im))
        for k in range(GROUP):
            left_side(table, 0, 0, z, u, k)
        for k in range(GROUP):
            right_side(table, 0, 0, u, w, k)
        for k in range(GROUP):
            m = g * GROUP + k
            for r in range(0, Q, CH):
                vre, vim = read_waves(w, k, r)
                vre, vim = hadamard(vre), hadamard(vim)
                for i in range(2):
                    for j in range(2):
                        rows, lanes = slice(Q * i + r, Q * i + r + CH), slice(Q * j, Q * j + Q)
                        psi_ref[p, m, 0, rows, lanes] = vre[i][j]
                        psi_ref[p, m, 1, rows, lanes] = vim[i][j]
        return 0

    group(0, 0)


def forward_last(table, o_ref, p, z, u, psi_ref, far_ref, int_ref):
    def group(g, _):
        for k in range(GROUP):
            m = g * GROUP + k
            for r in range(0, Q, CH):
                re, im = [[None] * 2 for _ in range(2)], [[None] * 2 for _ in range(2)]
                for i in range(2):
                    for j in range(2):
                        rows, lanes = slice(Q * i + r, Q * i + r + CH), slice(Q * j, Q * j + Q)
                        a = psi_ref[p, m, 0, rows, lanes]
                        b = psi_ref[p, m, 1, rows, lanes]
                        c, d = o_ref[2 * p + 1, 0, rows, lanes], o_ref[2 * p + 1, 1, rows, lanes]
                        re[i][j], im[i][j] = a * c - b * d, a * d + b * c
                store_waves(z, k, r, hadamard(re), hadamard(im))
        for k in range(GROUP):
            left_side(table, 1, 0, z, u, k)
        for k in range(GROUP):
            for j in range(2):
                far_ref[g * GROUP + k, j] = dot(u[k, j], table[1, j, 1])
        for j in range(2):
            for r in range(0, L, CH):
                total = None
                for k in range(GROUP):
                    x = far_ref[g * GROUP + k, j, r : r + CH, 0:Q]
                    y = far_ref[g * GROUP + k, j, r : r + CH, Q:L]
                    power = x * x + y * y
                    total = power if total is None else total + power
                int_ref[j, r : r + CH, :] = total
        return 0

    group(0, 0)


def residual_factor(int_ref, amp_ref, p, fac_ref, scale, offset, valid):
    for j in range(2):
        for i in range(2):
            intensity = scale * int_ref[j, Q * i : Q * i + Q, :] + offset
            ratio = amp_ref[p, i, :, Q * j : Q * j + Q] / jnp.sqrt(intensity)
            fac_ref[j, Q * i : Q * i + Q, :] = jnp.where(valid, scale * (1.0 - ratio), 0.0)


def cells(r):
    return [(i, j, slice(Q * i + r, Q * i + r + CH), slice(Q * j, Q * j + Q)) for i in range(2) for j in range(2)]


def add_conj(sums, n, a, b, x, y):
    gre, gim = a * x + b * y, a * y - b * x
    sums[n] = (gre, gim) if sums[n] is None else (sums[n][0] + gre, sums[n][1] + gim)


def store_sums(grad_ref, place, r, sums):
    for n, (i, j, rows, lanes) in enumerate(cells(r)):
        grad_ref[place, 0, rows, lanes], grad_ref[place, 1, rows, lanes] = sums[n]


def backward_last(table, o_ref, p, z, u, w, psi_ref, far_ref, fac_ref, grad_ref, gz_ref):
    def group(g, _):
        for k in range(GROUP):
            m = g * GROUP + k
            for j in range(2):
                for r in range(0, L, CH):
                    f = fac_ref[j, r : r + CH, :]
                    i, s = r // Q, r % Q
                    z[k, i, s : s + CH, Q * j : Q * j + Q] = (f * far_ref[m, j, r : r + CH, 0:Q]).astype(BF)
                    z[k, i, Q + s : Q + s + CH, Q * j : Q * j + Q] = (
                        f * far_ref[m, j, r : r + CH, Q:L]
                    ).astype(BF)
        for k in range(GROUP):
            left_side(table, 1, 1, z, u, k)
        for k in range(GROUP):
            right_side(table, 1, 1, u, w, k)
        for k in range(GROUP):
            m = g * GROUP + k
            for r in range(0, Q, CH):
                vre, vim = read_waves(w, k, r)
                vre, vim = hadamard(vre), hadamard(vim)
                re, im = [[None] * 2 for _ in range(2)], [[None] * 2 for _ in range(2)]
                for n, (i, j, rows, lanes) in enumerate(cells(r)):
                    x, y = vre[i][j], vim[i][j]
                    a, b = psi_ref[p, m, 0, rows, lanes], psi_ref[p, m, 1, rows, lanes]
                    gre, gim = a * x + b * y, a * y - b * x
                    if k > 0:
                        gre, gim = grad_ref.at[2 * p + 1][0, rows, lanes] + gre, grad_ref.at[2 * p + 1][1, rows, lanes] + gim
                    grad_ref.at[2 * p + 1][0, rows, lanes], grad_ref.at[2 * p + 1][1, rows, lanes] = gre, gim
                    c, d = o_ref[2 * p + 1, 0, rows, lanes], o_ref[2 * p + 1, 1, rows, lanes]
                    re[i][j], im[i][j] = c * x + d * y, c * y - d * x
                store_waves(gz_ref, m, r, hadamard(re), hadamard(im))
        return 0

    group(0, 0)


def backward_first(table, pr_ref, p, u, w, grad_ref, gz_ref):
    def group(g, _):
        for k in range(GROUP):
            m = g * GROUP + k
            for i in range(2):
                x = dot(table[0, i, 1], gz_ref[m, i]).astype(BF)
                for j in range(2):
                    u[k, j, Q * i : Q * i + Q, 0:Q] = x[0:Q, Q * j : Q * j + Q]
                    u[k, j, Q * i : Q * i + Q, Q:L] = x[Q:L, Q * j : Q * j + Q]
        for k in range(GROUP):
            right_side(table, 0, 1, u, w, k)
        for r in range(0, Q, CH):
            sums = [None] * 4
            for k in range(GROUP):
                m = g * GROUP + k
                vre, vim = read_waves(w, k, r)
                vre, vim = hadamard(vre), hadamard(vim)
                for n, (i, j, rows, lanes) in enumerate(cells(r)):
                    a, b = pr_ref[p, m, 0, rows, lanes], pr_ref[p, m, 1, rows, lanes]
                    add_conj(sums, n, a, b, vre[i][j], vim[i][j])
            store_sums(grad_ref, 2 * p, r, sums)
        return 0

    group(0, 0)


CHUNKS = 4
RELEASE = 3
MESH = pl.DeviceIdType.MESH


def wave_kernel(
    rows_in, cols_in, counts_in, dataset_in, dose_in, ground_in,
    trans, probe_in, measured_in, table_in, split_in,
    own_mine, own_in, halo_in, places_in,
    own_a, own_b, halo_a, halo_b, short, places, own_out, halo_out,
    probe, measured, table, split, spin,
    o_ref, pr_ref, psi_ref, far_ref, int_ref, fac_ref, amp_ref, z, u, w, gz, grad_ref, wide,
    load_sem, own_send, own_recv, side_send, side_recv, relay_send, relay_recv,
    place_send, place_recv, grad_send, grad_recv, part_send, part_recv, go,
    rows, cols, counts, dataset, dose, ground, small_sem,
):
    depth = lax.axis_index("depth")
    tile = lax.axis_index("tile")
    tiles = lax.axis_size("tile")
    ahead, behind = lax.rem(tile + 1, tiles), lax.rem(tile + tiles - 1, tiles)
    other = 1 - depth
    beside = (ahead, behind)

    upper, lower = tile < tiles - 1, tile > 0
    sends, takes = (upper, lower), (lower, upper)

    barrier = pltpu.get_barrier_semaphore()
    pl.semaphore_signal(barrier, inc=1, device_id=(tile, other), device_id_type=MESH)
    for side in range(2):
        @pl.when(sends[side])
        def _():
            for core in (depth, other):
                pl.semaphore_signal(barrier, inc=1, device_id=(beside[side], core), device_id_type=MESH)

    def remote(src, dst, send, recv, target):
        return pltpu.make_async_remote_copy(
            src_ref=src, dst_ref=dst, send_sem=send, recv_sem=recv, device_id=target, device_id_type=MESH
        )

    loads = [
        pltpu.make_async_copy(probe_in, probe, load_sem.at[0]),
        pltpu.make_async_copy(measured_in.at[pl.ds(depth * SLOTS, SLOTS)], measured, load_sem.at[1]),
        pltpu.make_async_copy(table_in, table, load_sem.at[2]),
        pltpu.make_async_copy(split_in, split, load_sem.at[3]),
    ]

    def own_load(ref):
        return pltpu.make_async_copy(trans.at[0], ref, load_sem.at[4])

    def own_copy(ref):
        return remote(trans.at[0], ref, own_send, own_recv, (tile, other))

    def side_copy(ref, side, k):
        span = pl.ds(k * (ROWS // CHUNKS), ROWS // CHUNKS)
        return remote(
            short.at[:, span, :], ref.at[side, :, span, :], side_send.at[side, k], side_recv.at[side, k],
            (beside[side], depth),
        )

    def relay_copy(ref, side, k):
        span = pl.ds(k * (ROWS // CHUNKS), ROWS // CHUNKS)
        return remote(
            ref.at[side, :, span, :], ref.at[side, :, span, :], relay_send.at[side, k], relay_recv.at[side, k],
            (tile, other),
        )

    def place_copy(side):
        return remote(places, places_in.at[side], place_send.at[side], place_recv.at[side], (beside[side], depth))

    def grad_copy(p, home, side):
        target = depth if home == 0 else other
        return remote(
            halo_out.at[p, home], halo_in.at[side, depth, p], grad_send.at[p, home, side],
            grad_recv.at[side, depth, p], (beside[side], target),
        )

    def grad_arrival(p, core, side):
        return remote(
            halo_out.at[p, 0], halo_in.at[side, core, p], grad_send.at[p, 0, side], grad_recv.at[side, core, p],
            (beside[side], depth),
        )

    def part_copy(p):
        return remote(own_out.at[p], own_in.at[p], part_send.at[p], part_recv.at[p], (tile, other))

    mine = {0: (own_a, halo_a), 1: (own_b, halo_b)}
    for d in range(2):
        @pl.when(depth == d)
        def _():
            own_load(mine[d][0]).start()
    smalls = [
        pltpu.make_async_copy(src, dst, small_sem.at[n])
        for n, (src, dst) in enumerate(
            (
                (rows_in, rows), (cols_in, cols), (counts_in, counts),
                (dataset_in, dataset), (dose_in, dose), (ground_in, ground),
            )
        )
    ]
    for load in smalls + loads:
        load.start()
    for d in range(2):
        @pl.when(depth == d)
        def _():
            own_load(mine[d][0]).wait()
            for c in range(2):
                short[c] = mine[d][0][c].astype(BF)
    pl.semaphore_wait(barrier, 1 + 2 * (lower.astype(jnp.int32) + upper.astype(jnp.int32)))

    def sides(flags, act):
        for side in range(2):
            @pl.when(flags[side])
            def _():
                act(side)

    def send_tiles(ref):
        for k in range(CHUNKS):
            sides(sends, lambda side: side_copy(ref, side, k).start())

    for d in range(2):
        @pl.when(depth == d)
        def _():
            own_copy(mine[d][0]).start()
    @pl.when(depth == 0)
    def _():
        send_tiles(halo_a)

    def spot(p):
        slot = depth * SLOTS + p
        return slot, jnp.clip(rows[slot], 0, ROWS - L), jnp.clip(cols[slot], 0, Q - 1)

    for load in smalls:
        load.wait()
    for n in range(4):
        places[n : n + 1, :] = jnp.full((1, Q), rows[n], jnp.int32)
        places[n + 4 : n + 5, :] = jnp.full((1, Q), cols[n], jnp.int32)
    for load in loads:
        load.wait()

    def turn(p, _):
        rotate_probe(probe, pr_ref, spin, p, spot(p)[2])
        amplitudes(measured, p, split, amp_ref, int_ref)
        return 0

    lax.fori_loop(0, SLOTS, turn, 0)

    def take(side, k, ref):
        side_copy(ref, side, k).wait_recv()
        relay_copy(ref, side, k).start()

    @pl.when(depth == 0)
    def _():
        for k in range(RELEASE):
            sides(sends, lambda side: side_copy(halo_a, side, k).wait_send())
        pl.semaphore_signal(go, inc=1, device_id=(tile, other), device_id_type=MESH)
        for k in range(CHUNKS):
            sides(takes, lambda side: take(side, k, halo_a))
        for k in range(RELEASE, CHUNKS):
            sides(sends, lambda side: side_copy(halo_a, side, k).wait_send())
        own_copy(own_b).wait_recv()

    @pl.when(depth == 1)
    def _():
        pl.semaphore_wait(go, 1)
        send_tiles(halo_b)
        own_copy(own_a).wait_recv()
        for k in range(CHUNKS):
            sides(takes, lambda side: relay_copy(halo_a, side, k).wait_recv())
    own_copy(own_a).wait_send()
    sides(sends, lambda side: place_copy(side).start())
    widen(halo_a, wide, takes)

    def start(p, _):
        _, row, col = spot(p)
        load_patch(own_a, wide, o_ref, 2 * p, row, col)
        forward_first(table, pr_ref, o_ref, p, z, u, w, psi_ref)

        @pl.when(depth == 1)
        def _():
            for kk in range(CHUNKS // SLOTS):
                sides(takes, lambda side: take(side, p * (CHUNKS // SLOTS) + kk, halo_b))
        return 0

    lax.fori_loop(0, SLOTS, start, 0)

    @pl.when(depth == 0)
    def _():
        for k in range(CHUNKS):
            sides(takes, lambda side: relay_copy(halo_b, side, k).wait_recv())
            sides(takes, lambda side: relay_copy(halo_a, side, k).wait_send())

    @pl.when(depth == 1)
    def _():
        for k in range(CHUNKS):
            sides(sends, lambda side: side_copy(halo_b, side, k).wait_send())
            sides(takes, lambda side: relay_copy(halo_b, side, k).wait_send())

    widen(halo_b, wide, takes)

    def hand_over(p, s):
        place = 2 * p + s
        @pl.when(depth == s)
        def _():
            halo_out[p, 0] = grad_ref[place, :, :, 0:Q].astype(BF)
            sides(sends, lambda side: grad_copy(p, 0, side).start())
            own_mine[p] = grad_ref[place, :, :, Q:L]
        @pl.when(depth != s)
        def _():
            halo_out[p, 1] = grad_ref[place, :, :, 0:Q].astype(BF)
            sides(sends, lambda side: grad_copy(p, 1, side).start())
            own_out[p] = grad_ref[place, :, :, Q:L].astype(BF)
            part_copy(p).start()

    def finish(p, _):
        slot, row, col = spot(p)
        which = jnp.clip(dataset[slot], 0, dose.shape[0] - 1)
        load_patch(own_b, wide, o_ref, 2 * p + 1, row, col)
        forward_last(table, o_ref, p, z, u, psi_ref, far_ref, int_ref)
        residual_factor(int_ref, amp_ref, p, fac_ref, dose[which], ground[which], slot < counts[0])
        backward_last(table, o_ref, p, z, u, w, psi_ref, far_ref, fac_ref, grad_ref, gz)
        hand_over(p, 1)
        backward_first(table, pr_ref, p, u, w, grad_ref, gz)
        hand_over(p, 0)
        return 0

    lax.fori_loop(0, SLOTS, finish, 0)

    sides(sends, lambda side: place_copy(side).wait_send())
    sides(takes, lambda side: place_copy(side).wait_recv())
    for p in range(SLOTS):
        part_copy(p).wait()
        for n in range(2):
            sides(sends, lambda side: grad_copy(p, n, side).wait_send())
            sides(takes, lambda side: grad_arrival(p, n, side).wait_recv())


def waves(scalars, transmission, probe, measured):
    vm = pl.BlockSpec(memory_space=VMEM)
    hbm = pl.BlockSpec(memory_space=pltpu.HBM)
    dma = pltpu.SemaphoreType.DMA
    return pl.pallas_call(
        wave_kernel,
        out_shape=(
            jax.ShapeDtypeStruct((SLOTS, 2, L, Q), F32),
            jax.ShapeDtypeStruct((SLOTS, 2, L, Q), BF),
            jax.ShapeDtypeStruct((2, 2, SLOTS, 2, L, Q), BF),
            jax.ShapeDtypeStruct((2, 8, Q), jnp.int32),
        ),
        in_specs=[hbm] * 11,
        out_specs=(vm,) * 4,
        scratch_shapes=[
            VMEM((2, ROWS, Q), F32),
            VMEM((2, ROWS, Q), F32),
            VMEM((2, 2, ROWS, Q), BF),
            VMEM((2, 2, ROWS, Q), BF),
            VMEM((2, ROWS, Q), BF),
            VMEM((8, Q), jnp.int32),
            VMEM((SLOTS, 2, L, Q), BF),
            VMEM((SLOTS, 2, 2, L, Q), BF),
            VMEM((MODES, 2, L, L), F32),
            VMEM((SLOTS, L, L), F32),
            VMEM((2, 2, 2, L, L), BF),
            VMEM((L, L), BF),
            VMEM((L, L), BF),
            VMEM((4, 2, L, L), F32),
            VMEM((SLOTS, MODES, 2, L, L), F32),
            VMEM((SLOTS, MODES, 2, L, L), F32),
            VMEM((MODES, 2, L, L), F32),
            VMEM((2, L, Q), F32),
            VMEM((2, L, Q), F32),
            VMEM((SLOTS, 2, Q, L), F32),
            VMEM((GROUP, 2, L, L), BF),
            VMEM((GROUP, 2, L, L), BF),
            VMEM((GROUP, 2, L, L), F32),
            VMEM((MODES, 2, L, L), BF),
            VMEM((4, 2, L, L), F32),
            VMEM((2, 2, ROWS, Q), F32),
            dma((5,)),
            dma(()),
            dma(()),
            dma((2, CHUNKS)),
            dma((2, CHUNKS)),
            dma((2, CHUNKS)),
            dma((2, CHUNKS)),
            dma((2,)),
            dma((2,)),
            dma((SLOTS, 2, 2)),
            dma((2, 2, SLOTS)),
            dma((SLOTS,)),
            dma((SLOTS,)),
            pltpu.SemaphoreType.REGULAR,
            SMEM((4,), jnp.int32),
            SMEM((4,), jnp.int32),
            SMEM((1,), jnp.int32),
            SMEM((4,), jnp.int32),
            SMEM((16,), F32),
            SMEM((16,), F32),
            dma((6,)),
        ],
        compiler_params=pltpu.CompilerParams(
            vmem_limit_bytes=60 * 2**20, collective_id=0, has_side_effects=True
        ),
        name="waves",
    )(
        *scalars,
        transmission,
        probe,
        measured,
        jnp.asarray(tables()).astype(BF),
        jnp.asarray(lane_split()).astype(BF),
    )


def combine_kernel(rows, places, mine, theirs, halo, out):
    depth = lax.axis_index("depth")
    tile = lax.axis_index("tile")
    lane = lax.broadcasted_iota(jnp.int32, (L, Q), 1)
    out[...] = jnp.zeros_like(out)

    def add(row, values):
        row = jnp.clip(row, 0, ROWS - L)
        for c in range(2):
            out[c, pl.ds(row, L), :] += values(c)

    for p in range(SLOTS):
        add(rows[depth * SLOTS + p], lambda c: mine[p, c])
        add(rows[(1 - depth) * SLOTS + p], lambda c: theirs[p, c].astype(F32))
        for core in range(2):
            slot = core * SLOTS + p

            @pl.when(tile > 0)
            def _():
                kept = lane < places[0, slot + 4, 0]
                add(places[0, slot, 0], lambda c: jnp.where(kept, halo[0, core, p, c].astype(F32), 0.0))

            @pl.when(tile < lax.axis_size("tile") - 1)
            def _():
                kept = lane >= places[1, slot + 4, 0]
                add(places[1, slot, 0], lambda c: jnp.where(kept, halo[1, core, p, c].astype(F32), 0.0))


def combine(rows, places, parts):
    vm = pl.BlockSpec(memory_space=VMEM)
    return pl.pallas_call(
        combine_kernel,
        out_shape=jax.ShapeDtypeStruct((2, ROWS, Q), F32),
        in_specs=[pl.BlockSpec(memory_space=SMEM)] * 2 + [vm] * 3,
        out_specs=vm,
        compiler_params=pltpu.CompilerParams(vmem_limit_bytes=8 * 2**20),
        name="combine",
    )(rows, places, *parts)


def shards(transmission, probe_modes, measured, scan_rows, scan_cols, counts, dataset, dose_scale, background):
    mine, theirs, halo, places = waves(
        (scan_rows, scan_cols, counts, dataset, dose_scale, background), transmission, probe_modes, measured
    )
    return combine(scan_rows, places, (mine, theirs, halo))[None]


def solution(mesh):
    in_specs = (
        P("depth", None, None, "tile"),
        P(),
        P("tile", None, None),
        P("tile"),
        P("tile"),
        P("tile"),
        P("tile"),
        P(),
        P(),
    )
    out_specs = P("depth", None, None, "tile")
    return jax.shard_map(shards, mesh=mesh, in_specs=in_specs, out_specs=out_specs, check_vma=False)
```

```python
import functools
import math

import jax
import jax.numpy as jnp
import numpy as np
from jax import lax
from jax.experimental import pallas as pl
from jax.experimental.pallas import tpu as pltpu
from jax.sharding import PartitionSpec as P

L = 256
Q = 128
MODES = 6
GROUP = 6
SLOTS = 2
ROWS = 1024
BF = jnp.bfloat16
F32 = jnp.float32
VMEM = pltpu.VMEM
SMEM = pltpu.SMEM


def rounded(values):
    return np.asarray(values, np.float32).astype(jnp.bfloat16).astype(np.float64)


def block(values):
    re, im = values.real, values.imag
    full = np.block([[re, -im], [im, re]])
    return np.stack([full, full.T])


@functools.cache
def tables():
    k = np.arange(L)
    dft = np.exp(-2j * np.pi / L * (k[:, None] * k[None, :] % L)) / math.sqrt(L)
    signed = np.where(k < Q, k, k - L)
    filt = np.exp(-1j * np.pi / L * (signed * signed % (2 * L)))
    prop = dft.conj() @ (filt[:, None] * dft)
    prop = rounded(prop.real) + 1j * rounded(prop.imag)
    dft = rounded(dft.real) + 1j * rounded(dft.imag)
    near, far = prop[:Q, :Q], prop[:Q, Q:]
    halves = [(near + far) / 2, (near - far) / 2]
    kinds = [[block(h) for h in halves], [block(dft[0::2, :Q]), block(dft[1::2, :Q])]]
    return np.stack([np.stack(kind) for kind in kinds]).astype(np.float32)


@functools.cache
def lane_split():
    k = np.arange(L)
    return (k[:, None] == np.where(k < Q, 2 * k, 2 * (k - Q) + 1)[None, :]).astype(np.float32)


def dot(a, b):
    return jnp.dot(a, b, preferred_element_type=F32)


def hadamard(q):
    s0, d0 = q[0][0] + q[0][1], q[0][0] - q[0][1]
    s1, d1 = q[1][0] + q[1][1], q[1][0] - q[1][1]
    return [[s0 + s1, d0 + d1], [s0 - s1, d0 - d1]]


def quads(fn):
    return [[fn(i, j) for j in range(2)] for i in range(2)]


CH = 8


def store_waves(z_ref, m, r, re, im):
    for i in range(2):
        for j in range(2):
            z_ref[m, i, r : r + CH, Q * j : Q * j + Q] = re[i][j].astype(BF)
            z_ref[m, i, Q + r : Q + r + CH, Q * j : Q * j + Q] = im[i][j].astype(BF)


def left_side(table, kind, back, z_ref, u_ref, m):
    for i in range(2):
        u = dot(table[kind, i, back], z_ref[m, i]).astype(BF)
        for j in range(2):
            u_ref[m, j, Q * i : Q * i + Q, 0:Q] = u[0:Q, Q * j : Q * j + Q]
            u_ref[m, j, Q * i : Q * i + Q, Q:L] = u[Q:L, Q * j : Q * j + Q]


def right_side(table, kind, back, u_ref, w_ref, m):
    for j in range(2):
        w_ref[m, j] = dot(u_ref[m, j], table[kind, j, 1 - back])


def read_waves(w_ref, m, r):
    re = quads(lambda i, j: w_ref[m, j, Q * i + r : Q * i + r + CH, 0:Q])
    im = quads(lambda i, j: w_ref[m, j, Q * i + r : Q * i + r + CH, Q:L])
    return re, im


def rotate_probe(probe, pr_ref, spin, p, col):
    shift = lax.broadcasted_iota(jnp.int32, (L, L), 1) - lax.broadcasted_iota(jnp.int32, (L, L), 0)
    spin[...] = jnp.where((shift == col) | (shift == col - L), 1.0, 0.0).astype(BF)

    def one(m, _):
        for c in range(2):
            x = probe[m, c]
            hi = x.astype(BF)
            lo = (x - hi.astype(F32)).astype(BF)
            pr_ref[p, m, c] = dot(hi, spin[...]) + dot(lo, spin[...])
        return 0

    lax.fori_loop(0, MODES, one, 0)


def widen(halo, wide, takes):
    for side in range(2):
        @pl.when(takes[side])
        def _():
            for c in range(2):
                wide[side, c] = halo[side, c].astype(F32)

        @pl.when(jnp.logical_not(takes[side]))
        def _():
            wide[side] = jnp.zeros((2, ROWS, Q), F32)


def load_patch(own, wide, o_ref, place, row, col):
    lane = lax.broadcasted_iota(jnp.int32, (L, Q), 1)
    right = lane < col
    for c in range(2):
        o_ref[place, c, :, 0:Q] = jnp.where(right, wide[1, c, pl.ds(row, L), :], wide[0, c, pl.ds(row, L), :])
        o_ref[place, c, :, Q:L] = own[c, pl.ds(row, L), :]


def amplitudes(measured, slot, split, amp_ref, tmp_ref):
    for j in range(2):
        tmp_ref[j] = jnp.sqrt(measured[slot, :, Q * j : Q * j + Q])
    for i in range(2):
        x = jnp.concatenate([tmp_ref[j, pl.ds(i, Q, stride=2), :] for j in range(2)], axis=1)
        hi = x.astype(BF)
        rest = x - hi.astype(F32)
        mid = rest.astype(BF)
        lo = (rest - mid.astype(F32)).astype(BF)
        amp_ref[slot, i] = dot(hi, split[...]) + (dot(mid, split[...]) + dot(lo, split[...]))


def forward_first(table, pr_ref, o_ref, p, z, u, w, psi_ref):
    def group(g, _):
        for k in range(GROUP):
            m = g * GROUP + k
            for r in range(0, Q, CH):
                re, im = [[None] * 2 for _ in range(2)], [[None] * 2 for _ in range(2)]
                for i in range(2):
                    for j in range(2):
                        rows, lanes = slice(Q * i + r, Q * i + r + CH), slice(Q * j, Q * j + Q)
                        a, b = pr_ref[p, m, 0, rows, lanes], pr_ref[p, m, 1, rows, lanes]
                        c, d = o_ref[2 * p, 0, rows, lanes], o_ref[2 * p, 1, rows, lanes]
                        re[i][j], im[i][j] = a * c - b * d, a * d + b * c
                store_waves(z, k, r, hadamard(re), hadamard(im))
        for k in range(GROUP):
            left_side(table, 0, 0, z, u, k)
        for k in range(GROUP):
            right_side(table, 0, 0, u, w, k)
        for k in range(GROUP):
            m = g * GROUP + k
            for r in range(0, Q, CH):
                vre, vim = read_waves(w, k, r)
                vre, vim = hadamard(vre), hadamard(vim)
                for i in range(2):
                    for j in range(2):
                        rows, lanes = slice(Q * i + r, Q * i + r + CH), slice(Q * j, Q * j + Q)
                        psi_ref[p, m, 0, rows, lanes] = vre[i][j]
                        psi_ref[p, m, 1, rows, lanes] = vim[i][j]
        return 0

    group(0, 0)


def forward_last(table, o_ref, p, z, u, psi_ref, far_ref, int_ref):
    def group(g, _):
        for k in range(GROUP):
            m = g * GROUP + k
            for r in range(0, Q, CH):
                re, im = [[None] * 2 for _ in range(2)], [[None] * 2 for _ in range(2)]
                for i in range(2):
                    for j in range(2):
                        rows, lanes = slice(Q * i + r, Q * i + r + CH), slice(Q * j, Q * j + Q)
                        a = psi_ref[p, m, 0, rows, lanes]
                        b = psi_ref[p, m, 1, rows, lanes]
                        c, d = o_ref[2 * p + 1, 0, rows, lanes], o_ref[2 * p + 1, 1, rows, lanes]
                        re[i][j], im[i][j] = a * c - b * d, a * d + b * c
                store_waves(z, k, r, hadamard(re), hadamard(im))
        for k in range(GROUP):
            left_side(table, 1, 0, z, u, k)
        for k in range(GROUP):
            for j in range(2):
                far_ref[g * GROUP + k, j] = dot(u[k, j], table[1, j, 1])
        for j in range(2):
            for r in range(0, L, CH):
                total = None
                for k in range(GROUP):
                    x = far_ref[g * GROUP + k, j, r : r + CH, 0:Q]
                    y = far_ref[g * GROUP + k, j, r : r + CH, Q:L]
                    power = x * x + y * y
                    total = power if total is None else total + power
                int_ref[j, r : r + CH, :] = total
        return 0

    group(0, 0)


def residual_factor(int_ref, amp_ref, p, fac_ref, scale, offset, valid):
    for j in range(2):
        for i in range(2):
            intensity = scale * int_ref[j, Q * i : Q * i + Q, :] + offset
            ratio = amp_ref[p, i, :, Q * j : Q * j + Q] / jnp.sqrt(intensity)
            fac_ref[j, Q * i : Q * i + Q, :] = jnp.where(valid, scale * (1.0 - ratio), 0.0)


def cells(r):
    return [(i, j, slice(Q * i + r, Q * i + r + CH), slice(Q * j, Q * j + Q)) for i in range(2) for j in range(2)]


def add_conj(sums, n, a, b, x, y):
    gre, gim = a * x + b * y, a * y - b * x
    sums[n] = (gre, gim) if sums[n] is None else (sums[n][0] + gre, sums[n][1] + gim)


def store_sums(grad_ref, place, r, sums):
    for n, (i, j, rows, lanes) in enumerate(cells(r)):
        grad_ref[place, 0, rows, lanes], grad_ref[place, 1, rows, lanes] = sums[n]


def backward_last(table, o_ref, p, z, u, w, psi_ref, far_ref, fac_ref, grad_ref, gz_ref):
    def group(g, _):
        for k in range(GROUP):
            m = g * GROUP + k
            for j in range(2):
                for r in range(0, L, CH):
                    f = fac_ref[j, r : r + CH, :]
                    i, s = r // Q, r % Q
                    z[k, i, s : s + CH, Q * j : Q * j + Q] = (f * far_ref[m, j, r : r + CH, 0:Q]).astype(BF)
                    z[k, i, Q + s : Q + s + CH, Q * j : Q * j + Q] = (
                        f * far_ref[m, j, r : r + CH, Q:L]
                    ).astype(BF)
        for k in range(GROUP):
            left_side(table, 1, 1, z, u, k)
        for k in range(GROUP):
            right_side(table, 1, 1, u, w, k)
        for k in range(GROUP):
            m = g * GROUP + k
            for r in range(0, Q, CH):
                vre, vim = read_waves(w, k, r)
                vre, vim = hadamard(vre), hadamard(vim)
                re, im = [[None] * 2 for _ in range(2)], [[None] * 2 for _ in range(2)]
                for n, (i, j, rows, lanes) in enumerate(cells(r)):
                    x, y = vre[i][j], vim[i][j]
                    a, b = psi_ref[p, m, 0, rows, lanes], psi_ref[p, m, 1, rows, lanes]
                    gre, gim = a * x + b * y, a * y - b * x
                    if k > 0:
                        gre, gim = grad_ref.at[2 * p + 1][0, rows, lanes] + gre, grad_ref.at[2 * p + 1][1, rows, lanes] + gim
                    grad_ref.at[2 * p + 1][0, rows, lanes], grad_ref.at[2 * p + 1][1, rows, lanes] = gre, gim
                    c, d = o_ref[2 * p + 1, 0, rows, lanes], o_ref[2 * p + 1, 1, rows, lanes]
                    re[i][j], im[i][j] = c * x + d * y, c * y - d * x
                store_waves(gz_ref, m, r, hadamard(re), hadamard(im))
        return 0

    group(0, 0)


def backward_first(table, pr_ref, p, u, w, grad_ref, gz_ref):
    def group(g, _):
        for k in range(GROUP):
            m = g * GROUP + k
            for i in range(2):
                x = dot(table[0, i, 1], gz_ref[m, i]).astype(BF)
                for j in range(2):
                    u[k, j, Q * i : Q * i + Q, 0:Q] = x[0:Q, Q * j : Q * j + Q]
                    u[k, j, Q * i : Q * i + Q, Q:L] = x[Q:L, Q * j : Q * j + Q]
        for k in range(GROUP):
            right_side(table, 0, 1, u, w, k)
        for r in range(0, Q, CH):
            sums = [None] * 4
            for k in range(GROUP):
                m = g * GROUP + k
                vre, vim = read_waves(w, k, r)
                vre, vim = hadamard(vre), hadamard(vim)
                for n, (i, j, rows, lanes) in enumerate(cells(r)):
                    a, b = pr_ref[p, m, 0, rows, lanes], pr_ref[p, m, 1, rows, lanes]
                    add_conj(sums, n, a, b, vre[i][j], vim[i][j])
            store_sums(grad_ref, 2 * p, r, sums)
        return 0

    group(0, 0)


CHUNKS = 4
RELEASE = 3
MESH = pl.DeviceIdType.MESH


def wave_kernel(
    rows_in, cols_in, counts_in, dataset_in, dose_in, ground_in,
    trans, probe_in, measured_in, table_in, split_in,
    own_mine, own_in, halo_in, places_in,
    own_a, own_b, halo_a, halo_b, short, places, own_out, halo_out,
    probe, measured, table, split, spin,
    o_ref, pr_ref, psi_ref, far_ref, int_ref, fac_ref, amp_ref, z, u, w, gz, grad_ref, wide,
    load_sem, own_send, own_recv, side_send, side_recv, relay_send, relay_recv,
    place_send, place_recv, grad_send, grad_recv, part_send, part_recv, go,
    rows, cols, counts, dataset, dose, ground, small_sem,
):
    depth = lax.axis_index("depth")
    tile = lax.axis_index("tile")
    tiles = lax.axis_size("tile")
    ahead, behind = lax.rem(tile + 1, tiles), lax.rem(tile + tiles - 1, tiles)
    other = 1 - depth
    beside = (ahead, behind)

    upper, lower = tile < tiles - 1, tile > 0
    sends, takes = (upper, lower), (lower, upper)

    barrier = pltpu.get_barrier_semaphore()
    pl.semaphore_signal(barrier, inc=1, device_id=(tile, other), device_id_type=MESH)
    for side in range(2):
        @pl.when(sends[side])
        def _():
            for core in (depth, other):
                pl.semaphore_signal(barrier, inc=1, device_id=(beside[side], core), device_id_type=MESH)

    def remote(src, dst, send, recv, target):
        return pltpu.make_async_remote_copy(
            src_ref=src, dst_ref=dst, send_sem=send, recv_sem=recv, device_id=target, device_id_type=MESH
        )

    loads = [
        pltpu.make_async_copy(probe_in, probe, load_sem.at[0]),
        pltpu.make_async_copy(measured_in.at[pl.ds(depth * SLOTS, SLOTS)], measured, load_sem.at[1]),
        pltpu.make_async_copy(table_in, table, load_sem.at[2]),
        pltpu.make_async_copy(split_in, split, load_sem.at[3]),
    ]

    def own_load(ref):
        return pltpu.make_async_copy(trans.at[0], ref, load_sem.at[4])

    def own_copy(ref):
        return remote(trans.at[0], ref, own_send, own_recv, (tile, other))

    def side_copy(ref, side, k):
        span = pl.ds(k * (ROWS // CHUNKS), ROWS // CHUNKS)
        return remote(
            short.at[:, span, :], ref.at[side, :, span, :], side_send.at[side, k], side_recv.at[side, k],
            (beside[side], depth),
        )

    def relay_copy(ref, side, k):
        span = pl.ds(k * (ROWS // CHUNKS), ROWS // CHUNKS)
        return remote(
            ref.at[side, :, span, :], ref.at[side, :, span, :], relay_send.at[side, k], relay_recv.at[side, k],
            (tile, other),
        )

    def place_copy(side):
        return remote(places, places_in.at[side], place_send.at[side], place_recv.at[side], (beside[side], depth))

    def grad_copy(p, home, side):
        target = depth if home == 0 else other
        return remote(
            halo_out.at[p, home], halo_in.at[side, depth, p], grad_send.at[p, home, side],
            grad_recv.at[side, depth, p], (beside[side], target),
        )

    def grad_arrival(p, core, side):
        return remote(
            halo_out.at[p, 0], halo_in.at[side, core, p], grad_send.at[p, 0, side], grad_recv.at[side, core, p],
            (beside[side], depth),
        )

    def part_copy(p):
        return remote(own_out.at[p], own_in.at[p], part_send.at[p], part_recv.at[p], (tile, other))

    mine = {0: (own_a, halo_a), 1: (own_b, halo_b)}
    for d in range(2):
        @pl.when(depth == d)
        def _():
            own_load(mine[d][0]).start()
    smalls = [
        pltpu.make_async_copy(src, dst, small_sem.at[n])
        for n, (src, dst) in enumerate(
            (
                (rows_in, rows), (cols_in, cols), (counts_in, counts),
                (dataset_in, dataset), (dose_in, dose), (ground_in, ground),
            )
        )
    ]
    for load in smalls + loads:
        load.start()
    for d in range(2):
        @pl.when(depth == d)
        def _():
            own_load(mine[d][0]).wait()
            for c in range(2):
                short[c] = mine[d][0][c].astype(BF)
    pl.semaphore_wait(barrier, 1 + 2 * (lower.astype(jnp.int32) + upper.astype(jnp.int32)))

    def sides(flags, act):
        for side in range(2):
            @pl.when(flags[side])
            def _():
                act(side)

    def send_tiles(ref):
        for k in range(CHUNKS):
            sides(sends, lambda side: side_copy(ref, side, k).start())

    for d in range(2):
        @pl.when(depth == d)
        def _():
            own_copy(mine[d][0]).start()
    @pl.when(depth == 0)
    def _():
        send_tiles(halo_a)

    def spot(p):
        slot = depth * SLOTS + p
        return slot, jnp.clip(rows[slot], 0, ROWS - L), jnp.clip(cols[slot], 0, Q - 1)

    for load in smalls:
        load.wait()
    for n in range(4):
        places[n : n + 1, :] = jnp.full((1, Q), rows[n], jnp.int32)
        places[n + 4 : n + 5, :] = jnp.full((1, Q), cols[n], jnp.int32)
    for load in loads:
        load.wait()

    def turn(p, _):
        rotate_probe(probe, pr_ref, spin, p, spot(p)[2])
        amplitudes(measured, p, split, amp_ref, int_ref)
        return 0

    lax.fori_loop(0, SLOTS, turn, 0)

    def take(side, k, ref):
        side_copy(ref, side, k).wait_recv()
        relay_copy(ref, side, k).start()

    @pl.when(depth == 0)
    def _():
        for k in range(RELEASE):
            sides(sends, lambda side: side_copy(halo_a, side, k).wait_send())
        pl.semaphore_signal(go, inc=1, device_id=(tile, other), device_id_type=MESH)
        for k in range(CHUNKS):
            sides(takes, lambda side: take(side, k, halo_a))
        for k in range(RELEASE, CHUNKS):
            sides(sends, lambda side: side_copy(halo_a, side, k).wait_send())
        own_copy(own_b).wait_recv()

    @pl.when(depth == 1)
    def _():
        pl.semaphore_wait(go, 1)
        send_tiles(halo_b)
        own_copy(own_a).wait_recv()
        for k in range(CHUNKS):
            sides(takes, lambda side: relay_copy(halo_a, side, k).wait_recv())
    own_copy(own_a).wait_send()
    sides(sends, lambda side: place_copy(side).start())
    widen(halo_a, wide, takes)

    def start(p, _):
        _, row, col = spot(p)
        load_patch(own_a, wide, o_ref, 2 * p, row, col)
        forward_first(table, pr_ref, o_ref, p, z, u, w, psi_ref)

        @pl.when(depth == 1)
        def _():
            for kk in range(CHUNKS // SLOTS):
                sides(takes, lambda side: take(side, p * (CHUNKS // SLOTS) + kk, halo_b))
        return 0

    lax.fori_loop(0, SLOTS, start, 0)

    @pl.when(depth == 0)
    def _():
        for k in range(CHUNKS):
            sides(takes, lambda side: relay_copy(halo_b, side, k).wait_recv())
            sides(takes, lambda side: relay_copy(halo_a, side, k).wait_send())

    @pl.when(depth == 1)
    def _():
        for k in range(CHUNKS):
            sides(sends, lambda side: side_copy(halo_b, side, k).wait_send())
            sides(takes, lambda side: relay_copy(halo_b, side, k).wait_send())

    widen(halo_b, wide, takes)

    def hand_over(p, s):
        place = 2 * p + s
        @pl.when(depth == s)
        def _():
            halo_out[p, 0] = grad_ref[place, :, :, 0:Q].astype(BF)
            sides(sends, lambda side: grad_copy(p, 0, side).start())
            own_mine[p] = grad_ref[place, :, :, Q:L]
        @pl.when(depth != s)
        def _():
            halo_out[p, 1] = grad_ref[place, :, :, 0:Q].astype(BF)
            sides(sends, lambda side: grad_copy(p, 1, side).start())
            own_out[p] = grad_ref[place, :, :, Q:L].astype(BF)
            part_copy(p).start()

    def finish(p, _):
        slot, row, col = spot(p)
        which = jnp.clip(dataset[slot], 0, dose.shape[0] - 1)
        load_patch(own_b, wide, o_ref, 2 * p + 1, row, col)
        forward_last(table, o_ref, p, z, u, psi_ref, far_ref, int_ref)
        residual_factor(int_ref, amp_ref, p, fac_ref, dose[which], ground[which], slot < counts[0])
        backward_last(table, o_ref, p, z, u, w, psi_ref, far_ref, fac_ref, grad_ref, gz)
        hand_over(p, 1)
        backward_first(table, pr_ref, p, u, w, grad_ref, gz)
        hand_over(p, 0)
        return 0

    lax.fori_loop(0, SLOTS, finish, 0)

    sides(sends, lambda side: place_copy(side).wait_send())
    sides(takes, lambda side: place_copy(side).wait_recv())
    for p in range(SLOTS):
        part_copy(p).wait()
        for n in range(2):
            sides(sends, lambda side: grad_copy(p, n, side).wait_send())
            sides(takes, lambda side: grad_arrival(p, n, side).wait_recv())


def waves(scalars, transmission, probe, measured):
    vm = pl.BlockSpec(memory_space=VMEM)
    hbm = pl.BlockSpec(memory_space=pltpu.HBM)
    dma = pltpu.SemaphoreType.DMA
    return pl.pallas_call(
        wave_kernel,
        out_shape=(
            jax.ShapeDtypeStruct((SLOTS, 2, L, Q), F32),
            jax.ShapeDtypeStruct((SLOTS, 2, L, Q), BF),
            jax.ShapeDtypeStruct((2, 2, SLOTS, 2, L, Q), BF),
            jax.ShapeDtypeStruct((2, 8, Q), jnp.int32),
        ),
        in_specs=[hbm] * 11,
        out_specs=(vm,) * 4,
        scratch_shapes=[
            VMEM((2, ROWS, Q), F32),
            VMEM((2, ROWS, Q), F32),
            VMEM((2, 2, ROWS, Q), BF),
            VMEM((2, 2, ROWS, Q), BF),
            VMEM((2, ROWS, Q), BF),
            VMEM((8, Q), jnp.int32),
            VMEM((SLOTS, 2, L, Q), BF),
            VMEM((SLOTS, 2, 2, L, Q), BF),
            VMEM((MODES, 2, L, L), F32),
            VMEM((SLOTS, L, L), F32),
            VMEM((2, 2, 2, L, L), BF),
            VMEM((L, L), BF),
            VMEM((L, L), BF),
            VMEM((4, 2, L, L), F32),
            VMEM((SLOTS, MODES, 2, L, L), F32),
            VMEM((SLOTS, MODES, 2, L, L), F32),
            VMEM((MODES, 2, L, L), F32),
            VMEM((2, L, Q), F32),
            VMEM((2, L, Q), F32),
            VMEM((SLOTS, 2, Q, L), F32),
            VMEM((GROUP, 2, L, L), BF),
            VMEM((GROUP, 2, L, L), BF),
            VMEM((GROUP, 2, L, L), F32),
            VMEM((MODES, 2, L, L), BF),
            VMEM((4, 2, L, L), F32),
            VMEM((2, 2, ROWS, Q), F32),
            dma((5,)),
            dma(()),
            dma(()),
            dma((2, CHUNKS)),
            dma((2, CHUNKS)),
            dma((2, CHUNKS)),
            dma((2, CHUNKS)),
            dma((2,)),
            dma((2,)),
            dma((SLOTS, 2, 2)),
            dma((2, 2, SLOTS)),
            dma((SLOTS,)),
            dma((SLOTS,)),
            pltpu.SemaphoreType.REGULAR,
            SMEM((4,), jnp.int32),
            SMEM((4,), jnp.int32),
            SMEM((1,), jnp.int32),
            SMEM((4,), jnp.int32),
            SMEM((16,), F32),
            SMEM((16,), F32),
            dma((6,)),
        ],
        compiler_params=pltpu.CompilerParams(
            vmem_limit_bytes=48 * 2**20, collective_id=0, has_side_effects=True
        ),
        name="waves",
    )(
        *[
            x if x.shape == (1,) else pltpu.with_memory_space_constraint(x, pltpu.HBM)
            for x in (
                *scalars,
                transmission,
                probe,
                measured,
                jnp.asarray(tables()).astype(BF),
                jnp.asarray(lane_split()).astype(BF),
            )
        ]
    )


def combine_kernel(rows, places, mine, theirs, halo, out):
    depth = lax.axis_index("depth")
    tile = lax.axis_index("tile")
    lane = lax.broadcasted_iota(jnp.int32, (L, Q), 1)
    out[...] = jnp.zeros_like(out)

    def add(row, values):
        row = jnp.clip(row, 0, ROWS - L)
        for c in range(2):
            out[c, pl.ds(row, L), :] += values(c)

    for p in range(SLOTS):
        add(rows[depth * SLOTS + p], lambda c: mine[p, c])
        add(rows[(1 - depth) * SLOTS + p], lambda c: theirs[p, c].astype(F32))
        for core in range(2):
            slot = core * SLOTS + p

            @pl.when(tile > 0)
            def _():
                kept = lane < places[0, slot + 4, 0]
                add(places[0, slot, 0], lambda c: jnp.where(kept, halo[0, core, p, c].astype(F32), 0.0))

            @pl.when(tile < lax.axis_size("tile") - 1)
            def _():
                kept = lane >= places[1, slot + 4, 0]
                add(places[1, slot, 0], lambda c: jnp.where(kept, halo[1, core, p, c].astype(F32), 0.0))


def combine(rows, places, parts):
    vm = pl.BlockSpec(memory_space=VMEM)
    return pl.pallas_call(
        combine_kernel,
        out_shape=jax.ShapeDtypeStruct((2, ROWS, Q), F32),
        in_specs=[pl.BlockSpec(memory_space=SMEM)] * 2 + [vm] * 3,
        out_specs=vm,
        compiler_params=pltpu.CompilerParams(vmem_limit_bytes=8 * 2**20),
        name="combine",
    )(rows, places, *parts)


def shards(transmission, probe_modes, measured, scan_rows, scan_cols, counts, dataset, dose_scale, background):
    mine, theirs, halo, places = waves(
        (scan_rows, scan_cols, counts, dataset, dose_scale, background), transmission, probe_modes, measured
    )
    return combine(scan_rows, places, (mine, theirs, halo))[None]


def solution(mesh):
    in_specs = (
        P("depth", None, None, "tile"),
        P(),
        P("tile", None, None),
        P("tile"),
        P("tile"),
        P("tile"),
        P("tile"),
        P(),
        P(),
    )
    out_specs = P("depth", None, None, "tile")
    return jax.shard_map(shards, mesh=mesh, in_specs=in_specs, out_specs=out_specs, check_vma=False)
```

```python
import functools
import math

import jax
import jax.numpy as jnp
import numpy as np
from jax import lax
from jax.experimental import pallas as pl
from jax.experimental.pallas import tpu as pltpu
from jax.sharding import PartitionSpec as P

L = 256
Q = 128
MODES = 6
GROUP = 6
SLOTS = 2
ROWS = 1024
BF = jnp.bfloat16
F32 = jnp.float32
VMEM = pltpu.VMEM
SMEM = pltpu.SMEM


def rounded(values):
    return np.asarray(values, np.float32).astype(jnp.bfloat16).astype(np.float64)


def block(values):
    re, im = values.real, values.imag
    full = np.block([[re, -im], [im, re]])
    return np.stack([full, full.T])


@functools.cache
def tables():
    k = np.arange(L)
    dft = np.exp(-2j * np.pi / L * (k[:, None] * k[None, :] % L)) / math.sqrt(L)
    signed = np.where(k < Q, k, k - L)
    filt = np.exp(-1j * np.pi / L * (signed * signed % (2 * L)))
    prop = dft.conj() @ (filt[:, None] * dft)
    prop = rounded(prop.real) + 1j * rounded(prop.imag)
    dft = rounded(dft.real) + 1j * rounded(dft.imag)
    near, far = prop[:Q, :Q], prop[:Q, Q:]
    halves = [(near + far) / 2, (near - far) / 2]
    kinds = [[block(h) for h in halves], [block(dft[0::2, :Q]), block(dft[1::2, :Q])]]
    return np.stack([np.stack(kind) for kind in kinds]).astype(np.float32)


@functools.cache
def lane_split():
    k = np.arange(L)
    return (k[:, None] == np.where(k < Q, 2 * k, 2 * (k - Q) + 1)[None, :]).astype(np.float32)


def dot(a, b):
    return jnp.dot(a, b, preferred_element_type=F32)


def hadamard(q):
    s0, d0 = q[0][0] + q[0][1], q[0][0] - q[0][1]
    s1, d1 = q[1][0] + q[1][1], q[1][0] - q[1][1]
    return [[s0 + s1, d0 + d1], [s0 - s1, d0 - d1]]


def quads(fn):
    return [[fn(i, j) for j in range(2)] for i in range(2)]


CH = 8


def store_waves(z_ref, m, r, re, im):
    for i in range(2):
        for j in range(2):
            z_ref[m, i, r : r + CH, Q * j : Q * j + Q] = re[i][j].astype(BF)
            z_ref[m, i, Q + r : Q + r + CH, Q * j : Q * j + Q] = im[i][j].astype(BF)


def left_side(table, kind, back, z_ref, u_ref, m):
    for i in range(2):
        u = dot(table[kind, i, back], z_ref[m, i]).astype(BF)
        for j in range(2):
            u_ref[m, j, Q * i : Q * i + Q, 0:Q] = u[0:Q, Q * j : Q * j + Q]
            u_ref[m, j, Q * i : Q * i + Q, Q:L] = u[Q:L, Q * j : Q * j + Q]


def right_side(table, kind, back, u_ref, w_ref, m):
    for j in range(2):
        w_ref[m, j] = dot(u_ref[m, j], table[kind, j, 1 - back])


def read_waves(w_ref, m, r):
    re = quads(lambda i, j: w_ref[m, j, Q * i + r : Q * i + r + CH, 0:Q])
    im = quads(lambda i, j: w_ref[m, j, Q * i + r : Q * i + r + CH, Q:L])
    return re, im


def rotate_probe(probe, pr_ref, spin, p, col):
    shift = lax.broadcasted_iota(jnp.int32, (L, L), 1) - lax.broadcasted_iota(jnp.int32, (L, L), 0)
    spin[...] = jnp.where((shift == col) | (shift == col - L), 1.0, 0.0).astype(BF)

    def one(m, _):
        for c in range(2):
            x = probe[m, c]
            hi = x.astype(BF)
            lo = (x - hi.astype(F32)).astype(BF)
            pr_ref[p, m, c] = dot(hi, spin[...]) + dot(lo, spin[...])
        return 0

    lax.fori_loop(0, MODES, one, 0)


def widen(halo, wide, takes):
    for side in range(2):
        @pl.when(takes[side])
        def _():
            for c in range(2):
                wide[side, c] = halo[side, c].astype(F32)

        @pl.when(jnp.logical_not(takes[side]))
        def _():
            wide[side] = jnp.zeros((2, ROWS, Q), F32)


def load_patch(own, wide, o_ref, place, row, col):
    lane = lax.broadcasted_iota(jnp.int32, (L, Q), 1)
    right = lane < col
    for c in range(2):
        o_ref[place, c, :, 0:Q] = jnp.where(right, wide[1, c, pl.ds(row, L), :], wide[0, c, pl.ds(row, L), :])
        o_ref[place, c, :, Q:L] = own[c, pl.ds(row, L), :]


def amplitudes(measured, slot, split, amp_ref, tmp_ref):
    for j in range(2):
        tmp_ref[j] = jnp.sqrt(measured[slot, :, Q * j : Q * j + Q])
    for i in range(2):
        x = jnp.concatenate([tmp_ref[j, pl.ds(i, Q, stride=2), :] for j in range(2)], axis=1)
        hi = x.astype(BF)
        rest = x - hi.astype(F32)
        mid = rest.astype(BF)
        lo = (rest - mid.astype(F32)).astype(BF)
        amp_ref[slot, i] = dot(hi, split[...]) + (dot(mid, split[...]) + dot(lo, split[...]))


def forward_first(table, pr_ref, o_ref, p, z, u, w, psi_ref):
    def group(g, _):
        for k in range(GROUP):
            m = g * GROUP + k
            for r in range(0, Q, CH):
                re, im = [[None] * 2 for _ in range(2)], [[None] * 2 for _ in range(2)]
                for i in range(2):
                    for j in range(2):
                        rows, lanes = slice(Q * i + r, Q * i + r + CH), slice(Q * j, Q * j + Q)
                        a, b = pr_ref[p, m, 0, rows, lanes], pr_ref[p, m, 1, rows, lanes]
                        c, d = o_ref[2 * p, 0, rows, lanes], o_ref[2 * p, 1, rows, lanes]
                        re[i][j], im[i][j] = a * c - b * d, a * d + b * c
                store_waves(z, k, r, hadamard(re), hadamard(im))
        for k in range(GROUP):
            left_side(table, 0, 0, z, u, k)
        for k in range(GROUP):
            right_side(table, 0, 0, u, w, k)
        for k in range(GROUP):
            m = g * GROUP + k
            for r in range(0, Q, CH):
                vre, vim = read_waves(w, k, r)
                vre, vim = hadamard(vre), hadamard(vim)
                for i in range(2):
                    for j in range(2):
                        rows, lanes = slice(Q * i + r, Q * i + r + CH), slice(Q * j, Q * j + Q)
                        psi_ref[p, m, 0, rows, lanes] = vre[i][j]
                        psi_ref[p, m, 1, rows, lanes] = vim[i][j]
        return 0

    group(0, 0)


def forward_last(table, o_ref, p, z, u, psi_ref, far_ref, int_ref):
    def group(g, _):
        for k in range(GROUP):
            m = g * GROUP + k
            for r in range(0, Q, CH):
                re, im = [[None] * 2 for _ in range(2)], [[None] * 2 for _ in range(2)]
                for i in range(2):
                    for j in range(2):
                        rows, lanes = slice(Q * i + r, Q * i + r + CH), slice(Q * j, Q * j + Q)
                        a = psi_ref[p, m, 0, rows, lanes]
                        b = psi_ref[p, m, 1, rows, lanes]
                        c, d = o_ref[2 * p + 1, 0, rows, lanes], o_ref[2 * p + 1, 1, rows, lanes]
                        re[i][j], im[i][j] = a * c - b * d, a * d + b * c
                store_waves(z, k, r, hadamard(re), hadamard(im))
        for k in range(GROUP):
            left_side(table, 1, 0, z, u, k)
        for k in range(GROUP):
            for j in range(2):
                far_ref[g * GROUP + k, j] = dot(u[k, j], table[1, j, 1])
        for j in range(2):
            for r in range(0, L, CH):
                total = None
                for k in range(GROUP):
                    x = far_ref[g * GROUP + k, j, r : r + CH, 0:Q]
                    y = far_ref[g * GROUP + k, j, r : r + CH, Q:L]
                    power = x * x + y * y
                    total = power if total is None else total + power
                int_ref[j, r : r + CH, :] = total
        return 0

    group(0, 0)


def residual_factor(int_ref, amp_ref, p, fac_ref, scale, offset, valid):
    for j in range(2):
        for i in range(2):
            intensity = scale * int_ref[j, Q * i : Q * i + Q, :] + offset
            ratio = amp_ref[p, i, :, Q * j : Q * j + Q] / jnp.sqrt(intensity)
            fac_ref[j, Q * i : Q * i + Q, :] = jnp.where(valid, scale * (1.0 - ratio), 0.0)


def cells(r):
    return [(i, j, slice(Q * i + r, Q * i + r + CH), slice(Q * j, Q * j + Q)) for i in range(2) for j in range(2)]


def add_conj(sums, n, a, b, x, y):
    gre, gim = a * x + b * y, a * y - b * x
    sums[n] = (gre, gim) if sums[n] is None else (sums[n][0] + gre, sums[n][1] + gim)


def store_sums(grad_ref, place, r, sums):
    for n, (i, j, rows, lanes) in enumerate(cells(r)):
        grad_ref[place, 0, rows, lanes], grad_ref[place, 1, rows, lanes] = sums[n]


def backward_last(table, o_ref, p, z, u, w, psi_ref, far_ref, fac_ref, grad_ref, gz_ref):
    def group(g, _):
        for k in range(GROUP):
            m = g * GROUP + k
            for j in range(2):
                for r in range(0, L, CH):
                    f = fac_ref[j, r : r + CH, :]
                    i, s = r // Q, r % Q
                    z[k, i, s : s + CH, Q * j : Q * j + Q] = (f * far_ref[m, j, r : r + CH, 0:Q]).astype(BF)
                    z[k, i, Q + s : Q + s + CH, Q * j : Q * j + Q] = (
                        f * far_ref[m, j, r : r + CH, Q:L]
                    ).astype(BF)
        for k in range(GROUP):
            left_side(table, 1, 1, z, u, k)
        for k in range(GROUP):
            right_side(table, 1, 1, u, w, k)
        for k in range(GROUP):
            m = g * GROUP + k
            for r in range(0, Q, CH):
                vre, vim = read_waves(w, k, r)
                vre, vim = hadamard(vre), hadamard(vim)
                re, im = [[None] * 2 for _ in range(2)], [[None] * 2 for _ in range(2)]
                for n, (i, j, rows, lanes) in enumerate(cells(r)):
                    x, y = vre[i][j], vim[i][j]
                    a, b = psi_ref[p, m, 0, rows, lanes], psi_ref[p, m, 1, rows, lanes]
                    gre, gim = a * x + b * y, a * y - b * x
                    if k > 0:
                        gre, gim = grad_ref.at[2 * p + 1][0, rows, lanes] + gre, grad_ref.at[2 * p + 1][1, rows, lanes] + gim
                    grad_ref.at[2 * p + 1][0, rows, lanes], grad_ref.at[2 * p + 1][1, rows, lanes] = gre, gim
                    c, d = o_ref[2 * p + 1, 0, rows, lanes], o_ref[2 * p + 1, 1, rows, lanes]
                    re[i][j], im[i][j] = c * x + d * y, c * y - d * x
                store_waves(gz_ref, m, r, hadamard(re), hadamard(im))
        return 0

    group(0, 0)


def backward_first(table, pr_ref, p, u, w, grad_ref, gz_ref):
    def group(g, _):
        for k in range(GROUP):
            m = g * GROUP + k
            for i in range(2):
                x = dot(table[0, i, 1], gz_ref[m, i]).astype(BF)
                for j in range(2):
                    u[k, j, Q * i : Q * i + Q, 0:Q] = x[0:Q, Q * j : Q * j + Q]
                    u[k, j, Q * i : Q * i + Q, Q:L] = x[Q:L, Q * j : Q * j + Q]
        for k in range(GROUP):
            right_side(table, 0, 1, u, w, k)
        for r in range(0, Q, CH):
            sums = [None] * 4
            for k in range(GROUP):
                m = g * GROUP + k
                vre, vim = read_waves(w, k, r)
                vre, vim = hadamard(vre), hadamard(vim)
                for n, (i, j, rows, lanes) in enumerate(cells(r)):
                    a, b = pr_ref[p, m, 0, rows, lanes], pr_ref[p, m, 1, rows, lanes]
                    add_conj(sums, n, a, b, vre[i][j], vim[i][j])
            store_sums(grad_ref, 2 * p, r, sums)
        return 0

    group(0, 0)


CHUNKS = 4
RELEASE = 3
MESH = pl.DeviceIdType.MESH


def wave_kernel(
    rows_in, cols_in, counts_in, dataset_in, dose_in, ground_in,
    trans, probe_in, measured_in, table_in, split_in,
    own_mine, own_in, halo_in, places_in,
    own_a, own_b, halo_a, halo_b, short, places, own_out, halo_out,
    probe, measured, table, split, spin,
    o_ref, pr_ref, psi_ref, far_ref, int_ref, fac_ref, amp_ref, z, u, w, gz, grad_ref, wide,
    load_sem, own_send, own_recv, side_send, side_recv, relay_send, relay_recv,
    place_send, place_recv, grad_send, grad_recv, part_send, part_recv, go,
    rows, cols, counts, dataset, dose, ground, small_sem,
):
    depth = lax.axis_index("depth")
    tile = lax.axis_index("tile")
    tiles = lax.axis_size("tile")
    ahead, behind = lax.rem(tile + 1, tiles), lax.rem(tile + tiles - 1, tiles)
    other = 1 - depth
    beside = (ahead, behind)

    upper, lower = tile < tiles - 1, tile > 0
    sends, takes = (upper, lower), (lower, upper)

    barrier = pltpu.get_barrier_semaphore()
    pl.semaphore_signal(barrier, inc=1, device_id=(tile, other), device_id_type=MESH)
    for side in range(2):
        @pl.when(sends[side])
        def _():
            for core in (depth, other):
                pl.semaphore_signal(barrier, inc=1, device_id=(beside[side], core), device_id_type=MESH)

    def remote(src, dst, send, recv, target):
        return pltpu.make_async_remote_copy(
            src_ref=src, dst_ref=dst, send_sem=send, recv_sem=recv, device_id=target, device_id_type=MESH
        )

    loads = [
        pltpu.make_async_copy(probe_in, probe, load_sem.at[0]),
        pltpu.make_async_copy(measured_in.at[pl.ds(depth * SLOTS, SLOTS)], measured, load_sem.at[1]),
        pltpu.make_async_copy(table_in, table, load_sem.at[2]),
        pltpu.make_async_copy(split_in, split, load_sem.at[3]),
    ]

    def own_load(ref):
        return pltpu.make_async_copy(trans.at[0], ref, load_sem.at[4])

    def own_copy(ref):
        return remote(trans.at[0], ref, own_send, own_recv, (tile, other))

    def side_copy(ref, side, k):
        span = pl.ds(k * (ROWS // CHUNKS), ROWS // CHUNKS)
        return remote(
            short.at[:, span, :], ref.at[side, :, span, :], side_send.at[side, k], side_recv.at[side, k],
            (beside[side], depth),
        )

    def relay_copy(ref, side, k):
        span = pl.ds(k * (ROWS // CHUNKS), ROWS // CHUNKS)
        return remote(
            ref.at[side, :, span, :], ref.at[side, :, span, :], relay_send.at[side, k], relay_recv.at[side, k],
            (tile, other),
        )

    def place_copy(side):
        return remote(places, places_in.at[side], place_send.at[side], place_recv.at[side], (beside[side], depth))

    def grad_copy(p, home, side):
        target = depth if home == 0 else other
        return remote(
            halo_out.at[p, home], halo_in.at[side, depth, p], grad_send.at[p, home, side],
            grad_recv.at[side, depth, p], (beside[side], target),
        )

    def grad_arrival(p, core, side):
        return remote(
            halo_out.at[p, 0], halo_in.at[side, core, p], grad_send.at[p, 0, side], grad_recv.at[side, core, p],
            (beside[side], depth),
        )

    def part_copy(p):
        return remote(own_out.at[p], own_in.at[p], part_send.at[p], part_recv.at[p], (tile, other))

    mine = {0: (own_a, halo_a), 1: (own_b, halo_b)}
    for d in range(2):
        @pl.when(depth == d)
        def _():
            own_load(mine[d][0]).start()
    smalls = [
        pltpu.make_async_copy(src, dst, small_sem.at[n])
        for n, (src, dst) in enumerate(
            (
                (rows_in, rows), (cols_in, cols), (counts_in, counts),
                (dataset_in, dataset), (dose_in, dose), (ground_in, ground),
            )
        )
    ]
    for load in smalls + loads:
        load.start()
    for d in range(2):
        @pl.when(depth == d)
        def _():
            own_load(mine[d][0]).wait()
            for c in range(2):
                short[c] = mine[d][0][c].astype(BF)
    pl.semaphore_wait(barrier, 1 + 2 * (lower.astype(jnp.int32) + upper.astype(jnp.int32)))

    def sides(flags, act):
        for side in range(2):
            @pl.when(flags[side])
            def _():
                act(side)

    def send_tiles(ref):
        for k in range(CHUNKS):
            sides(sends, lambda side: side_copy(ref, side, k).start())

    for d in range(2):
        @pl.when(depth == d)
        def _():
            own_copy(mine[d][0]).start()
    @pl.when(depth == 0)
    def _():
        send_tiles(halo_a)

    def spot(p):
        slot = depth * SLOTS + p
        return slot, jnp.clip(rows[slot], 0, ROWS - L), jnp.clip(cols[slot], 0, Q - 1)

    for load in smalls:
        load.wait()
    for n in range(4):
        places[n : n + 1, :] = jnp.full((1, Q), rows[n], jnp.int32)
        places[n + 4 : n + 5, :] = jnp.full((1, Q), cols[n], jnp.int32)
    for load in loads:
        load.wait()

    def turn(p, _):
        rotate_probe(probe, pr_ref, spin, p, spot(p)[2])
        amplitudes(measured, p, split, amp_ref, int_ref)
        return 0

    lax.fori_loop(0, SLOTS, turn, 0)

    def take(side, k, ref):
        side_copy(ref, side, k).wait_recv()
        relay_copy(ref, side, k).start()

    @pl.when(depth == 0)
    def _():
        for k in range(RELEASE):
            sides(sends, lambda side: side_copy(halo_a, side, k).wait_send())
        pl.semaphore_signal(go, inc=1, device_id=(tile, other), device_id_type=MESH)
        for k in range(CHUNKS):
            sides(takes, lambda side: take(side, k, halo_a))
        for k in range(RELEASE, CHUNKS):
            sides(sends, lambda side: side_copy(halo_a, side, k).wait_send())
        own_copy(own_b).wait_recv()

    @pl.when(depth == 1)
    def _():
        pl.semaphore_wait(go, 1)
        send_tiles(halo_b)
        own_copy(own_a).wait_recv()
        for k in range(CHUNKS):
            sides(takes, lambda side: relay_copy(halo_a, side, k).wait_recv())
    own_copy(own_a).wait_send()
    sides(sends, lambda side: place_copy(side).start())
    widen(halo_a, wide, takes)

    def start(p, _):
        _, row, col = spot(p)
        load_patch(own_a, wide, o_ref, 2 * p, row, col)
        forward_first(table, pr_ref, o_ref, p, z, u, w, psi_ref)

        @pl.when(depth == 1)
        def _():
            for kk in range(CHUNKS // SLOTS):
                sides(takes, lambda side: take(side, p * (CHUNKS // SLOTS) + kk, halo_b))
        return 0

    lax.fori_loop(0, SLOTS, start, 0)

    @pl.when(depth == 0)
    def _():
        for k in range(CHUNKS):
            sides(takes, lambda side: relay_copy(halo_b, side, k).wait_recv())
            sides(takes, lambda side: relay_copy(halo_a, side, k).wait_send())

    @pl.when(depth == 1)
    def _():
        for k in range(CHUNKS):
            sides(sends, lambda side: side_copy(halo_b, side, k).wait_send())
            sides(takes, lambda side: relay_copy(halo_b, side, k).wait_send())

    widen(halo_b, wide, takes)

    def hand_over(p, s):
        place = 2 * p + s
        @pl.when(depth == s)
        def _():
            halo_out[p, 0] = grad_ref[place, :, :, 0:Q].astype(BF)
            sides(sends, lambda side: grad_copy(p, 0, side).start())
            own_mine[p] = grad_ref[place, :, :, Q:L]
        @pl.when(depth != s)
        def _():
            halo_out[p, 1] = grad_ref[place, :, :, 0:Q].astype(BF)
            sides(sends, lambda side: grad_copy(p, 1, side).start())
            own_out[p] = grad_ref[place, :, :, Q:L].astype(BF)
            part_copy(p).start()

    def finish(p, _):
        slot, row, col = spot(p)
        which = jnp.clip(dataset[slot], 0, dose.shape[0] - 1)
        load_patch(own_b, wide, o_ref, 2 * p + 1, row, col)
        forward_last(table, o_ref, p, z, u, psi_ref, far_ref, int_ref)
        residual_factor(int_ref, amp_ref, p, fac_ref, dose[which], ground[which], slot < counts[0])
        backward_last(table, o_ref, p, z, u, w, psi_ref, far_ref, fac_ref, grad_ref, gz)
        hand_over(p, 1)
        backward_first(table, pr_ref, p, u, w, grad_ref, gz)
        hand_over(p, 0)
        return 0

    lax.fori_loop(0, SLOTS, finish, 0)

    sides(sends, lambda side: place_copy(side).wait_send())
    sides(takes, lambda side: place_copy(side).wait_recv())
    for p in range(SLOTS):
        part_copy(p).wait()
        for n in range(2):
            sides(sends, lambda side: grad_copy(p, n, side).wait_send())
            sides(takes, lambda side: grad_arrival(p, n, side).wait_recv())


def waves(scalars, transmission, probe, measured):
    vm = pl.BlockSpec(memory_space=VMEM)
    hbm = pl.BlockSpec(memory_space=pltpu.HBM)
    dma = pltpu.SemaphoreType.DMA
    return pl.pallas_call(
        wave_kernel,
        out_shape=(
            jax.ShapeDtypeStruct((SLOTS, 2, L, Q), F32),
            jax.ShapeDtypeStruct((SLOTS, 2, L, Q), BF),
            jax.ShapeDtypeStruct((2, 2, SLOTS, 2, L, Q), BF),
            jax.ShapeDtypeStruct((2, 8, Q), jnp.int32),
        ),
        in_specs=[hbm] * 11,
        out_specs=(vm,) * 4,
        scratch_shapes=[
            VMEM((2, ROWS, Q), F32),
            VMEM((2, ROWS, Q), F32),
            VMEM((2, 2, ROWS, Q), BF),
            VMEM((2, 2, ROWS, Q), BF),
            VMEM((2, ROWS, Q), BF),
            VMEM((8, Q), jnp.int32),
            VMEM((SLOTS, 2, L, Q), BF),
            VMEM((SLOTS, 2, 2, L, Q), BF),
            VMEM((MODES, 2, L, L), F32),
            VMEM((SLOTS, L, L), F32),
            VMEM((2, 2, 2, L, L), BF),
            VMEM((L, L), BF),
            VMEM((L, L), BF),
            VMEM((4, 2, L, L), F32),
            VMEM((SLOTS, MODES, 2, L, L), F32),
            VMEM((SLOTS, MODES, 2, L, L), F32),
            VMEM((MODES, 2, L, L), F32),
            VMEM((2, L, Q), F32),
            VMEM((2, L, Q), F32),
            VMEM((SLOTS, 2, Q, L), F32),
            VMEM((GROUP, 2, L, L), BF),
            VMEM((GROUP, 2, L, L), BF),
            VMEM((GROUP, 2, L, L), F32),
            VMEM((MODES, 2, L, L), BF),
            VMEM((4, 2, L, L), F32),
            VMEM((2, 2, ROWS, Q), F32),
            dma((5,)),
            dma(()),
            dma(()),
            dma((2, CHUNKS)),
            dma((2, CHUNKS)),
            dma((2, CHUNKS)),
            dma((2, CHUNKS)),
            dma((2,)),
            dma((2,)),
            dma((SLOTS, 2, 2)),
            dma((2, 2, SLOTS)),
            dma((SLOTS,)),
            dma((SLOTS,)),
            pltpu.SemaphoreType.REGULAR,
            SMEM((4,), jnp.int32),
            SMEM((4,), jnp.int32),
            SMEM((1,), jnp.int32),
            SMEM((4,), jnp.int32),
            SMEM((16,), F32),
            SMEM((16,), F32),
            dma((6,)),
        ],
        compiler_params=pltpu.CompilerParams(
            vmem_limit_bytes=48 * 2**20, collective_id=0, has_side_effects=True
        ),
        name="waves",
    )(
        *[
            x if x.shape == (1,) else pltpu.with_memory_space_constraint(x, pltpu.HBM)
            for x in (
                *scalars,
                transmission,
                probe,
                measured,
                jnp.asarray(tables()).astype(BF),
                jnp.asarray(lane_split()).astype(BF),
            )
        ]
    )


def combine_kernel(rows, places, mine, theirs, halo, out_hbm, out, sem):
    depth = lax.axis_index("depth")
    tile = lax.axis_index("tile")
    lane = lax.broadcasted_iota(jnp.int32, (L, Q), 1)

    def copy(c):
        return pltpu.make_async_copy(out.at[c], out_hbm.at[c], sem.at[c])

    for c in range(2):
        out[c] = jnp.zeros((ROWS, Q), F32)

        def add(row, values):
            out[c, pl.ds(jnp.clip(row, 0, ROWS - L), L), :] += values

        for p in range(SLOTS):
            add(rows[depth * SLOTS + p], mine[p, c])
            add(rows[(1 - depth) * SLOTS + p], theirs[p, c].astype(F32))
            for core in range(2):
                slot = core * SLOTS + p

                @pl.when(tile > 0)
                def _():
                    kept = lane < places[0, slot + 4, 0]
                    add(places[0, slot, 0], jnp.where(kept, halo[0, core, p, c].astype(F32), 0.0))

                @pl.when(tile < lax.axis_size("tile") - 1)
                def _():
                    kept = lane >= places[1, slot + 4, 0]
                    add(places[1, slot, 0], jnp.where(kept, halo[1, core, p, c].astype(F32), 0.0))
        copy(c).start()
    for c in range(2):
        copy(c).wait()


def combine(rows, places, parts):
    vm = pl.BlockSpec(memory_space=VMEM)
    return pl.pallas_call(
        combine_kernel,
        out_shape=jax.ShapeDtypeStruct((2, ROWS, Q), F32),
        in_specs=[pl.BlockSpec(memory_space=SMEM)] * 2 + [vm] * 3,
        out_specs=pl.BlockSpec(memory_space=pltpu.HBM),
        scratch_shapes=[VMEM((2, ROWS, Q), F32), pltpu.SemaphoreType.DMA((2,))],
        compiler_params=pltpu.CompilerParams(vmem_limit_bytes=8 * 2**20),
        name="combine",
    )(rows, places, *parts)


def shards(transmission, probe_modes, measured, scan_rows, scan_cols, counts, dataset, dose_scale, background):
    mine, theirs, halo, places = waves(
        (scan_rows, scan_cols, counts, dataset, dose_scale, background), transmission, probe_modes, measured
    )
    return combine(scan_rows, places, (mine, theirs, halo))[None]


def solution(mesh):
    in_specs = (
        P("depth", None, None, "tile"),
        P(),
        P("tile", None, None),
        P("tile"),
        P("tile"),
        P("tile"),
        P("tile"),
        P(),
        P(),
    )
    out_specs = P("depth", None, None, "tile")
    return jax.shard_map(shards, mesh=mesh, in_specs=in_specs, out_specs=out_specs, check_vma=False)
```

```python
import functools
import math

import jax
import jax.numpy as jnp
import numpy as np
from jax import lax
from jax.experimental import pallas as pl
from jax.experimental.pallas import tpu as pltpu
from jax.sharding import PartitionSpec as P

L = 256
Q = 128
MODES = 6
GROUP = 6
SLOTS = 2
ROWS = 1024
BF = jnp.bfloat16
F32 = jnp.float32
VMEM = pltpu.VMEM
SMEM = pltpu.SMEM


def rounded(values):
    return np.asarray(values, np.float32).astype(jnp.bfloat16).astype(np.float64)


def block(values):
    re, im = values.real, values.imag
    full = np.block([[re, -im], [im, re]])
    return np.stack([full, full.T])


@functools.cache
def tables():
    k = np.arange(L)
    dft = np.exp(-2j * np.pi / L * (k[:, None] * k[None, :] % L)) / math.sqrt(L)
    signed = np.where(k < Q, k, k - L)
    filt = np.exp(-1j * np.pi / L * (signed * signed % (2 * L)))
    prop = dft.conj() @ (filt[:, None] * dft)
    prop = rounded(prop.real) + 1j * rounded(prop.imag)
    dft = rounded(dft.real) + 1j * rounded(dft.imag)
    near, far = prop[:Q, :Q], prop[:Q, Q:]
    halves = [(near + far) / 2, (near - far) / 2]
    kinds = [[block(h) for h in halves], [block(dft[0::2, :Q]), block(dft[1::2, :Q])]]
    return np.stack([np.stack(kind) for kind in kinds]).astype(np.float32)


@functools.cache
def lane_split():
    k = np.arange(L)
    return (k[:, None] == np.where(k < Q, 2 * k, 2 * (k - Q) + 1)[None, :]).astype(np.float32)


def dot(a, b):
    return jnp.dot(a, b, preferred_element_type=F32)


def hadamard(q):
    s0, d0 = q[0][0] + q[0][1], q[0][0] - q[0][1]
    s1, d1 = q[1][0] + q[1][1], q[1][0] - q[1][1]
    return [[s0 + s1, d0 + d1], [s0 - s1, d0 - d1]]


def quads(fn):
    return [[fn(i, j) for j in range(2)] for i in range(2)]


CH = 8


def store_waves(z_ref, m, r, re, im):
    for i in range(2):
        for j in range(2):
            z_ref[m, i, r : r + CH, Q * j : Q * j + Q] = re[i][j].astype(BF)
            z_ref[m, i, Q + r : Q + r + CH, Q * j : Q * j + Q] = im[i][j].astype(BF)


def left_side(table, kind, back, z_ref, u_ref, m):
    for i in range(2):
        u = dot(table[kind, i, back], z_ref[m, i]).astype(BF)
        for j in range(2):
            u_ref[m, j, Q * i : Q * i + Q, 0:Q] = u[0:Q, Q * j : Q * j + Q]
            u_ref[m, j, Q * i : Q * i + Q, Q:L] = u[Q:L, Q * j : Q * j + Q]


def right_side(table, kind, back, u_ref, w_ref, m):
    for j in range(2):
        w_ref[m, j] = dot(u_ref[m, j], table[kind, j, 1 - back])


def read_waves(w_ref, m, r):
    re = quads(lambda i, j: w_ref[m, j, Q * i + r : Q * i + r + CH, 0:Q])
    im = quads(lambda i, j: w_ref[m, j, Q * i + r : Q * i + r + CH, Q:L])
    return re, im


def rotate_probe(probe, pr_ref, spin, p, col):
    shift = lax.broadcasted_iota(jnp.int32, (L, L), 1) - lax.broadcasted_iota(jnp.int32, (L, L), 0)
    spin[...] = jnp.where((shift == col) | (shift == col - L), 1.0, 0.0).astype(BF)

    def one(m, _):
        for c in range(2):
            x = probe[m, c]
            hi = x.astype(BF)
            lo = (x - hi.astype(F32)).astype(BF)
            pr_ref[p, m, c] = dot(hi, spin[...]) + dot(lo, spin[...])
        return 0

    lax.fori_loop(0, MODES, one, 0)


def widen(halo, wide, takes):
    for side in range(2):
        @pl.when(takes[side])
        def _():
            for c in range(2):
                wide[side, c] = halo[side, c].astype(F32)

        @pl.when(jnp.logical_not(takes[side]))
        def _():
            wide[side] = jnp.zeros((2, ROWS, Q), F32)


def load_patch(own, wide, o_ref, place, row, col):
    lane = lax.broadcasted_iota(jnp.int32, (L, Q), 1)
    right = lane < col
    for c in range(2):
        o_ref[place, c, :, 0:Q] = jnp.where(right, wide[1, c, pl.ds(row, L), :], wide[0, c, pl.ds(row, L), :])
        o_ref[place, c, :, Q:L] = own[c, pl.ds(row, L), :]


def amplitudes(measured, slot, split, amp_ref, tmp_ref):
    for j in range(2):
        tmp_ref[j] = jnp.sqrt(measured[slot, :, Q * j : Q * j + Q])
    for i in range(2):
        x = jnp.concatenate([tmp_ref[j, pl.ds(i, Q, stride=2), :] for j in range(2)], axis=1)
        hi = x.astype(BF)
        rest = x - hi.astype(F32)
        mid = rest.astype(BF)
        lo = (rest - mid.astype(F32)).astype(BF)
        amp_ref[slot, i] = dot(hi, split[...]) + (dot(mid, split[...]) + dot(lo, split[...]))


def forward_first(table, pr_ref, o_ref, p, z, u, w, psi_ref):
    def group(g, _):
        for k in range(GROUP):
            m = g * GROUP + k
            for r in range(0, Q, CH):
                re, im = [[None] * 2 for _ in range(2)], [[None] * 2 for _ in range(2)]
                for i in range(2):
                    for j in range(2):
                        rows, lanes = slice(Q * i + r, Q * i + r + CH), slice(Q * j, Q * j + Q)
                        a, b = pr_ref[p, m, 0, rows, lanes], pr_ref[p, m, 1, rows, lanes]
                        c, d = o_ref[2 * p, 0, rows, lanes], o_ref[2 * p, 1, rows, lanes]
                        re[i][j], im[i][j] = a * c - b * d, a * d + b * c
                store_waves(z, k, r, hadamard(re), hadamard(im))
        for k in range(GROUP):
            left_side(table, 0, 0, z, u, k)
        for k in range(GROUP):
            right_side(table, 0, 0, u, w, k)
        for k in range(GROUP):
            m = g * GROUP + k
            for r in range(0, Q, CH):
                vre, vim = read_waves(w, k, r)
                vre, vim = hadamard(vre), hadamard(vim)
                for i in range(2):
                    for j in range(2):
                        rows, lanes = slice(Q * i + r, Q * i + r + CH), slice(Q * j, Q * j + Q)
                        psi_ref[p, m, 0, rows, lanes] = vre[i][j]
                        psi_ref[p, m, 1, rows, lanes] = vim[i][j]
        return 0

    group(0, 0)


def forward_last(table, o_ref, p, z, u, psi_ref, far_ref, int_ref):
    def group(g, _):
        for k in range(GROUP):
            m = g * GROUP + k
            for r in range(0, Q, CH):
                re, im = [[None] * 2 for _ in range(2)], [[None] * 2 for _ in range(2)]
                for i in range(2):
                    for j in range(2):
                        rows, lanes = slice(Q * i + r, Q * i + r + CH), slice(Q * j, Q * j + Q)
                        a = psi_ref[p, m, 0, rows, lanes]
                        b = psi_ref[p, m, 1, rows, lanes]
                        c, d = o_ref[2 * p + 1, 0, rows, lanes], o_ref[2 * p + 1, 1, rows, lanes]
                        re[i][j], im[i][j] = a * c - b * d, a * d + b * c
                store_waves(z, k, r, hadamard(re), hadamard(im))
        for k in range(GROUP):
            left_side(table, 1, 0, z, u, k)
        for k in range(GROUP):
            for j in range(2):
                far_ref[g * GROUP + k, j] = dot(u[k, j], table[1, j, 1])
        for j in range(2):
            for r in range(0, L, CH):
                total = None
                for k in range(GROUP):
                    x = far_ref[g * GROUP + k, j, r : r + CH, 0:Q]
                    y = far_ref[g * GROUP + k, j, r : r + CH, Q:L]
                    power = x * x + y * y
                    total = power if total is None else total + power
                int_ref[j, r : r + CH, :] = total
        return 0

    group(0, 0)


def residual_factor(int_ref, amp_ref, p, fac_ref, scale, offset, valid):
    for j in range(2):
        for i in range(2):
            intensity = scale * int_ref[j, Q * i : Q * i + Q, :] + offset
            ratio = amp_ref[p, i, :, Q * j : Q * j + Q] / jnp.sqrt(intensity)
            fac_ref[j, Q * i : Q * i + Q, :] = jnp.where(valid, scale * (1.0 - ratio), 0.0)


def cells(r):
    return [(i, j, slice(Q * i + r, Q * i + r + CH), slice(Q * j, Q * j + Q)) for i in range(2) for j in range(2)]


def add_conj(sums, n, a, b, x, y):
    gre, gim = a * x + b * y, a * y - b * x
    sums[n] = (gre, gim) if sums[n] is None else (sums[n][0] + gre, sums[n][1] + gim)


def store_sums(grad_ref, place, r, sums):
    for n, (i, j, rows, lanes) in enumerate(cells(r)):
        grad_ref[place, 0, rows, lanes], grad_ref[place, 1, rows, lanes] = sums[n]


def backward_last(table, o_ref, p, z, u, w, psi_ref, far_ref, fac_ref, grad_ref, gz_ref):
    def group(g, _):
        for k in range(GROUP):
            m = g * GROUP + k
            for j in range(2):
                for r in range(0, L, CH):
                    f = fac_ref[j, r : r + CH, :]
                    i, s = r // Q, r % Q
                    z[k, i, s : s + CH, Q * j : Q * j + Q] = (f * far_ref[m, j, r : r + CH, 0:Q]).astype(BF)
                    z[k, i, Q + s : Q + s + CH, Q * j : Q * j + Q] = (
                        f * far_ref[m, j, r : r + CH, Q:L]
                    ).astype(BF)
        for k in range(GROUP):
            left_side(table, 1, 1, z, u, k)
        for k in range(GROUP):
            right_side(table, 1, 1, u, w, k)
        for k in range(GROUP):
            m = g * GROUP + k
            for r in range(0, Q, CH):
                vre, vim = read_waves(w, k, r)
                vre, vim = hadamard(vre), hadamard(vim)
                re, im = [[None] * 2 for _ in range(2)], [[None] * 2 for _ in range(2)]
                for n, (i, j, rows, lanes) in enumerate(cells(r)):
                    x, y = vre[i][j], vim[i][j]
                    a, b = psi_ref[p, m, 0, rows, lanes], psi_ref[p, m, 1, rows, lanes]
                    gre, gim = a * x + b * y, a * y - b * x
                    if k > 0:
                        gre, gim = grad_ref.at[2 * p + 1][0, rows, lanes] + gre, grad_ref.at[2 * p + 1][1, rows, lanes] + gim
                    grad_ref.at[2 * p + 1][0, rows, lanes], grad_ref.at[2 * p + 1][1, rows, lanes] = gre, gim
                    c, d = o_ref[2 * p + 1, 0, rows, lanes], o_ref[2 * p + 1, 1, rows, lanes]
                    re[i][j], im[i][j] = c * x + d * y, c * y - d * x
                store_waves(gz_ref, m, r, hadamard(re), hadamard(im))
        return 0

    group(0, 0)


def backward_first(table, pr_ref, p, u, w, grad_ref, gz_ref):
    def group(g, _):
        for k in range(GROUP):
            m = g * GROUP + k
            for i in range(2):
                x = dot(table[0, i, 1], gz_ref[m, i]).astype(BF)
                for j in range(2):
                    u[k, j, Q * i : Q * i + Q, 0:Q] = x[0:Q, Q * j : Q * j + Q]
                    u[k, j, Q * i : Q * i + Q, Q:L] = x[Q:L, Q * j : Q * j + Q]
        for k in range(GROUP):
            right_side(table, 0, 1, u, w, k)
        for r in range(0, Q, CH):
            sums = [None] * 4
            for k in range(GROUP):
                m = g * GROUP + k
                vre, vim = read_waves(w, k, r)
                vre, vim = hadamard(vre), hadamard(vim)
                for n, (i, j, rows, lanes) in enumerate(cells(r)):
                    a, b = pr_ref[p, m, 0, rows, lanes], pr_ref[p, m, 1, rows, lanes]
                    add_conj(sums, n, a, b, vre[i][j], vim[i][j])
            store_sums(grad_ref, 2 * p, r, sums)
        return 0

    group(0, 0)


CHUNKS = 8
RELEASE = 7
MESH = pl.DeviceIdType.MESH


def wave_kernel(
    rows_in, cols_in, counts_in, dataset_in, dose_in, ground_in,
    trans, probe_in, measured_in, table_in, split_in,
    own_mine, own_in, halo_in, places_in,
    own_a, own_b, halo_a, halo_b, short, places, own_out, halo_out,
    probe, measured, table, split, spin,
    o_ref, pr_ref, psi_ref, far_ref, int_ref, fac_ref, amp_ref, z, u, w, gz, grad_ref, wide,
    load_sem, own_send, own_recv, side_send, side_recv, relay_send, relay_recv,
    place_send, place_recv, grad_send, grad_recv, part_send, part_recv, go,
    rows, cols, counts, dataset, dose, ground, small_sem,
):
    depth = lax.axis_index("depth")
    tile = lax.axis_index("tile")
    tiles = lax.axis_size("tile")
    ahead, behind = lax.rem(tile + 1, tiles), lax.rem(tile + tiles - 1, tiles)
    other = 1 - depth
    beside = (ahead, behind)

    upper, lower = tile < tiles - 1, tile > 0
    sends, takes = (upper, lower), (lower, upper)

    barrier = pltpu.get_barrier_semaphore()
    pl.semaphore_signal(barrier, inc=1, device_id=(tile, other), device_id_type=MESH)
    for side in range(2):
        @pl.when(sends[side])
        def _():
            for core in (depth, other):
                pl.semaphore_signal(barrier, inc=1, device_id=(beside[side], core), device_id_type=MESH)

    def remote(src, dst, send, recv, target):
        return pltpu.make_async_remote_copy(
            src_ref=src, dst_ref=dst, send_sem=send, recv_sem=recv, device_id=target, device_id_type=MESH
        )

    loads = [
        pltpu.make_async_copy(probe_in, probe, load_sem.at[0]),
        pltpu.make_async_copy(measured_in.at[pl.ds(depth * SLOTS, SLOTS)], measured, load_sem.at[1]),
        pltpu.make_async_copy(table_in, table, load_sem.at[2]),
        pltpu.make_async_copy(split_in, split, load_sem.at[3]),
    ]

    def own_load(ref):
        return pltpu.make_async_copy(trans.at[0], ref, load_sem.at[4])

    def own_copy(ref):
        return remote(trans.at[0], ref, own_send, own_recv, (tile, other))

    def side_copy(ref, side, k):
        span = pl.ds(k * (ROWS // CHUNKS), ROWS // CHUNKS)
        return remote(
            short.at[:, span, :], ref.at[side, :, span, :], side_send.at[side, k], side_recv.at[side, k],
            (beside[side], depth),
        )

    def relay_copy(ref, side, k):
        span = pl.ds(k * (ROWS // CHUNKS), ROWS // CHUNKS)
        return remote(
            ref.at[side, :, span, :], ref.at[side, :, span, :], relay_send.at[side, k], relay_recv.at[side, k],
            (tile, other),
        )

    def place_copy(side):
        return remote(places, places_in.at[side], place_send.at[side], place_recv.at[side], (beside[side], depth))

    def grad_copy(p, home, side):
        target = depth if home == 0 else other
        return remote(
            halo_out.at[p, home], halo_in.at[side, depth, p], grad_send.at[p, home, side],
            grad_recv.at[side, depth, p], (beside[side], target),
        )

    def grad_arrival(p, core, side):
        return remote(
            halo_out.at[p, 0], halo_in.at[side, core, p], grad_send.at[p, 0, side], grad_recv.at[side, core, p],
            (beside[side], depth),
        )

    def part_copy(p):
        return remote(own_out.at[p], own_in.at[p], part_send.at[p], part_recv.at[p], (tile, other))

    mine = {0: (own_a, halo_a), 1: (own_b, halo_b)}
    for d in range(2):
        @pl.when(depth == d)
        def _():
            own_load(mine[d][0]).start()
    smalls = [
        pltpu.make_async_copy(src, dst, small_sem.at[n])
        for n, (src, dst) in enumerate(
            (
                (rows_in, rows), (cols_in, cols), (counts_in, counts),
                (dataset_in, dataset), (dose_in, dose), (ground_in, ground),
            )
        )
    ]
    for load in smalls + loads:
        load.start()
    for d in range(2):
        @pl.when(depth == d)
        def _():
            own_load(mine[d][0]).wait()
            for c in range(2):
                short[c] = mine[d][0][c].astype(BF)
    pl.semaphore_wait(barrier, 1 + 2 * (lower.astype(jnp.int32) + upper.astype(jnp.int32)))

    def sides(flags, act):
        for side in range(2):
            @pl.when(flags[side])
            def _():
                act(side)

    def send_tiles(ref):
        for k in range(CHUNKS):
            sides(sends, lambda side: side_copy(ref, side, k).start())

    for d in range(2):
        @pl.when(depth == d)
        def _():
            own_copy(mine[d][0]).start()
    @pl.when(depth == 0)
    def _():
        send_tiles(halo_a)

    def spot(p):
        slot = depth * SLOTS + p
        return slot, jnp.clip(rows[slot], 0, ROWS - L), jnp.clip(cols[slot], 0, Q - 1)

    for load in smalls:
        load.wait()
    for n in range(4):
        places[n : n + 1, :] = jnp.full((1, Q), rows[n], jnp.int32)
        places[n + 4 : n + 5, :] = jnp.full((1, Q), cols[n], jnp.int32)
    for load in loads:
        load.wait()

    def turn(p, _):
        rotate_probe(probe, pr_ref, spin, p, spot(p)[2])
        amplitudes(measured, p, split, amp_ref, int_ref)
        return 0

    lax.fori_loop(0, SLOTS, turn, 0)

    def take(side, k, ref):
        side_copy(ref, side, k).wait_recv()
        relay_copy(ref, side, k).start()

    @pl.when(depth == 0)
    def _():
        for k in range(RELEASE):
            sides(sends, lambda side: side_copy(halo_a, side, k).wait_send())
        pl.semaphore_signal(go, inc=1, device_id=(tile, other), device_id_type=MESH)
        for k in range(CHUNKS):
            sides(takes, lambda side: take(side, k, halo_a))
        for k in range(RELEASE, CHUNKS):
            sides(sends, lambda side: side_copy(halo_a, side, k).wait_send())
        own_copy(own_b).wait_recv()

    @pl.when(depth == 1)
    def _():
        pl.semaphore_wait(go, 1)
        send_tiles(halo_b)
        own_copy(own_a).wait_recv()
        for k in range(CHUNKS):
            sides(takes, lambda side: relay_copy(halo_a, side, k).wait_recv())
    own_copy(own_a).wait_send()
    sides(sends, lambda side: place_copy(side).start())
    widen(halo_a, wide, takes)

    def start(p, _):
        _, row, col = spot(p)
        load_patch(own_a, wide, o_ref, 2 * p, row, col)
        forward_first(table, pr_ref, o_ref, p, z, u, w, psi_ref)

        @pl.when(depth == 1)
        def _():
            for kk in range(CHUNKS // SLOTS):
                sides(takes, lambda side: take(side, p * (CHUNKS // SLOTS) + kk, halo_b))
        return 0

    lax.fori_loop(0, SLOTS, start, 0)

    @pl.when(depth == 0)
    def _():
        for k in range(CHUNKS):
            sides(takes, lambda side: relay_copy(halo_b, side, k).wait_recv())
            sides(takes, lambda side: relay_copy(halo_a, side, k).wait_send())

    @pl.when(depth == 1)
    def _():
        for k in range(CHUNKS):
            sides(sends, lambda side: side_copy(halo_b, side, k).wait_send())
            sides(takes, lambda side: relay_copy(halo_b, side, k).wait_send())

    widen(halo_b, wide, takes)

    def hand_over(p, s):
        place = 2 * p + s
        @pl.when(depth == s)
        def _():
            halo_out[p, 0] = grad_ref[place, :, :, 0:Q].astype(BF)
            sides(sends, lambda side: grad_copy(p, 0, side).start())
            own_mine[p] = grad_ref[place, :, :, Q:L]
        @pl.when(depth != s)
        def _():
            halo_out[p, 1] = grad_ref[place, :, :, 0:Q].astype(BF)
            sides(sends, lambda side: grad_copy(p, 1, side).start())
            own_out[p] = grad_ref[place, :, :, Q:L].astype(BF)
            part_copy(p).start()

    def finish(p, _):
        slot, row, col = spot(p)
        which = jnp.clip(dataset[slot], 0, dose.shape[0] - 1)
        load_patch(own_b, wide, o_ref, 2 * p + 1, row, col)
        forward_last(table, o_ref, p, z, u, psi_ref, far_ref, int_ref)
        residual_factor(int_ref, amp_ref, p, fac_ref, dose[which], ground[which], slot < counts[0])
        backward_last(table, o_ref, p, z, u, w, psi_ref, far_ref, fac_ref, grad_ref, gz)
        hand_over(p, 1)
        backward_first(table, pr_ref, p, u, w, grad_ref, gz)
        hand_over(p, 0)
        return 0

    lax.fori_loop(0, SLOTS, finish, 0)

    sides(sends, lambda side: place_copy(side).wait_send())
    sides(takes, lambda side: place_copy(side).wait_recv())
    for p in range(SLOTS):
        part_copy(p).wait()
        for n in range(2):
            sides(sends, lambda side: grad_copy(p, n, side).wait_send())
            sides(takes, lambda side: grad_arrival(p, n, side).wait_recv())


def waves(scalars, transmission, probe, measured):
    vm = pl.BlockSpec(memory_space=VMEM)
    hbm = pl.BlockSpec(memory_space=pltpu.HBM)
    dma = pltpu.SemaphoreType.DMA
    return pl.pallas_call(
        wave_kernel,
        out_shape=(
            jax.ShapeDtypeStruct((SLOTS, 2, L, Q), F32),
            jax.ShapeDtypeStruct((SLOTS, 2, L, Q), BF),
            jax.ShapeDtypeStruct((2, 2, SLOTS, 2, L, Q), BF),
            jax.ShapeDtypeStruct((2, 8, Q), jnp.int32),
        ),
        in_specs=[hbm] * 11,
        out_specs=(vm,) * 4,
        scratch_shapes=[
            VMEM((2, ROWS, Q), F32),
            VMEM((2, ROWS, Q), F32),
            VMEM((2, 2, ROWS, Q), BF),
            VMEM((2, 2, ROWS, Q), BF),
            VMEM((2, ROWS, Q), BF),
            VMEM((8, Q), jnp.int32),
            VMEM((SLOTS, 2, L, Q), BF),
            VMEM((SLOTS, 2, 2, L, Q), BF),
            VMEM((MODES, 2, L, L), F32),
            VMEM((SLOTS, L, L), F32),
            VMEM((2, 2, 2, L, L), BF),
            VMEM((L, L), BF),
            VMEM((L, L), BF),
            VMEM((4, 2, L, L), F32),
            VMEM((SLOTS, MODES, 2, L, L), F32),
            VMEM((SLOTS, MODES, 2, L, L), F32),
            VMEM((MODES, 2, L, L), F32),
            VMEM((2, L, Q), F32),
            VMEM((2, L, Q), F32),
            VMEM((SLOTS, 2, Q, L), F32),
            VMEM((GROUP, 2, L, L), BF),
            VMEM((GROUP, 2, L, L), BF),
            VMEM((GROUP, 2, L, L), F32),
            VMEM((MODES, 2, L, L), BF),
            VMEM((4, 2, L, L), F32),
            VMEM((2, 2, ROWS, Q), F32),
            dma((5,)),
            dma(()),
            dma(()),
            dma((2, CHUNKS)),
            dma((2, CHUNKS)),
            dma((2, CHUNKS)),
            dma((2, CHUNKS)),
            dma((2,)),
            dma((2,)),
            dma((SLOTS, 2, 2)),
            dma((2, 2, SLOTS)),
            dma((SLOTS,)),
            dma((SLOTS,)),
            pltpu.SemaphoreType.REGULAR,
            SMEM((4,), jnp.int32),
            SMEM((4,), jnp.int32),
            SMEM((1,), jnp.int32),
            SMEM((4,), jnp.int32),
            SMEM((16,), F32),
            SMEM((16,), F32),
            dma((6,)),
        ],
        compiler_params=pltpu.CompilerParams(
            vmem_limit_bytes=48 * 2**20, collective_id=0, has_side_effects=True
        ),
        name="waves",
    )(
        *[
            x if x.shape == (1,) else pltpu.with_memory_space_constraint(x, pltpu.HBM)
            for x in (
                *scalars,
                transmission,
                probe,
                measured,
                jnp.asarray(tables()).astype(BF),
                jnp.asarray(lane_split()).astype(BF),
            )
        ]
    )


def combine_kernel(rows, places, mine, theirs, halo, out_hbm, out, sem):
    depth = lax.axis_index("depth")
    tile = lax.axis_index("tile")
    lane = lax.broadcasted_iota(jnp.int32, (L, Q), 1)

    def copy(c):
        return pltpu.make_async_copy(out.at[c], out_hbm.at[c], sem.at[c])

    for c in range(2):
        out[c] = jnp.zeros((ROWS, Q), F32)

        def add(row, values):
            out[c, pl.ds(jnp.clip(row, 0, ROWS - L), L), :] += values

        for p in range(SLOTS):
            add(rows[depth * SLOTS + p], mine[p, c])
            add(rows[(1 - depth) * SLOTS + p], theirs[p, c].astype(F32))
            for core in range(2):
                slot = core * SLOTS + p

                @pl.when(tile > 0)
                def _():
                    kept = lane < places[0, slot + 4, 0]
                    add(places[0, slot, 0], jnp.where(kept, halo[0, core, p, c].astype(F32), 0.0))

                @pl.when(tile < lax.axis_size("tile") - 1)
                def _():
                    kept = lane >= places[1, slot + 4, 0]
                    add(places[1, slot, 0], jnp.where(kept, halo[1, core, p, c].astype(F32), 0.0))
        copy(c).start()
    for c in range(2):
        copy(c).wait()


def combine(rows, places, parts):
    vm = pl.BlockSpec(memory_space=VMEM)
    return pl.pallas_call(
        combine_kernel,
        out_shape=jax.ShapeDtypeStruct((2, ROWS, Q), F32),
        in_specs=[pl.BlockSpec(memory_space=SMEM)] * 2 + [vm] * 3,
        out_specs=pl.BlockSpec(memory_space=pltpu.HBM),
        scratch_shapes=[VMEM((2, ROWS, Q), F32), pltpu.SemaphoreType.DMA((2,))],
        compiler_params=pltpu.CompilerParams(vmem_limit_bytes=8 * 2**20),
        name="combine",
    )(rows, places, *parts)


def shards(transmission, probe_modes, measured, scan_rows, scan_cols, counts, dataset, dose_scale, background):
    mine, theirs, halo, places = waves(
        (scan_rows, scan_cols, counts, dataset, dose_scale, background), transmission, probe_modes, measured
    )
    return combine(scan_rows, places, (mine, theirs, halo))[None]


def solution(mesh):
    in_specs = (
        P("depth", None, None, "tile"),
        P(),
        P("tile", None, None),
        P("tile"),
        P("tile"),
        P("tile"),
        P("tile"),
        P(),
        P(),
    )
    out_specs = P("depth", None, None, "tile")
    return jax.shard_map(shards, mesh=mesh, in_specs=in_specs, out_specs=out_specs, check_vma=False)
```
